8 devices in a mesh: dp: 1 (over z), tp: 2 (over y), sp: 4 (over x, core).
Axes of the slice: x: 2, y: 2, z: 1, core: 2. Of those that a mesh axis runs over, the one named last changes fastest.
Arguments:
- hidden: bfloat16 [64, 3072], P('dp')
- positions: int32 [64], P('dp')
- k_cache: bfloat16 [2, 64, 256, 8, 128], P(None, 'dp', 'sp', 'tp')
- v_cache: bfloat16 [2, 64, 256, 8, 128], P(None, 'dp', 'sp', 'tp')
- ln_gain: bfloat16 [2, 2, 3072], replicated
- ln_bias: bfloat16 [2, 2, 3072], replicated
- w_qkv: bfloat16 [2, 3072, 5120], P(None, None, 'tp')
- b_qkv: bfloat16 [2, 5120], P(None, 'tp')
- w_dense: bfloat16 [2, 3072, 3072], P(None, 'tp')
- b_dense: bfloat16 [2, 3072], replicated
- w_up: bfloat16 [2, 3072, 16384], P(None, None, 'tp')
- b_up: bfloat16 [2, 16384], P(None, 'tp')
- w_down: bfloat16 [2, 8192, 3072], P(None, 'tp')
- b_down: bfloat16 [2, 3072], replicated
Outputs:
- output 1: bfloat16 [64, 3072], P('dp')
- output 2: bfloat16 [2, 64, 256, 8, 128], P(None, 'dp', 'sp', 'tp')
- output 3: bfloat16 [2, 64, 256, 8, 128], P(None, 'dp', 'sp', 'tp')
All inputs are finite; a program needn't handle non-finite values.
Results may differ from the reference program's by a relative error of at most 0.017098.
Values sent between devices are 32-bit elements.
A program may use at most 1 GiB of HBM per device.

```python
import functools
import jax
import jax.numpy as jnp
from jax import lax

NUM_SEQS = 64
SEQ_LEN = 256
D_MODEL = 3072
N_HEADS = 24
KV_HEADS = 8
HEAD_DIM = 128
FF_DIM = 8192
BLOCK_SIZE = 64
LOCAL_BLOCKS = 16
VERT_STRIDE = 8
ROPE_THETA = 1000000.0
GELU_LIMIT = 20.0
NORM_EPS = 0.00001
MASKED = -1e30
GROUP_SIZE = N_HEADS // KV_HEADS
QKV_COLS = KV_HEADS * (GROUP_SIZE + 2) * HEAD_DIM
QK_GAIN = (3.0 * HEAD_DIM ** 0.5) ** 0.5
V_GAIN = 1.5


def normal_draw(key, shape, scale):
    return (jax.random.normal(key, shape, jnp.float32) * scale).astype(jnp.bfloat16)


def setup_inputs(seed: int = 0, part: int = 0) -> dict:
    base = jax.random.key(seed)
    shared = jax.random.split(base, 10)
    local = jax.random.split(jax.random.fold_in(base, part), 4)
    slot_gain = jnp.concatenate([jnp.full((GROUP_SIZE + 1,), QK_GAIN, jnp.float32), jnp.full((1,), V_GAIN, jnp.float32)])
    col_gain = jnp.tile(jnp.repeat(slot_gain, HEAD_DIM), KV_HEADS)
    seq_ids = jnp.arange(NUM_SEQS)
    rand_pos = jax.random.randint(local[1], (NUM_SEQS,), 0, SEQ_LEN)
    positions = jnp.where(seq_ids == 0, SEQ_LEN - 1, jnp.where(seq_ids == 1, SEQ_LEN // 2 + BLOCK_SIZE // 2, rand_pos))
    cache_shape = (2, NUM_SEQS, SEQ_LEN, KV_HEADS, HEAD_DIM)
    return {
        'hidden': normal_draw(local[0], (NUM_SEQS, D_MODEL), 1.0),
        'positions': positions.astype(jnp.int32),
        'k_cache': normal_draw(local[2], cache_shape, QK_GAIN),
        'v_cache': normal_draw(local[3], cache_shape, V_GAIN),
        'ln_gain': jax.random.uniform(shared[0], (2, 2, D_MODEL), jnp.float32, 0.5, 1.5).astype(jnp.bfloat16),
        'ln_bias': normal_draw(shared[1], (2, 2, D_MODEL), 0.3),
        'w_qkv': normal_draw(shared[2], (2, D_MODEL, QKV_COLS), col_gain * D_MODEL ** -0.5),
        'b_qkv': normal_draw(shared[3], (2, QKV_COLS), col_gain * 0.5),
        'w_dense': normal_draw(shared[4], (2, N_HEADS * HEAD_DIM, D_MODEL), (N_HEADS * HEAD_DIM) ** -0.5),
        'b_dense': normal_draw(shared[5], (2, D_MODEL), 0.3),
        'w_up': normal_draw(shared[6], (2, D_MODEL, 2 * FF_DIM), D_MODEL ** -0.5),
        'b_up': normal_draw(shared[7], (2, 2 * FF_DIM), 0.3),
        'w_down': normal_draw(shared[8], (2, FF_DIM, D_MODEL), FF_DIM ** -0.5),
        'b_down': normal_draw(shared[9], (2, D_MODEL), 0.3),
    }


def layer_norm(vec, gain, shift):
    wide_vec = vec.astype(jnp.float32)
    mean_val = jnp.mean(wide_vec, axis=-1, keepdims=True)
    variance = jnp.mean(jnp.square(wide_vec - mean_val), axis=-1, keepdims=True)
    normed = (wide_vec - mean_val) * lax.rsqrt(variance + NORM_EPS)
    return (normed * gain.astype(jnp.float32) + shift.astype(jnp.float32)).astype(jnp.bfloat16)


def rotary(col_pairs, positions):
    half_dim = HEAD_DIM // 2
    inv_freq = ROPE_THETA ** (-jnp.arange(half_dim).astype(jnp.float32) * (2.0 / HEAD_DIM))
    angles = positions.astype(jnp.float32)[:, None] * inv_freq[None, :]
    cos_part = jnp.cos(angles)[:, None, None, :]
    sin_part = jnp.sin(angles)[:, None, None, :]
    first_half = col_pairs[..., :half_dim]
    second_half = col_pairs[..., half_dim:]
    return jnp.concatenate([first_half * cos_part - second_half * sin_part, second_half * cos_part + first_half * sin_part], axis=-1)


def gegelu(up_proj):
    col_pairs = up_proj.reshape(up_proj.shape[0], -1, 2)
    gate_part = jnp.minimum(col_pairs[..., 0], GELU_LIMIT)
    linear_part = jnp.clip(col_pairs[..., 1], -GELU_LIMIT, GELU_LIMIT)
    return gate_part * jax.nn.sigmoid(1.702 * gate_part) * (linear_part + 1.0)


def seq_attention(packed, sparse):
    query_rot, key_rows, value_rows, position = packed
    slot_ids = jnp.arange(SEQ_LEN)
    keep_mask = (slot_ids <= position)[None, None, :]
    if sparse:
        blocks = slot_ids // BLOCK_SIZE
        head_ids = jnp.arange(N_HEADS).reshape(KV_HEADS, GROUP_SIZE)
        near_mask = (position // BLOCK_SIZE - blocks) < LOCAL_BLOCKS
        vertical = (blocks[None, None, :] + head_ids[:, :, None] + 1) % VERT_STRIDE == 0
        keep_mask = keep_mask & (near_mask[None, None, :] | vertical)
    scores = jnp.einsum('kgd,skd->kgs', query_rot.astype(jnp.float32), key_rows.astype(jnp.float32)) / HEAD_DIM
    scores = jnp.where(keep_mask, scores, MASKED)
    peak_score = jnp.max(scores, axis=-1, keepdims=True)
    weights = jnp.where(keep_mask, jnp.exp(scores - peak_score), 0.0)
    mixed_vals = jnp.einsum('kgs,skd->kgd', weights, value_rows.astype(jnp.float32))
    return (mixed_vals / jnp.sum(weights, axis=-1, keepdims=True)).astype(jnp.bfloat16)


def decoder_layer(hidden, positions, k_layer, v_layer, params, sparse):
    gains, shifts, w_qkv, b_qkv, w_dense, b_dense, w_up, b_up, w_down, b_down = params
    normed = layer_norm(hidden, gains[0], shifts[0])
    qkv_proj = jnp.dot(normed, w_qkv, preferred_element_type=jnp.float32) + b_qkv.astype(jnp.float32)
    qkv_proj = qkv_proj.reshape(NUM_SEQS, KV_HEADS, GROUP_SIZE + 2, HEAD_DIM)
    turned = rotary(qkv_proj[:, :, :GROUP_SIZE + 1], positions)
    query_rot = turned[:, :, :GROUP_SIZE].astype(jnp.bfloat16)
    k_new = turned[:, :, GROUP_SIZE].astype(jnp.bfloat16)
    v_new = qkv_proj[:, :, GROUP_SIZE + 1].astype(jnp.bfloat16)
    hit_mask = (jnp.arange(SEQ_LEN)[None, :] == positions[:, None])[:, :, None, None]
    k_layer = jnp.where(hit_mask, k_new[:, None], k_layer)
    v_layer = jnp.where(hit_mask, v_new[:, None], v_layer)
    attn_out = lax.map(functools.partial(seq_attention, sparse=sparse), (query_rot, k_layer, v_layer, positions))
    attn_proj = jnp.dot(attn_out.reshape(NUM_SEQS, N_HEADS * HEAD_DIM), w_dense, preferred_element_type=jnp.float32)
    residual = (hidden.astype(jnp.float32) + attn_proj + b_dense.astype(jnp.float32)).astype(jnp.bfloat16)
    normed_two = layer_norm(residual, gains[1], shifts[1])
    up_proj = jnp.dot(normed_two, w_up, preferred_element_type=jnp.float32) + b_up.astype(jnp.float32)
    gated = gegelu(up_proj).astype(jnp.bfloat16)
    down_proj = jnp.dot(gated, w_down, preferred_element_type=jnp.float32)
    out_hidden = (residual.astype(jnp.float32) + down_proj + b_down.astype(jnp.float32)).astype(jnp.bfloat16)
    return out_hidden, k_layer, v_layer


def reference(hidden, positions, k_cache, v_cache, ln_gain, ln_bias, w_qkv, b_qkv, w_dense, b_dense, w_up, b_up, w_down, b_down):
    k_layers = []
    v_layers = []
    for layer_idx in range(2):
        params = tuple(arr[layer_idx] for arr in (ln_gain, ln_bias, w_qkv, b_qkv, w_dense, b_dense, w_up, b_up, w_down, b_down))
        hidden, k_layer, v_layer = decoder_layer(hidden, positions, k_cache[layer_idx], v_cache[layer_idx], params, layer_idx == 0)
        k_layers.append(k_layer)
        v_layers.append(v_layer)
    return hidden, jnp.stack(k_layers), jnp.stack(v_layers)
```

```python
import functools

import jax
import jax.numpy as jnp
from jax import lax
from jax.experimental import pallas as pl
from jax.experimental.pallas import tpu as pltpu
from jax.sharding import PartitionSpec as P

BLOCK_SIZE = 64
LOCAL_BLOCKS = 16
VERT_STRIDE = 8
ROPE_THETA = 1000000.0
GELU_LIMIT = 20.0
NORM_EPS = 0.00001
MASKED = -1e30
MESH = pl.DeviceIdType.MESH

NB = 64
D = 3072
HD = 128
KVL = 4
GRP = 3
SLOTS = 64
QW = KVL * (GRP + 2) * HD
QROWS = 16
KCH = 6
KCS = D // KCH
G = 8
NG = NB // G
MSG = GRP * NB + 8
F_LOC = 2048
M_LOC = 1024
NCH = 4
CW = D // NCH
DR = GRP * HD
VMEM_BYTES = 60 * 1024 * 1024

f32 = jnp.float32
bf16 = jnp.bfloat16


def norm_rows(rows, gain, shift):
    mean = jnp.mean(rows, axis=-1, keepdims=True)
    cent = rows - mean
    var = jnp.mean(jnp.square(cent), axis=-1, keepdims=True)
    return (cent * lax.rsqrt(var + NORM_EPS)) * gain + shift


def attn_kernel(layer, pos, x, cos, sin, gain, shift, b_qkv, w_hbm, kc_hbm, vc_hbm, *rest):
    if layer == 1:
        rest = rest[2:]
    (msg, ko_hbm, vo_hbm, w, kbuf, vbuf, u, acc, qs, kns, vns, os, ms, ls, wsem, ksem, vsem, osem) = rest
    sp = lax.axis_index('sp')
    tp = lax.axis_index('tp')
    base = sp * SLOTS

    def w_copy(i):
        return pltpu.make_async_copy(w_hbm.at[layer, pl.ds(i * KCS, KCS), :], w.at[i], wsem.at[i])

    def in_copy(hbm, buf, sem, i):
        return pltpu.make_async_copy(hbm.at[layer, pl.ds(i * G, G)], buf.at[pl.ds(i * G, G)], sem.at[i])

    def out_copy(buf, hbm, j, i):
        return pltpu.make_async_copy(buf.at[pl.ds(i * G, G)], hbm.at[layer, pl.ds(i * G, G)], osem.at[j, i])

    for i in range(KCH):
        w_copy(i).start()
    for i in range(NG):
        in_copy(kc_hbm, kbuf, ksem, i).start()
        in_copy(vc_hbm, vbuf, vsem, i).start()

    g_row = gain[layer, 0:1, :].astype(f32)
    s_row = shift[layer, 0:1, :].astype(f32)
    for i in range(NB // 16):
        rows = x[pl.ds(i * 16, 16), :].astype(f32)
        normed = norm_rows(rows, g_row, s_row).astype(bf16)
        for j in range(KCH):
            u[j, pl.ds(i * 16, 16), :] = normed[:, j * KCS:(j + 1) * KCS]
    acc[...] = jnp.broadcast_to(b_qkv[layer:layer + 1, :].astype(f32), (NB, QW))
    qs[...] = jnp.zeros_like(qs)

    def qkv_step(i, carry):
        w_copy(i).wait()
        acc[...] += jnp.dot(u[i], w[i], preferred_element_type=f32)
        return carry

    lax.fori_loop(0, KCH, qkv_step, 0)

    cos_t = cos[...]
    sin_t = sin[...]
    for c in range(KVL):
        for j in range(GRP + 2):
            col = (c * (GRP + 2) + j) * HD
            tile = acc[:, col:col + HD]
            if j <= GRP:
                tile = tile * cos_t + pltpu.roll(tile, HD // 2, 1) * sin_t
            for i in range(NB // 8):
                part = tile[i * 8:(i + 1) * 8]
                if j < GRP:
                    qs[pl.ds(i * 8 * QROWS + c * GRP + j, 8, stride=QROWS), :] = part
                else:
                    dst = kns if j == GRP else vns
                    dst[pl.ds(i * 64 + c, 8, stride=8), :] = part
                    dst[pl.ds(i * 64 + c + 4, 8, stride=8), :] = part

    row_h = lax.broadcasted_iota(jnp.int32, (QROWS, SLOTS * KVL), 0)
    col_i = lax.broadcasted_iota(jnp.int32, (QROWS, SLOTS * KVL), 1)
    slot_of = jnp.where(row_h // GRP == col_i % KVL, col_i // KVL, 1 << 20)
    head_id = tp * KVL * GRP + row_h
    vertical = (sp + head_id + 1) % VERT_STRIDE == 0
    sub_row = lax.broadcasted_iota(jnp.int32, (16, HD), 0) // KVL

    def attn_step(i, carry):
        in_copy(kc_hbm, kbuf, ksem, i).wait()
        in_copy(vc_hbm, vbuf, vsem, i).wait()
        for bi in range(G):
            b = i * G + bi
            p = pos[b]
            pl_ = p - base
            pc = jnp.clip(pl_, 0, SLOTS - 1)
            hit = jnp.logical_and(pl_ >= 0, pl_ < SLOTS)
            sub = jnp.where(hit, pc % KVL, -1)
            r0 = pl.multiple_of((pc // KVL) * 16, 16)
            put = sub_row == sub
            for buf, new in ((kbuf, kns), (vbuf, vns)):
                new8 = new[pl.ds(pl.multiple_of(b * 8, 8), 8), :]
                new16 = jnp.concatenate([new8, new8], axis=0)
                old = buf[b, pl.ds(r0, 16), :].astype(f32)
                buf[b, pl.ds(r0, 16), :] = jnp.where(put, new16, old).astype(bf16)
            q = qs[pl.ds(pl.multiple_of(b * QROWS, QROWS), QROWS), :].astype(bf16)
            s = lax.dot_general(q, kbuf[b], (((1,), (1,)), ((), ())), preferred_element_type=f32) * (1.0 / HD)
            if layer == 0:
                near = p // BLOCK_SIZE - sp < LOCAL_BLOCKS
                limit = jnp.where(vertical, pl_, jnp.where(near, pl_, -1))
                keep = slot_of <= limit
            else:
                keep = slot_of <= pl_
            s = jnp.where(keep, s, MASKED)
            peak = jnp.max(s, axis=1, keepdims=True)
            wt = jnp.where(keep, jnp.exp(s - peak), 0.0)
            tot = jnp.sum(wt, axis=1, keepdims=True)
            o = jnp.dot(wt.astype(bf16), vbuf[b], preferred_element_type=f32)
            rows = pl.ds(pl.multiple_of(b * QROWS, QROWS), QROWS)
            os[rows, :] = o
            ms[rows, :] = jnp.broadcast_to(peak, (QROWS, HD))
            ls[rows, :] = jnp.broadcast_to(tot, (QROWS, HD))

        @pl.when(i > 0)
        def _():
            out_copy(kbuf, ko_hbm, 0, i - 1).start()
            out_copy(vbuf, vo_hbm, 1, i - 1).start()

        return carry

    lax.fori_loop(0, NG, attn_step, 0)

    lane = lax.broadcasted_iota(jnp.int32, (8, HD), 1)
    for c in range(KVL):
        stat = jnp.zeros((8, HD), f32)
        for g in range(GRP):
            for i in range(NB // 8):
                rows = pl.ds(i * 8 * QROWS + c * GRP + g, 8, stride=QROWS)
                msg[c, pl.ds(g * NB + i * 8, 8), :] = os[rows, :]
                stat = jnp.where(lane == 16 * i + 2 * g, ms[rows, :], stat)
                stat = jnp.where(lane == 16 * i + 2 * g + 1, ls[rows, :], stat)
        msg[c, pl.ds(GRP * NB, 8), :] = stat
    out_copy(kbuf, ko_hbm, 0, NG - 1).start()
    out_copy(vbuf, vo_hbm, 1, NG - 1).start()
    for i in range(NG):
        out_copy(kbuf, ko_hbm, 0, i).wait()
        out_copy(vbuf, vo_hbm, 1, i).wait()


def attn_call(layer, pos, x, cos, sin, gain, shift, b_qkv, w_qkv, k_cache, v_cache, prev):
    vm = pl.BlockSpec(memory_space=pltpu.VMEM)
    hbm = pl.BlockSpec(memory_space=pl.ANY)
    args = [pos, x, cos, sin, gain, shift, b_qkv, w_qkv, k_cache, v_cache]
    specs = [pl.BlockSpec(memory_space=pltpu.SMEM)] + [vm] * 6 + [hbm] * 3
    alias = {}
    if prev is not None:
        args += list(prev)
        specs += [hbm, hbm]
        alias = {10: 1, 11: 2}
    cache = jax.ShapeDtypeStruct(k_cache.shape, bf16)
    return pl.pallas_call(
        functools.partial(attn_kernel, layer),
        out_shape=(jax.ShapeDtypeStruct((KVL, MSG, HD), f32), cache, cache),
        in_specs=specs,
        out_specs=(vm, hbm, hbm),
        scratch_shapes=[
            pltpu.VMEM((KCH, KCS, QW), bf16),
            pltpu.VMEM((NB, SLOTS * KVL, HD), bf16),
            pltpu.VMEM((NB, SLOTS * KVL, HD), bf16),
            pltpu.VMEM((KCH, NB, KCS), bf16),
            pltpu.VMEM((NB, QW), f32),
            pltpu.VMEM((NB * QROWS, HD), f32),
            pltpu.VMEM((NB * 8, HD), f32),
            pltpu.VMEM((NB * 8, HD), f32),
            pltpu.VMEM((NB * QROWS, HD), f32),
            pltpu.VMEM((NB * QROWS, HD), f32),
            pltpu.VMEM((NB * QROWS, HD), f32),
            pltpu.SemaphoreType.DMA((KCH,)),
            pltpu.SemaphoreType.DMA((NG,)),
            pltpu.SemaphoreType.DMA((NG,)),
            pltpu.SemaphoreType.DMA((2, NG)),
        ],
        input_output_aliases=alias,
        compiler_params=pltpu.CompilerParams(vmem_limit_bytes=VMEM_BYTES),
        name=f'attn{layer}',
    )(*args)


def rest_kernel(layer, msg, x, gain, shift, b_dense, b_up, b_down, wd_hbm, wu_hbm, wn_hbm, out,
                wd, wu, wn, got, o_buf, part, pair, rs_out, rs_in, ag, xrow, up, mbuf,
                wsem, a_sem, d_sem, r_sem, g_sem, f_sem):
    dp = lax.axis_index('dp')
    tp = lax.axis_index('tp')
    sp = lax.axis_index('sp')
    core = sp % 2
    cx = sp // 2
    ox = 1 - cx
    oy = 1 - tp
    mate = cx * 2 + 1 - core

    def dev(y, s):
        return (dp, y, s)

    chips = ((cx, tp), (ox, tp), (cx, oy), (ox, oy))

    def row_of(x_, y_, c_):
        return pl.multiple_of(8 * (c_ * 4 + y_ * 2 + x_), 8)

    def load(src, dst, i):
        return pltpu.make_async_copy(src, dst, wsem.at[i])

    wd_copy = load(wd_hbm.at[layer, pl.ds(pl.multiple_of(sp * DR, DR), DR), :], wd, 0)

    def wu_copy(i):
        return load(wu_hbm.at[layer, pl.ds(i * CW, CW), pl.ds(pl.multiple_of(sp * F_LOC, F_LOC), F_LOC)], wu.at[i], 1 + i)

    wn_copy = load(wn_hbm.at[layer, pl.ds(pl.multiple_of(sp * M_LOC, M_LOC), M_LOC), :], wn, 1 + NCH)

    barrier = pltpu.get_barrier_semaphore()
    peers = (dev(tp, mate), dev(tp, ox * 2 + core), dev(tp, ox * 2 + 1 - core), dev(oy, sp), dev(oy, ox * 2 + core))
    for peer in peers:
        pl.semaphore_signal(barrier, inc=1, device_id=peer, device_id_type=MESH)
    wd_copy.start()
    for i in range(NCH):
        wu_copy(i).start()
    wn_copy.start()
    pl.semaphore_wait(barrier, len(peers))

    def remote(src, dst, sems, idx, peer):
        return pltpu.make_async_remote_copy(
            src_ref=src, dst_ref=dst, send_sem=sems.at[(0,) + idx], recv_sem=sems.at[(1,) + idx],
            device_id=peer, device_id_type=MESH)

    homes = (ox * 2 + core, ox * 2 + 1 - core, mate)
    a2a = [remote(msg.at[h], got.at[j], a_sem, (j,), dev(tp, h)) for j, h in enumerate(homes)]
    for copy in a2a:
        copy.start()

    gain1 = gain[layer, 1:2, :].astype(f32)
    shift1 = shift[layer, 1:2, :].astype(f32)
    me = core * 4 + tp * 2 + cx
    two = x[pl.ds(pl.multiple_of(16 * (me // 2), 16), 16), :].astype(f32)
    xrow[...] = jnp.where(me % 2 == 0, two[:8], two[8:])

    for copy in a2a:
        copy.wait_recv()
    for i in range(NB // 8):
        for g in range(GRP):
            at = 16 * i + 2 * g
            peaks, sums = [], []
            for j in range(4):
                src = msg.at[sp] if j == 3 else got.at[j]
                stat = src[pl.ds(GRP * NB, 8), :]
                peaks.append(jnp.broadcast_to(stat[:, at:at + 1], (8, HD)))
                sums.append(jnp.broadcast_to(stat[:, at + 1:at + 2], (8, HD)))
            top = jnp.maximum(jnp.maximum(peaks[0], peaks[1]), jnp.maximum(peaks[2], peaks[3]))
            num = jnp.zeros((8, HD), f32)
            den = jnp.zeros((8, HD), f32)
            for j in range(4):
                src = msg.at[sp] if j == 3 else got.at[j]
                scale = jnp.exp(peaks[j] - top)
                num += src[pl.ds(g * NB + i * 8, 8), :] * scale
                den += sums[j] * scale
            o_buf[pl.ds(i * 8, 8), g * HD:(g + 1) * HD] = num / den
    for copy in a2a:
        copy.wait_send()

    def reduce_scatter(ph, product, finish):
        mine = pl.multiple_of(core * 32, 32)
        theirs = pl.multiple_of((1 - core) * 32, 32)
        first = [remote(part.at[ph, n, pl.ds(theirs, 32), :], pair.at[ph, n], d_sem, (ph, n), dev(tp, mate)) for n in range(NCH)]
        for n in range(NCH):
            part[ph, n] = product(n)
            first[n].start()
        second = []
        for n in range(NCH):
            first[n].wait_recv()
            rs_out[ph, n] = part[ph, n, pl.ds(mine, 32), :] + pair[ph, n]
            for q in (3, 1, 2):
                x_, y_ = chips[q]
                rows = pl.ds(pl.multiple_of(8 * (y_ * 2 + x_), 8), 8)
                copy = remote(rs_out.at[ph, n, rows, :], rs_in.at[ph, q - 1, n], r_sem, (ph, q - 1, n), dev(y_, x_ * 2 + core))
                copy.start()
                second.append(copy)
        for n in range(NCH):
            for copy in second[3 * n:3 * n + 3]:
                copy.wait_recv()
            own = rs_out[ph, n, pl.ds(pl.multiple_of(8 * (tp * 2 + cx), 8), 8), :]
            finish(n, (own + rs_in[ph, 0, n]) + (rs_in[ph, 1, n] + rs_in[ph, 2, n]))
        for copy in first + second:
            copy.wait_send()

    def all_gather(ph, value, use):
        my_rows = pl.ds(row_of(cx, tp, core), 8)
        direct = []
        sends = []
        for n in range(NCH):
            ag[ph, n, my_rows, :] = value(n)
            here = ag.at[ph, n, my_rows, :]
            for q in (3, 1, 2):
                x_, y_ = chips[q]
                copy = remote(here, here, g_sem, (ph, q - 1, n), dev(y_, x_ * 2 + core))
                copy.start()
                direct.append(copy)
            copy = remote(here, here, f_sem, (ph, 0, n), dev(tp, mate))
            copy.start()
            sends.append(copy)
        for n in range(NCH):
            for k, q in enumerate((1, 2, 3)):
                x_, y_ = chips[q]
                rows = pl.ds(row_of(x_, y_, core), 8)
                there = ag.at[ph, n, rows, :]
                remote(there, there, g_sem, (ph, q - 1, n), dev(y_, x_ * 2 + core)).wait_recv()
                copy = remote(there, there, f_sem, (ph, q, n), dev(tp, mate))
                copy.start()
                sends.append(copy)
        for n in range(NCH):
            for q in range(4):
                x_, y_ = chips[q]
                there = ag.at[ph, n, pl.ds(row_of(x_, y_, 1 - core), 8), :]
                remote(there, there, f_sem, (ph, q, n), dev(tp, mate)).wait_recv()
            use(n)
        for copy in direct + sends:
            copy.wait_send()

    wd_copy.wait()
    o = o_buf[...].astype(bf16)

    def take_dense(n, total):
        cols = slice(n * CW, (n + 1) * CW)
        v = xrow[:, cols] + total + b_dense[layer:layer + 1, cols].astype(f32)
        xrow[:, cols] = v.astype(bf16).astype(f32)

    reduce_scatter(0, lambda n: jnp.dot(o, wd[:, n * CW:(n + 1) * CW], preferred_element_type=f32), take_dense)
    normed = norm_rows(xrow[...], gain1, shift1)
    cols_up = pl.ds(pl.multiple_of(sp * F_LOC, F_LOC), F_LOC)
    up[...] = jnp.broadcast_to(b_up[layer:layer + 1, cols_up].astype(f32), (NB, F_LOC))

    def use_up(n):
        wu_copy(n).wait()
        up[...] += jnp.dot(ag[0, n].astype(bf16), wu[n], preferred_element_type=f32)

    all_gather(0, lambda n: normed[:, n * CW:(n + 1) * CW].astype(bf16).astype(f32), use_up)

    pick = (lax.broadcasted_iota(jnp.int32, (256, 128), 0) == 2 * lax.broadcasted_iota(jnp.int32, (256, 128), 1))
    pick = jnp.where(pick, 1.0, 0.0).astype(bf16)
    for k in range(F_LOC // 256):
        a = up[:, k * 256:(k + 1) * 256]
        z = jnp.minimum(a, GELU_LIMIT)
        gate = z * jax.nn.sigmoid(1.702 * z)
        lin = jnp.clip(a, -GELU_LIMIT, GELU_LIMIT) + 1.0
        prod = (gate * pltpu.roll(lin, 255, 1)).astype(bf16)
        mbuf[:, k * 128:(k + 1) * 128] = jnp.dot(prod, pick, preferred_element_type=f32).astype(bf16)
    wn_copy.wait()
    m = mbuf[...]

    def take_down(n, total):
        cols = slice(n * CW, (n + 1) * CW)
        v = xrow[:, cols] + total + b_down[layer:layer + 1, cols].astype(f32)
        xrow[:, cols] = v.astype(bf16).astype(f32)

    reduce_scatter(1, lambda n: jnp.dot(m, wn[:, n * CW:(n + 1) * CW], preferred_element_type=f32), take_down)

    def use_out(n):
        out[:, n * CW:(n + 1) * CW] = ag[1, n].astype(bf16)

    all_gather(1, lambda n: xrow[:, n * CW:(n + 1) * CW], use_out)


def rest_call(layer, msg, x, gain, shift, b_dense, b_up, b_down, w_dense, w_up, w_down):
    vm = pl.BlockSpec(memory_space=pltpu.VMEM)
    hbm = pl.BlockSpec(memory_space=pl.ANY)
    return pl.pallas_call(
        functools.partial(rest_kernel, layer),
        out_shape=jax.ShapeDtypeStruct((NB, D), bf16),
        in_specs=[vm] * 7 + [hbm] * 3,
        out_specs=vm,
        scratch_shapes=[
            pltpu.VMEM((DR, D), bf16),
            pltpu.VMEM((NCH, CW, F_LOC), bf16),
            pltpu.VMEM((M_LOC, D), bf16),
            pltpu.VMEM((3, MSG, HD), f32),
            pltpu.VMEM((NB, DR), f32),
            pltpu.VMEM((2, NCH, NB, CW), f32),
            pltpu.VMEM((2, NCH, 32, CW), f32),
            pltpu.VMEM((2, NCH, 32, CW), f32),
            pltpu.VMEM((2, 3, NCH, 8, CW), f32),
            pltpu.VMEM((2, NCH, NB, CW), f32),
            pltpu.VMEM((8, D), f32),
            pltpu.VMEM((NB, F_LOC), f32),
            pltpu.VMEM((NB, M_LOC), bf16),
            pltpu.SemaphoreType.DMA((2 + NCH,)),
            pltpu.SemaphoreType.DMA((2, 3)),
            pltpu.SemaphoreType.DMA((2, 2, NCH)),
            pltpu.SemaphoreType.DMA((2, 2, 3, NCH)),
            pltpu.SemaphoreType.DMA((2, 2, 3, NCH)),
            pltpu.SemaphoreType.DMA((2, 2, 4, NCH)),
        ],
        compiler_params=pltpu.CompilerParams(vmem_limit_bytes=VMEM_BYTES, collective_id=layer, has_side_effects=True),
        name=f'rest{layer}',
    )(msg, x, gain, shift, b_dense, b_up, b_down, w_dense, w_up, w_down)


def solution(mesh):
    cache_spec = P(None, 'dp', 'sp', 'tp', None)
    in_specs = (P('dp', None), P('dp'), cache_spec, cache_spec, P(), P(), P(None, None, 'tp'), P(None, 'tp'), P(None, 'tp', None), P(), P(None, None, 'tp'), P(None, 'tp'), P(None, 'tp', None), P())
    out_specs = (P('dp', None), cache_spec, cache_spec)

    def device_step(hidden, positions, k_cache, v_cache, ln_gain, ln_bias, w_qkv, b_qkv, w_dense, b_dense, w_up, b_up, w_down, b_down):
        shape = k_cache.shape
        flat = (2, NB, SLOTS * KVL, HD)
        k_cache = k_cache.reshape(flat)
        v_cache = v_cache.reshape(flat)
        half = HD // 2
        inv_freq = ROPE_THETA ** (-jnp.arange(half).astype(f32) * (2.0 / HD))
        angles = positions.astype(f32)[:, None] * inv_freq[None, :]
        cos_part = jnp.cos(angles)
        sin_part = jnp.sin(angles)
        cos = jnp.concatenate([cos_part, cos_part], axis=1)
        sin = jnp.concatenate([-sin_part, sin_part], axis=1)
        caches = None
        for layer in range(2):
            msg, *caches = attn_call(layer, positions, hidden, cos, sin, ln_gain, ln_bias, b_qkv, w_qkv, k_cache, v_cache, caches)
            hidden = rest_call(layer, msg, hidden, ln_gain, ln_bias, b_dense, b_up, b_down, w_dense, w_up, w_down)
        return hidden, caches[0].reshape(shape), caches[1].reshape(shape)

    return jax.shard_map(device_step, mesh=mesh, in_specs=in_specs, out_specs=out_specs, check_vma=False)
```

```python
import functools

import jax
import jax.numpy as jnp
from jax import lax
from jax.experimental import pallas as pl
from jax.experimental.pallas import tpu as pltpu
from jax.sharding import PartitionSpec as P

BLOCK_SIZE = 64
LOCAL_BLOCKS = 16
VERT_STRIDE = 8
ROPE_THETA = 1000000.0
GELU_LIMIT = 20.0
NORM_EPS = 0.00001
MASKED = -1e30
MESH = pl.DeviceIdType.MESH

NB = 64
D = 3072
HD = 128
KVL = 4
GRP = 3
SLOTS = 64
QW = KVL * (GRP + 2) * HD
QROWS = 16
KCH = 6
KCS = D // KCH
G = 8
NG = NB // G
MSG = GRP * NB + 8
F_LOC = 2048
M_LOC = 1024
NCH = 4
CW = D // NCH
DR = GRP * HD
VMEM_BYTES = 40 * 1024 * 1024

f32 = jnp.float32
bf16 = jnp.bfloat16


def norm_rows(rows, gain, shift):
    mean = jnp.mean(rows, axis=-1, keepdims=True)
    cent = rows - mean
    var = jnp.mean(jnp.square(cent), axis=-1, keepdims=True)
    return (cent * lax.rsqrt(var + NORM_EPS)) * gain + shift


def attn_kernel(layer, pos, x, cos, sin, gain, shift, b_qkv, w_hbm, kc_hbm, vc_hbm, *rest):
    if layer == 1:
        rest = rest[2:]
    (msg, ko_hbm, vo_hbm, w, kbuf, vbuf, u, acc, qs, kns, vns, os, ms, ls, wsem, ksem, vsem, osem) = rest
    sp = lax.axis_index('sp')
    tp = lax.axis_index('tp')
    base = sp * SLOTS

    def w_copy(i):
        return pltpu.make_async_copy(w_hbm.at[layer, pl.ds(i * KCS, KCS), :], w.at[i], wsem.at[i])

    def in_copy(hbm, buf, sem, i):
        return pltpu.make_async_copy(hbm.at[layer, pl.ds(i * G, G)], buf.at[pl.ds(i * G, G)], sem.at[i])

    def out_copy(buf, hbm, j, i):
        return pltpu.make_async_copy(buf.at[pl.ds(i * G, G)], hbm.at[layer, pl.ds(i * G, G)], osem.at[j, i])

    for i in range(KCH):
        w_copy(i).start()
    for i in range(NG):
        in_copy(kc_hbm, kbuf, ksem, i).start()
        in_copy(vc_hbm, vbuf, vsem, i).start()

    g_row = gain[layer, 0:1, :].astype(f32)
    s_row = shift[layer, 0:1, :].astype(f32)
    for i in range(NB // 16):
        rows = x[pl.ds(i * 16, 16), :].astype(f32)
        normed = norm_rows(rows, g_row, s_row).astype(bf16)
        for j in range(KCH):
            u[j, pl.ds(i * 16, 16), :] = normed[:, j * KCS:(j + 1) * KCS]
    acc[...] = jnp.broadcast_to(b_qkv[layer:layer + 1, :].astype(f32), (NB, QW))
    qs[...] = jnp.zeros_like(qs)

    def qkv_step(i, carry):
        w_copy(i).wait()
        acc[...] += jnp.dot(u[i], w[i], preferred_element_type=f32)
        return carry

    lax.fori_loop(0, KCH, qkv_step, 0)

    cos_t = cos[...]
    sin_t = sin[...]
    for c in range(KVL):
        for j in range(GRP + 2):
            col = (c * (GRP + 2) + j) * HD
            tile = acc[:, col:col + HD]
            if j <= GRP:
                tile = tile * cos_t + pltpu.roll(tile, HD // 2, 1) * sin_t
            for i in range(NB // 8):
                part = tile[i * 8:(i + 1) * 8]
                if j < GRP:
                    qs[pl.ds(i * 8 * QROWS + c * GRP + j, 8, stride=QROWS), :] = part
                else:
                    dst = kns if j == GRP else vns
                    dst[pl.ds(i * 64 + c, 8, stride=8), :] = part
                    dst[pl.ds(i * 64 + c + 4, 8, stride=8), :] = part

    row_h = lax.broadcasted_iota(jnp.int32, (QROWS, SLOTS * KVL), 0)
    col_i = lax.broadcasted_iota(jnp.int32, (QROWS, SLOTS * KVL), 1)
    slot_of = jnp.where(row_h // GRP == col_i % KVL, col_i // KVL, 1 << 20)
    head_id = tp * KVL * GRP + row_h
    vertical = (sp + head_id + 1) % VERT_STRIDE == 0
    sub_row = lax.broadcasted_iota(jnp.int32, (16, HD), 0) // KVL

    def attn_step(i, carry):
        in_copy(kc_hbm, kbuf, ksem, i).wait()
        in_copy(vc_hbm, vbuf, vsem, i).wait()
        limits = []
        for bi in range(G):
            b = i * G + bi
            p = pos[b]
            pl_ = p - base
            pc = jnp.clip(pl_, 0, SLOTS - 1)
            hit = jnp.logical_and(pl_ >= 0, pl_ < SLOTS)
            sub = jnp.where(hit, pc % KVL, -1)
            r0 = pl.multiple_of((pc // KVL) * 16, 16)
            put = sub_row == sub
            for buf, new in ((kbuf, kns), (vbuf, vns)):
                new8 = new[pl.ds(pl.multiple_of(b * 8, 8), 8), :]
                new16 = jnp.concatenate([new8, new8], axis=0)
                old = buf[b, pl.ds(r0, 16), :].astype(f32)
                buf[b, pl.ds(r0, 16), :] = jnp.where(put, new16, old).astype(bf16)
            if layer == 0:
                near = p // BLOCK_SIZE - sp < LOCAL_BLOCKS
                limits.append(jnp.where(vertical, pl_, jnp.where(near, pl_, -1)))
            else:
                limits.append(pl_)
        scores = []
        for bi in range(G):
            b = i * G + bi
            q = qs[pl.ds(pl.multiple_of(b * QROWS, QROWS), QROWS), :].astype(bf16)
            scores.append(lax.dot_general(q, kbuf[b], (((1,), (1,)), ((), ())), preferred_element_type=f32))
        keeps = [slot_of <= limit for limit in limits]
        scores = [jnp.where(keep, s * (1.0 / HD), MASKED) for keep, s in zip(keeps, scores)]
        peaks = [jnp.max(s, axis=1, keepdims=True) for s in scores]
        weights = [jnp.where(keep, jnp.exp(s - peak), 0.0) for keep, s, peak in zip(keeps, scores, peaks)]
        outs = [jnp.dot(wt.astype(bf16), vbuf[i * G + bi], preferred_element_type=f32) for bi, wt in enumerate(weights)]
        sums = [jnp.sum(wt, axis=1, keepdims=True) for wt in weights]
        for bi in range(G):
            rows = pl.ds(pl.multiple_of((i * G + bi) * QROWS, QROWS), QROWS)
            ms[rows, :] = jnp.broadcast_to(peaks[bi], (QROWS, HD))
            ls[rows, :] = jnp.broadcast_to(sums[bi], (QROWS, HD))
            os[rows, :] = outs[bi]

        @pl.when(i > 0)
        def _():
            out_copy(kbuf, ko_hbm, 0, i - 1).start()
            out_copy(vbuf, vo_hbm, 1, i - 1).start()

        return carry

    lax.fori_loop(0, NG, attn_step, 0)

    lane = lax.broadcasted_iota(jnp.int32, (8, HD), 1)
    for c in range(KVL):
        stat = jnp.zeros((8, HD), f32)
        for g in range(GRP):
            for i in range(NB // 8):
                rows = pl.ds(i * 8 * QROWS + c * GRP + g, 8, stride=QROWS)
                msg[c, pl.ds(g * NB + i * 8, 8), :] = os[rows, :]
                stat = jnp.where(lane == 16 * i + 2 * g, ms[rows, :], stat)
                stat = jnp.where(lane == 16 * i + 2 * g + 1, ls[rows, :], stat)
        msg[c, pl.ds(GRP * NB, 8), :] = stat
    out_copy(kbuf, ko_hbm, 0, NG - 1).start()
    out_copy(vbuf, vo_hbm, 1, NG - 1).start()
    for i in range(NG):
        out_copy(kbuf, ko_hbm, 0, i).wait()
        out_copy(vbuf, vo_hbm, 1, i).wait()


def attn_call(layer, pos, x, cos, sin, gain, shift, b_qkv, w_qkv, k_cache, v_cache, prev):
    vm = pl.BlockSpec(memory_space=pltpu.VMEM)
    hbm = pl.BlockSpec(memory_space=pltpu.HBM)
    args = [pos, x, cos, sin, gain, shift, b_qkv, w_qkv, k_cache, v_cache]
    specs = [pl.BlockSpec(memory_space=pltpu.SMEM)] + [vm] * 6 + [hbm] * 3
    alias = {}
    if prev is not None:
        args += list(prev)
        specs += [hbm, hbm]
        alias = {10: 1, 11: 2}
    cache = jax.ShapeDtypeStruct(k_cache.shape, bf16)
    return pl.pallas_call(
        functools.partial(attn_kernel, layer),
        out_shape=(jax.ShapeDtypeStruct((KVL, MSG, HD), f32), cache, cache),
        in_specs=specs,
        out_specs=(vm, hbm, hbm),
        scratch_shapes=[
            pltpu.VMEM((KCH, KCS, QW), bf16),
            pltpu.VMEM((NB, SLOTS * KVL, HD), bf16),
            pltpu.VMEM((NB, SLOTS * KVL, HD), bf16),
            pltpu.VMEM((KCH, NB, KCS), bf16),
            pltpu.VMEM((NB, QW), f32),
            pltpu.VMEM((NB * QROWS, HD), f32),
            pltpu.VMEM((NB * 8, HD), f32),
            pltpu.VMEM((NB * 8, HD), f32),
            pltpu.VMEM((NB * QROWS, HD), f32),
            pltpu.VMEM((NB * QROWS, HD), f32),
            pltpu.VMEM((NB * QROWS, HD), f32),
            pltpu.SemaphoreType.DMA((KCH,)),
            pltpu.SemaphoreType.DMA((NG,)),
            pltpu.SemaphoreType.DMA((NG,)),
            pltpu.SemaphoreType.DMA((2, NG)),
        ],
        input_output_aliases=alias,
        compiler_params=pltpu.CompilerParams(vmem_limit_bytes=VMEM_BYTES),
        name=f'attn{layer}',
    )(*args)


def rest_kernel(layer, msg, x, gain, shift, b_dense, b_up, b_down, wd_hbm, wu_hbm, wn_hbm, out,
                wd, wu, wn, got, o_buf, part, pair, rs_out, rs_in, ag, xrow, up, mbuf,
                wsem, a_sem, d_sem, r_sem, g_sem, f_sem):
    dp = lax.axis_index('dp')
    tp = lax.axis_index('tp')
    sp = lax.axis_index('sp')
    core = sp % 2
    cx = sp // 2
    ox = 1 - cx
    oy = 1 - tp
    mate = cx * 2 + 1 - core

    def dev(y, s):
        return (dp, y, s)

    chips = ((cx, tp), (ox, tp), (cx, oy), (ox, oy))

    def row_of(x_, y_, c_):
        return pl.multiple_of(8 * (c_ * 4 + y_ * 2 + x_), 8)

    def load(src, dst, i):
        return pltpu.make_async_copy(src, dst, wsem.at[i])

    wd_copy = load(wd_hbm.at[layer, pl.ds(pl.multiple_of(sp * DR, DR), DR), :], wd, 0)

    def wu_copy(i):
        return load(wu_hbm.at[layer, pl.ds(i * CW, CW), pl.ds(pl.multiple_of(sp * F_LOC, F_LOC), F_LOC)], wu.at[i], 1 + i)

    wn_copy = load(wn_hbm.at[layer, pl.ds(pl.multiple_of(sp * M_LOC, M_LOC), M_LOC), :], wn, 1 + NCH)

    barrier = pltpu.get_barrier_semaphore()
    peers = (dev(tp, mate), dev(tp, ox * 2 + core), dev(tp, ox * 2 + 1 - core), dev(oy, sp), dev(oy, ox * 2 + core))
    for peer in peers:
        pl.semaphore_signal(barrier, inc=1, device_id=peer, device_id_type=MESH)
    wd_copy.start()
    for i in range(NCH):
        wu_copy(i).start()
    wn_copy.start()
    pl.semaphore_wait(barrier, len(peers))

    def remote(src, dst, sems, idx, peer):
        return pltpu.make_async_remote_copy(
            src_ref=src, dst_ref=dst, send_sem=sems.at[(0,) + idx], recv_sem=sems.at[(1,) + idx],
            device_id=peer, device_id_type=MESH)

    homes = (ox * 2 + core, ox * 2 + 1 - core, mate)
    a2a = [remote(msg.at[h], got.at[j], a_sem, (j,), dev(tp, h)) for j, h in enumerate(homes)]
    for copy in a2a:
        copy.start()

    gain1 = gain[layer, 1:2, :].astype(f32)
    shift1 = shift[layer, 1:2, :].astype(f32)
    me = core * 4 + tp * 2 + cx
    two = x[pl.ds(pl.multiple_of(16 * (me // 2), 16), 16), :].astype(f32)
    xrow[...] = jnp.where(me % 2 == 0, two[:8], two[8:])

    for copy in a2a:
        copy.wait_recv()
    for i in range(NB // 8):
        for g in range(GRP):
            at = 16 * i + 2 * g
            peaks, sums = [], []
            for j in range(4):
                src = msg.at[sp] if j == 3 else got.at[j]
                stat = src[pl.ds(GRP * NB, 8), :]
                peaks.append(jnp.broadcast_to(stat[:, at:at + 1], (8, HD)))
                sums.append(jnp.broadcast_to(stat[:, at + 1:at + 2], (8, HD)))
            top = jnp.maximum(jnp.maximum(peaks[0], peaks[1]), jnp.maximum(peaks[2], peaks[3]))
            num = jnp.zeros((8, HD), f32)
            den = jnp.zeros((8, HD), f32)
            for j in range(4):
                src = msg.at[sp] if j == 3 else got.at[j]
                scale = jnp.exp(peaks[j] - top)
                num += src[pl.ds(g * NB + i * 8, 8), :] * scale
                den += sums[j] * scale
            o_buf[pl.ds(i * 8, 8), g * HD:(g + 1) * HD] = num / den
    for copy in a2a:
        copy.wait_send()

    def reduce_scatter(ph, product, finish):
        mine = pl.multiple_of(core * 32, 32)
        theirs = pl.multiple_of((1 - core) * 32, 32)
        first = [remote(part.at[ph, n, pl.ds(theirs, 32), :], pair.at[ph, n], d_sem, (ph, n), dev(tp, mate)) for n in range(NCH)]
        for n in range(NCH):
            part[ph, n] = product(n)
            first[n].start()
        second = []
        for n in range(NCH):
            first[n].wait_recv()
            rs_out[ph, n] = part[ph, n, pl.ds(mine, 32), :] + pair[ph, n]
            for q in (3, 1, 2):
                x_, y_ = chips[q]
                rows = pl.ds(pl.multiple_of(8 * (y_ * 2 + x_), 8), 8)
                copy = remote(rs_out.at[ph, n, rows, :], rs_in.at[ph, q - 1, n], r_sem, (ph, q - 1, n), dev(y_, x_ * 2 + core))
                copy.start()
                second.append(copy)
        for n in range(NCH):
            for copy in second[3 * n:3 * n + 3]:
                copy.wait_recv()
            own = rs_out[ph, n, pl.ds(pl.multiple_of(8 * (tp * 2 + cx), 8), 8), :]
            finish(n, (own + rs_in[ph, 0, n]) + (rs_in[ph, 1, n] + rs_in[ph, 2, n]))
        for copy in first + second:
            copy.wait_send()

    def all_gather(ph, value, use):
        my_rows = pl.ds(row_of(cx, tp, core), 8)
        direct = []
        sends = []
        for n in range(NCH):
            ag[ph, n, my_rows, :] = value(n)
            here = ag.at[ph, n, my_rows, :]
            for q in (3, 1, 2):
                x_, y_ = chips[q]
                copy = remote(here, here, g_sem, (ph, q - 1, n), dev(y_, x_ * 2 + core))
                copy.start()
                direct.append(copy)
            copy = remote(here, here, f_sem, (ph, 0, n), dev(tp, mate))
            copy.start()
            sends.append(copy)
        for n in range(NCH):
            for k, q in enumerate((1, 2, 3)):
                x_, y_ = chips[q]
                rows = pl.ds(row_of(x_, y_, core), 8)
                there = ag.at[ph, n, rows, :]
                remote(there, there, g_sem, (ph, q - 1, n), dev(y_, x_ * 2 + core)).wait_recv()
                copy = remote(there, there, f_sem, (ph, q, n), dev(tp, mate))
                copy.start()
                sends.append(copy)
        for n in range(NCH):
            for q in range(4):
                x_, y_ = chips[q]
                there = ag.at[ph, n, pl.ds(row_of(x_, y_, 1 - core), 8), :]
                remote(there, there, f_sem, (ph, q, n), dev(tp, mate)).wait_recv()
            use(n)
        for copy in direct + sends:
            copy.wait_send()

    wd_copy.wait()
    o = o_buf[...].astype(bf16)

    def take_dense(n, total):
        cols = slice(n * CW, (n + 1) * CW)
        v = xrow[:, cols] + total + b_dense[layer:layer + 1, cols].astype(f32)
        xrow[:, cols] = v.astype(bf16).astype(f32)

    reduce_scatter(0, lambda n: jnp.dot(o, wd[:, n * CW:(n + 1) * CW], preferred_element_type=f32), take_dense)
    normed = norm_rows(xrow[...], gain1, shift1)
    cols_up = pl.ds(pl.multiple_of(sp * F_LOC, F_LOC), F_LOC)
    up[...] = jnp.broadcast_to(b_up[layer:layer + 1, cols_up].astype(f32), (NB, F_LOC))

    def use_up(n):
        wu_copy(n).wait()
        up[...] += jnp.dot(ag[0, n].astype(bf16), wu[n], preferred_element_type=f32)

    all_gather(0, lambda n: normed[:, n * CW:(n + 1) * CW].astype(bf16).astype(f32), use_up)

    pick = (lax.broadcasted_iota(jnp.int32, (256, 128), 0) == 2 * lax.broadcasted_iota(jnp.int32, (256, 128), 1))
    pick = jnp.where(pick, 1.0, 0.0).astype(bf16)
    for k in range(F_LOC // 256):
        a = up[:, k * 256:(k + 1) * 256]
        z = jnp.minimum(a, GELU_LIMIT)
        gate = z * jax.nn.sigmoid(1.702 * z)
        lin = jnp.clip(a, -GELU_LIMIT, GELU_LIMIT) + 1.0
        prod = (gate * pltpu.roll(lin, 255, 1)).astype(bf16)
        mbuf[:, k * 128:(k + 1) * 128] = jnp.dot(prod, pick, preferred_element_type=f32).astype(bf16)
    wn_copy.wait()
    m = mbuf[...]

    def take_down(n, total):
        cols = slice(n * CW, (n + 1) * CW)
        v = xrow[:, cols] + total + b_down[layer:layer + 1, cols].astype(f32)
        xrow[:, cols] = v.astype(bf16).astype(f32)

    reduce_scatter(1, lambda n: jnp.dot(m, wn[:, n * CW:(n + 1) * CW], preferred_element_type=f32), take_down)

    def use_out(n):
        out[:, n * CW:(n + 1) * CW] = ag[1, n].astype(bf16)

    all_gather(1, lambda n: xrow[:, n * CW:(n + 1) * CW], use_out)


def rest_call(layer, msg, x, gain, shift, b_dense, b_up, b_down, w_dense, w_up, w_down):
    vm = pl.BlockSpec(memory_space=pltpu.VMEM)
    hbm = pl.BlockSpec(memory_space=pltpu.HBM)
    return pl.pallas_call(
        functools.partial(rest_kernel, layer),
        out_shape=jax.ShapeDtypeStruct((NB, D), bf16),
        in_specs=[vm] * 7 + [hbm] * 3,
        out_specs=vm,
        scratch_shapes=[
            pltpu.VMEM((DR, D), bf16),
            pltpu.VMEM((NCH, CW, F_LOC), bf16),
            pltpu.VMEM((M_LOC, D), bf16),
            pltpu.VMEM((3, MSG, HD), f32),
            pltpu.VMEM((NB, DR), f32),
            pltpu.VMEM((2, NCH, NB, CW), f32),
            pltpu.VMEM((2, NCH, 32, CW), f32),
            pltpu.VMEM((2, NCH, 32, CW), f32),
            pltpu.VMEM((2, 3, NCH, 8, CW), f32),
            pltpu.VMEM((2, NCH, NB, CW), f32),
            pltpu.VMEM((8, D), f32),
            pltpu.VMEM((NB, F_LOC), f32),
            pltpu.VMEM((NB, M_LOC), bf16),
            pltpu.SemaphoreType.DMA((2 + NCH,)),
            pltpu.SemaphoreType.DMA((2, 3)),
            pltpu.SemaphoreType.DMA((2, 2, NCH)),
            pltpu.SemaphoreType.DMA((2, 2, 3, NCH)),
            pltpu.SemaphoreType.DMA((2, 2, 3, NCH)),
            pltpu.SemaphoreType.DMA((2, 2, 4, NCH)),
        ],
        compiler_params=pltpu.CompilerParams(vmem_limit_bytes=VMEM_BYTES, collective_id=layer, has_side_effects=True),
        name=f'rest{layer}',
    )(msg, x, gain, shift, b_dense, b_up, b_down, w_dense, w_up, w_down)


def solution(mesh):
    cache_spec = P(None, 'dp', 'sp', 'tp', None)
    in_specs = (P('dp', None), P('dp'), cache_spec, cache_spec, P(), P(), P(None, None, 'tp'), P(None, 'tp'), P(None, 'tp', None), P(), P(None, None, 'tp'), P(None, 'tp'), P(None, 'tp', None), P())
    out_specs = (P('dp', None), cache_spec, cache_spec)

    def device_step(hidden, positions, k_cache, v_cache, ln_gain, ln_bias, w_qkv, b_qkv, w_dense, b_dense, w_up, b_up, w_down, b_down):
        shape = k_cache.shape
        flat = (2, NB, SLOTS * KVL, HD)
        k_cache = k_cache.reshape(flat)
        v_cache = v_cache.reshape(flat)
        half = HD // 2
        inv_freq = ROPE_THETA ** (-jnp.arange(half).astype(f32) * (2.0 / HD))
        angles = positions.astype(f32)[:, None] * inv_freq[None, :]
        cos_part = jnp.cos(angles)
        sin_part = jnp.sin(angles)
        cos = jnp.concatenate([cos_part, cos_part], axis=1)
        sin = jnp.concatenate([-sin_part, sin_part], axis=1)
        caches = None
        for layer in range(2):
            msg, *caches = attn_call(layer, positions, hidden, cos, sin, ln_gain, ln_bias, b_qkv, w_qkv, k_cache, v_cache, caches)
            hidden = rest_call(layer, msg, hidden, ln_gain, ln_bias, b_dense, b_up, b_down, w_dense, w_up, w_down)
        return hidden, caches[0].reshape(shape), caches[1].reshape(shape)

    return jax.shard_map(device_step, mesh=mesh, in_specs=in_specs, out_specs=out_specs, check_vma=False)
```

```python
import functools

import jax
import jax.numpy as jnp
from jax import lax
from jax.experimental import pallas as pl
from jax.experimental.pallas import tpu as pltpu
from jax.sharding import PartitionSpec as P

BLOCK_SIZE = 64
LOCAL_BLOCKS = 16
VERT_STRIDE = 8
ROPE_THETA = 1000000.0
GELU_LIMIT = 20.0
NORM_EPS = 0.00001
MASKED = -1e30
MESH = pl.DeviceIdType.MESH

NB = 64
D = 3072
HD = 128
KVL = 4
GRP = 3
SLOTS = 64
QW = KVL * (GRP + 2) * HD
QROWS = 16
KCH = 6
KCS = D // KCH
G = 8
NG = NB // G
MSG = GRP * NB + 8
F_LOC = 2048
M_LOC = 1024
NCH = 4
CW = D // NCH
ORDER = (0, 2, 1, 3)
DR = GRP * HD
VMEM_BYTES = 52 * 1024 * 1024

f32 = jnp.float32
bf16 = jnp.bfloat16


def norm_rows(rows, gain, shift):
    mean = jnp.mean(rows, axis=-1, keepdims=True)
    cent = rows - mean
    var = jnp.mean(jnp.square(cent), axis=-1, keepdims=True)
    return (cent * lax.rsqrt(var + NORM_EPS)) * gain + shift


def attn_kernel(layer, pos, x, cos, sin, gain, shift, b_qkv, w_hbm, kc_hbm, vc_hbm, *rest):
    if layer == 1:
        rest = rest[2:]
    (msg, ko_hbm, vo_hbm, w, kbuf, vbuf, u, acc, qs, kns, vns, os, ms, ls, wsem, ksem, vsem, osem) = rest
    sp = lax.axis_index('sp')
    tp = lax.axis_index('tp')
    base = sp * SLOTS

    def w_copy(i):
        return pltpu.make_async_copy(w_hbm.at[layer, pl.ds(i * KCS, KCS), :], w.at[i], wsem.at[i])

    def in_copy(hbm, buf, sem, i):
        return pltpu.make_async_copy(hbm.at[layer, pl.ds(i * G, G)], buf.at[pl.ds(i * G, G)], sem.at[i])

    def out_copy(buf, hbm, j, i):
        return pltpu.make_async_copy(buf.at[pl.ds(i * G, G)], hbm.at[layer, pl.ds(i * G, G)], osem.at[j, i])

    for i in range(KCH):
        w_copy(i).start()
    for i in range(NG):
        in_copy(kc_hbm, kbuf, ksem, i).start()
        in_copy(vc_hbm, vbuf, vsem, i).start()

    g_row = gain[layer, 0:1, :].astype(f32)
    s_row = shift[layer, 0:1, :].astype(f32)
    for i in range(NB // 16):
        rows = x[pl.ds(i * 16, 16), :].astype(f32)
        normed = norm_rows(rows, g_row, s_row).astype(bf16)
        for j in range(KCH):
            u[j, pl.ds(i * 16, 16), :] = normed[:, j * KCS:(j + 1) * KCS]
    acc[...] = jnp.broadcast_to(b_qkv[layer:layer + 1, :].astype(f32), (NB, QW))
    qs[...] = jnp.zeros_like(qs)

    def qkv_step(i, carry):
        w_copy(i).wait()
        acc[...] += jnp.dot(u[i], w[i], preferred_element_type=f32)
        return carry

    lax.fori_loop(0, KCH, qkv_step, 0)

    cos_t = cos[...]
    sin_t = sin[...]
    for c in range(KVL):
        for j in range(GRP + 2):
            col = (c * (GRP + 2) + j) * HD
            tile = acc[:, col:col + HD]
            if j <= GRP:
                tile = tile * cos_t + pltpu.roll(tile, HD // 2, 1) * sin_t
            for i in range(NB // 8):
                part = tile[i * 8:(i + 1) * 8]
                if j < GRP:
                    qs[pl.ds(i * 8 * QROWS + c * GRP + j, 8, stride=QROWS), :] = part
                else:
                    dst = kns if j == GRP else vns
                    dst[pl.ds(i * 64 + c, 8, stride=8), :] = part
                    dst[pl.ds(i * 64 + c + 4, 8, stride=8), :] = part

    row_h = lax.broadcasted_iota(jnp.int32, (QROWS, SLOTS * KVL), 0)
    col_i = lax.broadcasted_iota(jnp.int32, (QROWS, SLOTS * KVL), 1)
    slot_of = jnp.where(row_h // GRP == col_i % KVL, col_i // KVL, 1 << 20)
    head_id = tp * KVL * GRP + row_h
    vertical = (sp + head_id + 1) % VERT_STRIDE == 0
    sub_row = lax.broadcasted_iota(jnp.int32, (16, HD), 0) // KVL

    def attn_step(i, carry):
        in_copy(kc_hbm, kbuf, ksem, i).wait()
        in_copy(vc_hbm, vbuf, vsem, i).wait()
        limits = []
        for bi in range(G):
            b = i * G + bi
            p = pos[b]
            pl_ = p - base
            pc = jnp.clip(pl_, 0, SLOTS - 1)
            hit = jnp.logical_and(pl_ >= 0, pl_ < SLOTS)
            sub = jnp.where(hit, pc % KVL, -1)
            r0 = pl.multiple_of((pc // KVL) * 16, 16)
            put = sub_row == sub
            for buf, new in ((kbuf, kns), (vbuf, vns)):
                new8 = new[pl.ds(pl.multiple_of(b * 8, 8), 8), :]
                new16 = jnp.concatenate([new8, new8], axis=0)
                old = buf[b, pl.ds(r0, 16), :].astype(f32)
                buf[b, pl.ds(r0, 16), :] = jnp.where(put, new16, old).astype(bf16)
            if layer == 0:
                near = p // BLOCK_SIZE - sp < LOCAL_BLOCKS
                limits.append(jnp.where(vertical, pl_, jnp.where(near, pl_, -1)))
            else:
                limits.append(pl_)
        scores = []
        for bi in range(G):
            b = i * G + bi
            q = qs[pl.ds(pl.multiple_of(b * QROWS, QROWS), QROWS), :].astype(bf16)
            scores.append(lax.dot_general(q, kbuf[b], (((1,), (1,)), ((), ())), preferred_element_type=f32))
        keeps = [slot_of <= limit for limit in limits]
        scores = [jnp.where(keep, s * (1.0 / HD), MASKED) for keep, s in zip(keeps, scores)]
        peaks = [jnp.max(s, axis=1, keepdims=True) for s in scores]
        weights = [jnp.where(keep, jnp.exp(s - peak), 0.0) for keep, s, peak in zip(keeps, scores, peaks)]
        outs = [jnp.dot(wt.astype(bf16), vbuf[i * G + bi], preferred_element_type=f32) for bi, wt in enumerate(weights)]
        sums = [jnp.sum(wt, axis=1, keepdims=True) for wt in weights]
        for bi in range(G):
            rows = pl.ds(pl.multiple_of((i * G + bi) * QROWS, QROWS), QROWS)
            ms[rows, :] = jnp.broadcast_to(peaks[bi], (QROWS, HD))
            ls[rows, :] = jnp.broadcast_to(sums[bi], (QROWS, HD))
            os[rows, :] = outs[bi]

        @pl.when(i > 0)
        def _():
            out_copy(kbuf, ko_hbm, 0, i - 1).start()
            out_copy(vbuf, vo_hbm, 1, i - 1).start()

        return carry

    lax.fori_loop(0, NG, attn_step, 0)

    lane = lax.broadcasted_iota(jnp.int32, (8, HD), 1)
    for c in range(KVL):
        stat = jnp.zeros((8, HD), f32)
        for g in range(GRP):
            for i in range(NB // 8):
                rows = pl.ds(i * 8 * QROWS + c * GRP + g, 8, stride=QROWS)
                msg[c, pl.ds(g * NB + i * 8, 8), :] = os[rows, :]
                stat = jnp.where(lane == 16 * i + 2 * g, ms[rows, :], stat)
                stat = jnp.where(lane == 16 * i + 2 * g + 1, ls[rows, :], stat)
        msg[c, pl.ds(GRP * NB, 8), :] = stat
    out_copy(kbuf, ko_hbm, 0, NG - 1).start()
    out_copy(vbuf, vo_hbm, 1, NG - 1).start()
    for i in range(NG):
        out_copy(kbuf, ko_hbm, 0, i).wait()
        out_copy(vbuf, vo_hbm, 1, i).wait()


def attn_call(layer, pos, x, cos, sin, gain, shift, b_qkv, w_qkv, k_cache, v_cache, prev):
    vm = pl.BlockSpec(memory_space=pltpu.VMEM)
    hbm = pl.BlockSpec(memory_space=pltpu.HBM)
    args = [pos, x, cos, sin, gain, shift, b_qkv, w_qkv, k_cache, v_cache]
    specs = [pl.BlockSpec(memory_space=pltpu.SMEM)] + [vm] * 6 + [hbm] * 3
    alias = {}
    if prev is not None:
        args += list(prev)
        specs += [hbm, hbm]
        alias = {10: 1, 11: 2}
    cache = jax.ShapeDtypeStruct(k_cache.shape, bf16)
    return pl.pallas_call(
        functools.partial(attn_kernel, layer),
        out_shape=(jax.ShapeDtypeStruct((KVL, MSG, HD), f32), cache, cache),
        in_specs=specs,
        out_specs=(vm, hbm, hbm),
        scratch_shapes=[
            pltpu.VMEM((KCH, KCS, QW), bf16),
            pltpu.VMEM((NB, SLOTS * KVL, HD), bf16),
            pltpu.VMEM((NB, SLOTS * KVL, HD), bf16),
            pltpu.VMEM((KCH, NB, KCS), bf16),
            pltpu.VMEM((NB, QW), f32),
            pltpu.VMEM((NB * QROWS, HD), f32),
            pltpu.VMEM((NB * 8, HD), f32),
            pltpu.VMEM((NB * 8, HD), f32),
            pltpu.VMEM((NB * QROWS, HD), f32),
            pltpu.VMEM((NB * QROWS, HD), f32),
            pltpu.VMEM((NB * QROWS, HD), f32),
            pltpu.SemaphoreType.DMA((KCH,)),
            pltpu.SemaphoreType.DMA((NG,)),
            pltpu.SemaphoreType.DMA((NG,)),
            pltpu.SemaphoreType.DMA((2, NG)),
        ],
        input_output_aliases=alias,
        compiler_params=pltpu.CompilerParams(vmem_limit_bytes=VMEM_BYTES),
        name=f'attn{layer}',
    )(*args)


def rest_kernel(layer, msg, x, gain, shift, b_dense, b_up, b_down, wd_hbm, wu_hbm, wn_hbm, out,
                wd, wu, wn, got, sent, o_buf, part, pair, rs_out, rs_via, rs_sum, rs_in, ag, xrow, up, mbuf,
                wsem, a_sem, d_sem, r_sem, g_sem, f_sem):
    dp = lax.axis_index('dp')
    tp = lax.axis_index('tp')
    sp = lax.axis_index('sp')
    core = sp % 2
    cx = sp // 2
    ox = 1 - cx
    oy = 1 - tp
    mate = cx * 2 + 1 - core

    def dev(y, s):
        return (dp, y, s)

    chips = ((cx, tp), (ox, tp), (cx, oy), (ox, oy))

    def row_of(x_, y_, c_):
        return pl.multiple_of(8 * (c_ * 4 + y_ * 2 + x_), 8)

    def load(src, dst, i):
        return pltpu.make_async_copy(src, dst, wsem.at[i])

    wd_copy = load(wd_hbm.at[layer, pl.ds(pl.multiple_of(sp * DR, DR), DR), :], wd, 0)

    def wu_copy(i):
        return load(wu_hbm.at[layer, pl.ds(i * CW, CW), pl.ds(pl.multiple_of(sp * F_LOC, F_LOC), F_LOC)], wu.at[i], 1 + i)

    wn_copy = load(wn_hbm.at[layer, pl.ds(pl.multiple_of(sp * M_LOC, M_LOC), M_LOC), :], wn, 1 + NCH)

    barrier = pltpu.get_barrier_semaphore()
    peers = (dev(tp, mate), dev(tp, ox * 2 + core), dev(oy, sp), dev(oy, ox * 2 + core))
    for peer in peers:
        pl.semaphore_signal(barrier, inc=1, device_id=peer, device_id_type=MESH)
    wd_copy.start()
    for i in range(NCH):
        wu_copy(i).start()
    wn_copy.start()
    pl.semaphore_wait(barrier, len(peers))

    def remote(src, dst, sems, idx, peer):
        return pltpu.make_async_remote_copy(
            src_ref=src, dst_ref=dst, send_sem=sems.at[(0,) + idx], recv_sem=sems.at[(1,) + idx],
            device_id=peer, device_id_type=MESH)

    mine_h = cx * 2 + core
    far_h = ox * 2 + core
    swap = [remote(msg.at[ox * 2 + 1 - core], got.at[0], a_sem, (0,), dev(tp, mate)),
            remote(msg.at[mate], got.at[1], a_sem, (1,), dev(tp, mate))]
    for copy in swap:
        copy.start()

    gain1 = gain[layer, 1:2, :].astype(f32)
    shift1 = shift[layer, 1:2, :].astype(f32)
    me = core * 4 + tp * 2 + cx
    two = x[pl.ds(pl.multiple_of(16 * (me // 2), 16), 16), :].astype(f32)
    xrow[...] = jnp.where(me % 2 == 0, two[:8], two[8:])

    lane = lax.broadcasted_iota(jnp.int32, (8, HD), 1)

    def merge(one, two, put, stat_out=None):
        stats = [ref[pl.ds(GRP * NB, 8), :] for ref in (one, two)]
        new_stat = jnp.zeros((8, HD), f32)
        for i in range(NB // 8):
            for g in range(GRP):
                at = 16 * i + 2 * g
                peaks = [jnp.broadcast_to(st[:, at:at + 1], (8, HD)) for st in stats]
                sums = [jnp.broadcast_to(st[:, at + 1:at + 2], (8, HD)) for st in stats]
                top = jnp.maximum(peaks[0], peaks[1])
                scale = [jnp.exp(p - top) for p in peaks]
                rows = pl.ds(g * NB + i * 8, 8)
                num = one[rows, :] * scale[0] + two[rows, :] * scale[1]
                den = sums[0] * scale[0] + sums[1] * scale[1]
                put(i, g, num, den)
                if stat_out is not None:
                    new_stat = jnp.where(lane == at, top, new_stat)
                    new_stat = jnp.where(lane == at + 1, den, new_stat)
        if stat_out is not None:
            stat_out[pl.ds(GRP * NB, 8), :] = new_stat

    def put_part(ref):
        def put(i, g, num, den):
            ref[pl.ds(g * NB + i * 8, 8), :] = num
        return put

    def put_out(i, g, num, den):
        o_buf[pl.ds(i * 8, 8), g * HD:(g + 1) * HD] = num / den

    swap[0].wait_recv()
    merge(msg.at[far_h], got.at[0], put_part(sent.at[0]), sent.at[0])
    cross = remote(sent.at[0], got.at[2], a_sem, (2,), dev(tp, far_h))
    cross.start()
    swap[1].wait_recv()
    merge(msg.at[mine_h], got.at[1], put_part(sent.at[1]), sent.at[1])
    cross.wait_recv()
    merge(sent.at[1], got.at[2], put_out)
    for copy in swap + [cross]:
        copy.wait_send()

    def reduce_scatter(ph, product, finish):
        mine = pl.multiple_of(core * 32, 32)
        theirs = pl.multiple_of((1 - core) * 32, 32)
        first = [remote(part.at[ph, n, pl.ds(theirs, 32), :], pair.at[ph, n], d_sem, (ph, n), dev(tp, mate)) for n in range(NCH)]
        for n in ORDER:
            part[ph, n] = product(n)
            first[n].start()
        d_rows, x_rows, y_rows = (pl.ds(pl.multiple_of(8 * (y_ * 2 + x_), 8), 8) for x_, y_ in (chips[3], chips[1], chips[2]))
        x_dev, y_dev = dev(tp, far_h), dev(oy, sp)
        relay, plain, merged = {}, {}, {}
        for n in ORDER:
            first[n].wait_recv()
            rs_out[ph, n] = part[ph, n, pl.ds(mine, 32), :] + pair[ph, n]
            relay[n] = remote(rs_out.at[ph, n, d_rows, :], rs_via.at[ph, n], r_sem, (ph, 0, n), x_dev if n < NCH // 2 else y_dev)
            relay[n].start()
        for n in ORDER:
            rows, peer = (x_rows, x_dev) if n < NCH // 2 else (y_rows, y_dev)
            plain[n] = remote(rs_out.at[ph, n, rows, :], rs_in.at[ph, 0, n], r_sem, (ph, 1, n), peer)
            plain[n].start()
        for n in ORDER:
            rows, peer = (y_rows, y_dev) if n < NCH // 2 else (x_rows, x_dev)
            relay[n].wait_recv()
            rs_sum[ph, n] = rs_out[ph, n, rows, :] + rs_via[ph, n]
            merged[n] = remote(rs_sum.at[ph, n], rs_in.at[ph, 1, n], r_sem, (ph, 2, n), peer)
            merged[n].start()
        for n in ORDER:
            plain[n].wait_recv()
            merged[n].wait_recv()
            own = rs_out[ph, n, pl.ds(pl.multiple_of(8 * (tp * 2 + cx), 8), 8), :]
            finish(n, own + rs_in[ph, 0, n] + rs_in[ph, 1, n])
        for copy in first + list(relay.values()) + list(plain.values()) + list(merged.values()):
            copy.wait_send()

    def all_gather(ph, value, use):
        my_rows = pl.ds(row_of(cx, tp, core), 8)
        direct = []
        sends = []
        for n in range(NCH):
            ag[ph, n, my_rows, :] = value(n)
            here = ag.at[ph, n, my_rows, :]
            for q in (3, 1, 2):
                x_, y_ = chips[q]
                copy = remote(here, here, g_sem, (ph, q - 1, n), dev(y_, x_ * 2 + core))
                copy.start()
                direct.append(copy)
            copy = remote(here, here, f_sem, (ph, 0, n), dev(tp, mate))
            copy.start()
            sends.append(copy)
        def finish(n):
            for q in range(4):
                x_, y_ = chips[q]
                there = ag.at[ph, n, pl.ds(row_of(x_, y_, 1 - core), 8), :]
                remote(there, there, f_sem, (ph, q, n), dev(tp, mate)).wait_recv()
            use(n)

        for n in range(NCH):
            for q in (1, 2, 3):
                x_, y_ = chips[q]
                rows = pl.ds(row_of(x_, y_, core), 8)
                there = ag.at[ph, n, rows, :]
                remote(there, there, g_sem, (ph, q - 1, n), dev(y_, x_ * 2 + core)).wait_recv()
                copy = remote(there, there, f_sem, (ph, q, n), dev(tp, mate))
                copy.start()
                sends.append(copy)
            if n > 0:
                finish(n - 1)
        finish(NCH - 1)
        for copy in direct + sends:
            copy.wait_send()

    wd_copy.wait()
    o = o_buf[...].astype(bf16)

    def take_dense(n, total):
        cols = slice(n * CW, (n + 1) * CW)
        v = xrow[:, cols] + total + b_dense[layer:layer + 1, cols].astype(f32)
        xrow[:, cols] = v.astype(bf16).astype(f32)

    reduce_scatter(0, lambda n: jnp.dot(o, wd[:, n * CW:(n + 1) * CW], preferred_element_type=f32), take_dense)
    normed = norm_rows(xrow[...], gain1, shift1)
    cols_up = pl.ds(pl.multiple_of(sp * F_LOC, F_LOC), F_LOC)
    up[...] = jnp.broadcast_to(b_up[layer:layer + 1, cols_up].astype(f32), (NB, F_LOC))

    def use_up(n):
        wu_copy(n).wait()
        up[...] += jnp.dot(ag[0, n].astype(bf16), wu[n], preferred_element_type=f32)

    all_gather(0, lambda n: normed[:, n * CW:(n + 1) * CW].astype(bf16).astype(f32), use_up)

    pick = (lax.broadcasted_iota(jnp.int32, (256, 128), 0) == 2 * lax.broadcasted_iota(jnp.int32, (256, 128), 1))
    pick = jnp.where(pick, 1.0, 0.0).astype(bf16)
    for k in range(F_LOC // 256):
        a = up[:, k * 256:(k + 1) * 256]
        z = jnp.minimum(a, GELU_LIMIT)
        gate = z * jax.nn.sigmoid(1.702 * z)
        lin = jnp.clip(a, -GELU_LIMIT, GELU_LIMIT) + 1.0
        prod = (gate * pltpu.roll(lin, 255, 1)).astype(bf16)
        mbuf[:, k * 128:(k + 1) * 128] = jnp.dot(prod, pick, preferred_element_type=f32).astype(bf16)
    wn_copy.wait()
    m = mbuf[...]

    def take_down(n, total):
        cols = slice(n * CW, (n + 1) * CW)
        v = xrow[:, cols] + total + b_down[layer:layer + 1, cols].astype(f32)
        xrow[:, cols] = v.astype(bf16).astype(f32)

    reduce_scatter(1, lambda n: jnp.dot(m, wn[:, n * CW:(n + 1) * CW], preferred_element_type=f32), take_down)

    def use_out(n):
        out[:, n * CW:(n + 1) * CW] = ag[1, n].astype(bf16)

    all_gather(1, lambda n: xrow[:, n * CW:(n + 1) * CW], use_out)


def rest_call(layer, msg, x, gain, shift, b_dense, b_up, b_down, w_dense, w_up, w_down):
    vm = pl.BlockSpec(memory_space=pltpu.VMEM)
    hbm = pl.BlockSpec(memory_space=pltpu.HBM)
    return pl.pallas_call(
        functools.partial(rest_kernel, layer),
        out_shape=jax.ShapeDtypeStruct((NB, D), bf16),
        in_specs=[vm] * 7 + [hbm] * 3,
        out_specs=vm,
        scratch_shapes=[
            pltpu.VMEM((DR, D), bf16),
            pltpu.VMEM((NCH, CW, F_LOC), bf16),
            pltpu.VMEM((M_LOC, D), bf16),
            pltpu.VMEM((3, MSG, HD), f32),
            pltpu.VMEM((2, MSG, HD), f32),
            pltpu.VMEM((NB, DR), f32),
            pltpu.VMEM((2, NCH, NB, CW), f32),
            pltpu.VMEM((2, NCH, 32, CW), f32),
            pltpu.VMEM((2, NCH, 32, CW), f32),
            pltpu.VMEM((2, NCH, 8, CW), f32),
            pltpu.VMEM((2, NCH, 8, CW), f32),
            pltpu.VMEM((2, 2, NCH, 8, CW), f32),
            pltpu.VMEM((2, NCH, NB, CW), f32),
            pltpu.VMEM((8, D), f32),
            pltpu.VMEM((NB, F_LOC), f32),
            pltpu.VMEM((NB, M_LOC), bf16),
            pltpu.SemaphoreType.DMA((2 + NCH,)),
            pltpu.SemaphoreType.DMA((2, 3)),
            pltpu.SemaphoreType.DMA((2, 2, NCH)),
            pltpu.SemaphoreType.DMA((2, 2, 3, NCH)),
            pltpu.SemaphoreType.DMA((2, 2, 3, NCH)),
            pltpu.SemaphoreType.DMA((2, 2, 4, NCH)),
        ],
        compiler_params=pltpu.CompilerParams(vmem_limit_bytes=VMEM_BYTES, collective_id=layer, has_side_effects=True),
        name=f'rest{layer}',
    )(msg, x, gain, shift, b_dense, b_up, b_down, w_dense, w_up, w_down)


def solution(mesh):
    cache_spec = P(None, 'dp', 'sp', 'tp', None)
    in_specs = (P('dp', None), P('dp'), cache_spec, cache_spec, P(), P(), P(None, None, 'tp'), P(None, 'tp'), P(None, 'tp', None), P(), P(None, None, 'tp'), P(None, 'tp'), P(None, 'tp', None), P())
    out_specs = (P('dp', None), cache_spec, cache_spec)

    def device_step(hidden, positions, k_cache, v_cache, ln_gain, ln_bias, w_qkv, b_qkv, w_dense, b_dense, w_up, b_up, w_down, b_down):
        shape = k_cache.shape
        flat = (2, NB, SLOTS * KVL, HD)
        k_cache = k_cache.reshape(flat)
        v_cache = v_cache.reshape(flat)
        half = HD // 2
        inv_freq = ROPE_THETA ** (-jnp.arange(half).astype(f32) * (2.0 / HD))
        angles = positions.astype(f32)[:, None] * inv_freq[None, :]
        cos_part = jnp.cos(angles)
        sin_part = jnp.sin(angles)
        cos = jnp.concatenate([cos_part, cos_part], axis=1)
        sin = jnp.concatenate([-sin_part, sin_part], axis=1)
        caches = None
        for layer in range(2):
            msg, *caches = attn_call(layer, positions, hidden, cos, sin, ln_gain, ln_bias, b_qkv, w_qkv, k_cache, v_cache, caches)
            hidden = rest_call(layer, msg, hidden, ln_gain, ln_bias, b_dense, b_up, b_down, w_dense, w_up, w_down)
        return hidden, caches[0].reshape(shape), caches[1].reshape(shape)

    return jax.shard_map(device_step, mesh=mesh, in_specs=in_specs, out_specs=out_specs, check_vma=False)
```

```python
import functools

import jax
import jax.numpy as jnp
from jax import lax
from jax.experimental import pallas as pl
from jax.experimental.pallas import tpu as pltpu
from jax.sharding import PartitionSpec as P

BLOCK_SIZE = 64
LOCAL_BLOCKS = 16
VERT_STRIDE = 8
ROPE_THETA = 1000000.0
GELU_LIMIT = 20.0
NORM_EPS = 0.00001
MASKED = -1e30
MESH = pl.DeviceIdType.MESH

NB = 64
D = 3072
HD = 128
KVL = 4
GRP = 3
SLOTS = 64
QW = KVL * (GRP + 2) * HD
QROWS = 16
KCH = 6
KCS = D // KCH
G = 8
NG = NB // G
HALF = NB // 2
HPC = 6
MSG = HPC * HALF + 8
ROWS = HALF // 2
F_LOC = 4096
M_LOC = F_LOC // 2
NCH = 4
CW = D // NCH
DR = HPC * HD
LAG = 2
VMEM_BYTES = 52 * 1024 * 1024

f32 = jnp.float32
bf16 = jnp.bfloat16


def norm_rows(rows, gain, shift):
    mean = jnp.mean(rows, axis=-1, keepdims=True)
    cent = rows - mean
    var = jnp.mean(jnp.square(cent), axis=-1, keepdims=True)
    return (cent * lax.rsqrt(var + NORM_EPS)) * gain + shift


def attn_kernel(layer, pos, x, cos, sin, gain, shift, b_qkv, w_hbm, kc_hbm, vc_hbm, *rest):
    if layer == 1:
        rest = rest[2:]
    (msg, ko_hbm, vo_hbm, w, kbuf, vbuf, u, acc, qs, kns, vns, os, ms, ls, wsem, ksem, vsem, osem) = rest
    sp = lax.axis_index('sp')
    tp = lax.axis_index('tp')
    base = sp * SLOTS

    def w_copy(i):
        return pltpu.make_async_copy(w_hbm.at[layer, pl.ds(i * KCS, KCS), :], w.at[i], wsem.at[i])

    def in_copy(hbm, buf, sem, i):
        return pltpu.make_async_copy(hbm.at[layer, pl.ds(i * G, G)], buf.at[pl.ds(i * G, G)], sem.at[i])

    def out_copy(buf, hbm, j, i):
        return pltpu.make_async_copy(buf.at[pl.ds(i * G, G)], hbm.at[layer, pl.ds(i * G, G)], osem.at[j, i])

    for i in range(KCH):
        w_copy(i).start()
    for i in range(NG):
        in_copy(kc_hbm, kbuf, ksem, i).start()
        in_copy(vc_hbm, vbuf, vsem, i).start()

    g_row = gain[layer, 0:1, :].astype(f32)
    s_row = shift[layer, 0:1, :].astype(f32)
    for i in range(NB // 16):
        rows = x[pl.ds(i * 16, 16), :].astype(f32)
        normed = norm_rows(rows, g_row, s_row).astype(bf16)
        for j in range(KCH):
            u[j, pl.ds(i * 16, 16), :] = normed[:, j * KCS:(j + 1) * KCS]
    acc[...] = jnp.broadcast_to(b_qkv[layer:layer + 1, :].astype(f32), (NB, QW))
    qs[...] = jnp.zeros_like(qs)

    def qkv_step(i, carry):
        w_copy(i).wait()
        acc[...] += jnp.dot(u[i], w[i], preferred_element_type=f32)
        return carry

    lax.fori_loop(0, KCH, qkv_step, 0)

    cos_t = cos[...]
    sin_t = sin[...]
    for c in range(KVL):
        for j in range(GRP + 2):
            col = (c * (GRP + 2) + j) * HD
            tile = acc[:, col:col + HD]
            if j <= GRP:
                tile = tile * cos_t + pltpu.roll(tile, HD // 2, 1) * sin_t
            for i in range(NB // 8):
                part = tile[i * 8:(i + 1) * 8]
                if j < GRP:
                    qs[pl.ds(i * 8 * QROWS + c * GRP + j, 8, stride=QROWS), :] = part
                else:
                    dst = kns if j == GRP else vns
                    dst[pl.ds(i * 64 + c, 8, stride=8), :] = part
                    dst[pl.ds(i * 64 + c + 4, 8, stride=8), :] = part

    row_h = lax.broadcasted_iota(jnp.int32, (QROWS, SLOTS * KVL), 0)
    col_i = lax.broadcasted_iota(jnp.int32, (QROWS, SLOTS * KVL), 1)
    slot_of = jnp.where(row_h // GRP == col_i % KVL, col_i // KVL, 1 << 20)
    head_id = tp * KVL * GRP + row_h
    vertical = (sp + head_id + 1) % VERT_STRIDE == 0
    sub_row = lax.broadcasted_iota(jnp.int32, (16, HD), 0) // KVL

    def attn_step(i, carry):
        in_copy(kc_hbm, kbuf, ksem, i).wait()
        in_copy(vc_hbm, vbuf, vsem, i).wait()
        limits = []
        for bi in range(G):
            b = i * G + bi
            p = pos[b]
            pl_ = p - base
            pc = jnp.clip(pl_, 0, SLOTS - 1)
            hit = jnp.logical_and(pl_ >= 0, pl_ < SLOTS)
            sub = jnp.where(hit, pc % KVL, -1)
            r0 = pl.multiple_of((pc // KVL) * 16, 16)
            put = sub_row == sub
            for buf, new in ((kbuf, kns), (vbuf, vns)):
                new8 = new[pl.ds(pl.multiple_of(b * 8, 8), 8), :]
                new16 = jnp.concatenate([new8, new8], axis=0)
                old = buf[b, pl.ds(r0, 16), :].astype(f32)
                buf[b, pl.ds(r0, 16), :] = jnp.where(put, new16, old).astype(bf16)
            if layer == 0:
                near = p // BLOCK_SIZE - sp < LOCAL_BLOCKS
                limits.append(jnp.where(vertical, pl_, jnp.where(near, pl_, -1)))
            else:
                limits.append(pl_)
        scores = []
        for bi in range(G):
            b = i * G + bi
            q = qs[pl.ds(pl.multiple_of(b * QROWS, QROWS), QROWS), :].astype(bf16)
            scores.append(lax.dot_general(q, kbuf[b], (((1,), (1,)), ((), ())), preferred_element_type=f32))
        keeps = [slot_of <= limit for limit in limits]
        scores = [jnp.where(keep, s * (1.0 / HD), MASKED) for keep, s in zip(keeps, scores)]
        peaks = [jnp.max(s, axis=1, keepdims=True) for s in scores]
        weights = [jnp.where(keep, jnp.exp(s - peak), 0.0) for keep, s, peak in zip(keeps, scores, peaks)]
        outs = [jnp.dot(wt.astype(bf16), vbuf[i * G + bi], preferred_element_type=f32) for bi, wt in enumerate(weights)]
        sums = [jnp.sum(wt, axis=1, keepdims=True) for wt in weights]
        for bi in range(G):
            rows = pl.ds(pl.multiple_of((i * G + bi) * QROWS, QROWS), QROWS)
            ms[rows, :] = jnp.broadcast_to(peaks[bi], (QROWS, HD))
            ls[rows, :] = jnp.broadcast_to(sums[bi], (QROWS, HD))
            os[rows, :] = outs[bi]

        @pl.when(i > 0)
        def _():
            out_copy(kbuf, ko_hbm, 0, i - 1).start()
            out_copy(vbuf, vo_hbm, 1, i - 1).start()

        return carry

    lax.fori_loop(0, NG, attn_step, 0)

    lane = lax.broadcasted_iota(jnp.int32, (8, HD), 1)
    for half in range(2):
        for c in range(2):
            stat = jnp.zeros((8, HD), f32)
            for g in range(HPC):
                for i in range(HALF // 8):
                    rows = pl.ds((half * HALF + i * 8) * QROWS + c * HPC + g, 8, stride=QROWS)
                    at = 2 * (g * (HALF // 8) + i)
                    msg[half * 2 + c, pl.ds(g * HALF + i * 8, 8), :] = os[rows, :]
                    stat = jnp.where(lane == at, ms[rows, :], stat)
                    stat = jnp.where(lane == at + 1, ls[rows, :], stat)
            msg[half * 2 + c, pl.ds(HPC * HALF, 8), :] = stat
    out_copy(kbuf, ko_hbm, 0, NG - 1).start()
    out_copy(vbuf, vo_hbm, 1, NG - 1).start()
    for i in range(NG):
        out_copy(kbuf, ko_hbm, 0, i).wait()
        out_copy(vbuf, vo_hbm, 1, i).wait()


def attn_call(layer, pos, x, cos, sin, gain, shift, b_qkv, w_qkv, k_cache, v_cache, prev):
    vm = pl.BlockSpec(memory_space=pltpu.VMEM)
    hbm = pl.BlockSpec(memory_space=pltpu.HBM)
    args = [pos, x, cos, sin, gain, shift, b_qkv, w_qkv, k_cache, v_cache]
    specs = [pl.BlockSpec(memory_space=pltpu.SMEM)] + [vm] * 6 + [hbm] * 3
    alias = {}
    if prev is not None:
        args += list(prev)
        specs += [hbm, hbm]
        alias = {10: 1, 11: 2}
    cache = jax.ShapeDtypeStruct(k_cache.shape, bf16)
    return pl.pallas_call(
        functools.partial(attn_kernel, layer),
        out_shape=(jax.ShapeDtypeStruct((KVL, MSG, HD), f32), cache, cache),
        in_specs=specs,
        out_specs=(vm, hbm, hbm),
        scratch_shapes=[
            pltpu.VMEM((KCH, KCS, QW), bf16),
            pltpu.VMEM((NB, SLOTS * KVL, HD), bf16),
            pltpu.VMEM((NB, SLOTS * KVL, HD), bf16),
            pltpu.VMEM((KCH, NB, KCS), bf16),
            pltpu.VMEM((NB, QW), f32),
            pltpu.VMEM((NB * QROWS, HD), f32),
            pltpu.VMEM((NB * 8, HD), f32),
            pltpu.VMEM((NB * 8, HD), f32),
            pltpu.VMEM((NB * QROWS, HD), f32),
            pltpu.VMEM((NB * QROWS, HD), f32),
            pltpu.VMEM((NB * QROWS, HD), f32),
            pltpu.SemaphoreType.DMA((KCH,)),
            pltpu.SemaphoreType.DMA((NG,)),
            pltpu.SemaphoreType.DMA((NG,)),
            pltpu.SemaphoreType.DMA((2, NG)),
        ],
        input_output_aliases=alias,
        compiler_params=pltpu.CompilerParams(vmem_limit_bytes=VMEM_BYTES),
        name=f'attn{layer}',
    )(*args)


def rest_kernel(layer, msg, x, gain, shift, b_dense, b_up, b_down, wd_hbm, wu_hbm, wn_hbm, out,
                wd, wu, wn, got, sent, o_buf, part, pair, sums, other, ag, full, xrow, up, mbuf,
                wsem, a_sem, d_sem, y_sem, g_sem, x_sem):
    dp = lax.axis_index('dp')
    tp = lax.axis_index('tp')
    sp = lax.axis_index('sp')
    core = sp % 2
    cx = sp // 2
    ox = 1 - cx
    mate = (dp, tp, cx * 2 + 1 - core)
    x_dev = (dp, tp, ox * 2 + core)
    y_dev = (dp, 1 - tp, sp)

    def load(src, dst, i):
        return pltpu.make_async_copy(src, dst, wsem.at[i])

    wd_copy = load(wd_hbm.at[layer, pl.ds(pl.multiple_of(core * DR, DR), DR), :], wd, 0)

    def wu_copy(i):
        return load(wu_hbm.at[layer, pl.ds(i * CW, CW), pl.ds(pl.multiple_of(core * F_LOC, F_LOC), F_LOC)], wu.at[i], 1 + i)

    wn_copy = load(wn_hbm.at[layer, pl.ds(pl.multiple_of(core * M_LOC, M_LOC), M_LOC), :], wn, 1 + NCH)

    barrier = pltpu.get_barrier_semaphore()
    for peer in (mate, x_dev, y_dev):
        pl.semaphore_signal(barrier, inc=1, device_id=peer, device_id_type=MESH)
    wd_copy.start()
    for i in range(NCH):
        wu_copy(i).start()
    wn_copy.start()
    pl.semaphore_wait(barrier, 3)

    def remote(src, dst, sems, idx, peer):
        return pltpu.make_async_remote_copy(
            src_ref=src, dst_ref=dst, send_sem=sems.at[(0,) + idx], recv_sem=sems.at[(1,) + idx],
            device_id=peer, device_id_type=MESH)

    near = cx * 2 + core
    far = ox * 2 + core
    swap = [remote(msg.at[ox * 2 + 1 - core], got.at[0], a_sem, (0,), mate),
            remote(msg.at[cx * 2 + 1 - core], got.at[1], a_sem, (1,), mate)]
    for copy in swap:
        copy.start()

    gain1 = gain[layer, 1:2, :].astype(f32)
    shift1 = shift[layer, 1:2, :].astype(f32)
    own = pl.ds(pl.multiple_of(core * ROWS, ROWS), ROWS)
    theirs = pl.ds(pl.multiple_of((1 - core) * ROWS, ROWS), ROWS)

    def all_rows(x_, c_):
        return pl.ds(pl.multiple_of(x_ * HALF + c_ * ROWS, ROWS), ROWS)

    xrow[...] = x[all_rows(cx, core), :].astype(f32)
    lane = lax.broadcasted_iota(jnp.int32, (8, HD), 1)

    def merge(one, two, put, stat_out=None):
        stats = [ref[pl.ds(HPC * HALF, 8), :] for ref in (one, two)]
        new_stat = jnp.zeros((8, HD), f32)
        for g in range(HPC):
            for i in range(HALF // 8):
                at = 2 * (g * (HALF // 8) + i)
                peaks = [jnp.broadcast_to(st[:, at:at + 1], (8, HD)) for st in stats]
                tots = [jnp.broadcast_to(st[:, at + 1:at + 2], (8, HD)) for st in stats]
                top = jnp.maximum(peaks[0], peaks[1])
                scale = [jnp.exp(p - top) for p in peaks]
                rows = pl.ds(g * HALF + i * 8, 8)
                num = one[rows, :] * scale[0] + two[rows, :] * scale[1]
                den = tots[0] * scale[0] + tots[1] * scale[1]
                put(g, i, num, den)
                if stat_out is not None:
                    new_stat = jnp.where(lane == at, top, new_stat)
                    new_stat = jnp.where(lane == at + 1, den, new_stat)
        if stat_out is not None:
            stat_out[pl.ds(HPC * HALF, 8), :] = new_stat

    def put_part(ref):
        def put(g, i, num, den):
            ref[pl.ds(g * HALF + i * 8, 8), :] = num
        return put

    def put_out(g, i, num, den):
        o_buf[pl.ds(i * 8, 8), g * HD:(g + 1) * HD] = num / den

    swap[0].wait_recv()
    merge(msg.at[far], got.at[0], put_part(sent.at[0]), sent.at[0])
    cross = remote(sent.at[0], got.at[2], a_sem, (2,), x_dev)
    cross.start()
    swap[1].wait_recv()
    merge(msg.at[near], got.at[1], put_part(sent.at[1]), sent.at[1])
    cross.wait_recv()
    merge(sent.at[1], got.at[2], put_out)
    for copy in swap + [cross]:
        copy.wait_send()

    def reduce(ph, product, finish):
        first = [remote(part.at[ph, n, theirs, :], pair.at[ph, n], d_sem, (ph, n), mate) for n in range(NCH)]
        second = [remote(sums.at[ph, n], other.at[ph, n], y_sem, (ph, n), y_dev) for n in range(NCH)]
        for step in range(NCH + LAG):
            if step < NCH:
                part[ph, step] = product(step)
                first[step].start()
            if step >= LAG:
                n = step - LAG
                first[n].wait_recv()
                sums[ph, n] = part[ph, n, own, :] + pair[ph, n]
                second[n].start()
        for n in range(NCH):
            second[n].wait_recv()
            finish(n, sums[ph, n] + other[ph, n])
        return first + second

    def residual(n, total, bias):
        cols = slice(n * CW, (n + 1) * CW)
        v = xrow[:, cols] + total + bias[layer:layer + 1, cols].astype(f32)
        xrow[:, cols] = v.astype(bf16).astype(f32)

    wd_copy.wait()
    o = o_buf[...].astype(bf16)
    sends = reduce(0, lambda n: jnp.dot(o, wd[:, n * CW:(n + 1) * CW], preferred_element_type=f32),
                   lambda n, total: residual(n, total, b_dense))

    normed = norm_rows(xrow[...], gain1, shift1).astype(bf16).astype(f32)
    swap = []
    for n in range(NCH):
        ag[n, own, :] = normed[:, n * CW:(n + 1) * CW]
        here = ag.at[n, own, :]
        swap.append(remote(here, here, g_sem, (n,), mate))
        swap[n].start()
    cols_up = pl.ds(pl.multiple_of(core * F_LOC, F_LOC), F_LOC)
    up[...] = jnp.broadcast_to(b_up[layer:layer + 1, cols_up].astype(f32), (HALF, F_LOC))
    for n in range(NCH):
        wu_copy(n).wait()
        swap[n].wait_recv()
        up[...] += jnp.dot(ag[n].astype(bf16), wu[n], preferred_element_type=f32)

    pick = (lax.broadcasted_iota(jnp.int32, (256, 128), 0) == 2 * lax.broadcasted_iota(jnp.int32, (256, 128), 1))
    pick = jnp.where(pick, 1.0, 0.0).astype(bf16)
    for k in range(F_LOC // 256):
        a = up[:, k * 256:(k + 1) * 256]
        z = jnp.minimum(a, GELU_LIMIT)
        gate = z * jax.nn.sigmoid(1.702 * z)
        lin = jnp.clip(a, -GELU_LIMIT, GELU_LIMIT) + 1.0
        prod = (gate * pltpu.roll(lin, 255, 1)).astype(bf16)
        mbuf[:, k * 128:(k + 1) * 128] = jnp.dot(prod, pick, preferred_element_type=f32).astype(bf16)
    wn_copy.wait()
    m = mbuf[...]
    sends += swap

    def spread(n, total):
        residual(n, total, b_down)
        full[n, all_rows(cx, core), :] = xrow[:, n * CW:(n + 1) * CW]
        here = full.at[n, all_rows(cx, core), :]
        for k, peer in enumerate((x_dev, mate)):
            copy = remote(here, here, x_sem, (k, n), peer)
            copy.start()
            sends.append(copy)

    sends += reduce(1, lambda n: jnp.dot(m, wn[:, n * CW:(n + 1) * CW], preferred_element_type=f32), spread)
    for n in range(NCH):
        there = full.at[n, all_rows(ox, core), :]
        remote(there, there, x_sem, (0, n), x_dev).wait_recv()
        copy = remote(there, there, x_sem, (2, n), mate)
        copy.start()
        sends.append(copy)
    for n in range(NCH):
        for k, x_ in ((1, cx), (2, ox)):
            there = full.at[n, all_rows(x_, 1 - core), :]
            remote(there, there, x_sem, (k, n), mate).wait_recv()
        out[:, n * CW:(n + 1) * CW] = full[n].astype(bf16)
    for copy in sends:
        copy.wait_send()


def rest_call(layer, msg, x, gain, shift, b_dense, b_up, b_down, w_dense, w_up, w_down):
    vm = pl.BlockSpec(memory_space=pltpu.VMEM)
    hbm = pl.BlockSpec(memory_space=pltpu.HBM)
    return pl.pallas_call(
        functools.partial(rest_kernel, layer),
        out_shape=jax.ShapeDtypeStruct((NB, D), bf16),
        in_specs=[vm] * 7 + [hbm] * 3,
        out_specs=vm,
        scratch_shapes=[
            pltpu.VMEM((DR, D), bf16),
            pltpu.VMEM((NCH, CW, F_LOC), bf16),
            pltpu.VMEM((M_LOC, D), bf16),
            pltpu.VMEM((3, MSG, HD), f32),
            pltpu.VMEM((2, MSG, HD), f32),
            pltpu.VMEM((HALF, DR), f32),
            pltpu.VMEM((2, NCH, HALF, CW), f32),
            pltpu.VMEM((2, NCH, ROWS, CW), f32),
            pltpu.VMEM((2, NCH, ROWS, CW), f32),
            pltpu.VMEM((2, NCH, ROWS, CW), f32),
            pltpu.VMEM((NCH, HALF, CW), f32),
            pltpu.VMEM((NCH, NB, CW), f32),
            pltpu.VMEM((ROWS, D), f32),
            pltpu.VMEM((HALF, F_LOC), f32),
            pltpu.VMEM((HALF, M_LOC), bf16),
            pltpu.SemaphoreType.DMA((2 + NCH,)),
            pltpu.SemaphoreType.DMA((2, 3)),
            pltpu.SemaphoreType.DMA((2, 2, NCH)),
            pltpu.SemaphoreType.DMA((2, 2, NCH)),
            pltpu.SemaphoreType.DMA((2, NCH)),
            pltpu.SemaphoreType.DMA((2, 3, NCH)),
        ],
        compiler_params=pltpu.CompilerParams(vmem_limit_bytes=VMEM_BYTES, collective_id=layer, has_side_effects=True),
        name=f'rest{layer}',
    )(msg, x, gain, shift, b_dense, b_up, b_down, w_dense, w_up, w_down)


def solution(mesh):
    cache_spec = P(None, 'dp', 'sp', 'tp', None)
    in_specs = (P('dp', None), P('dp'), cache_spec, cache_spec, P(), P(), P(None, None, 'tp'), P(None, 'tp'), P(None, 'tp', None), P(), P(None, None, 'tp'), P(None, 'tp'), P(None, 'tp', None), P())
    out_specs = (P('dp', None), cache_spec, cache_spec)

    def device_step(hidden, positions, k_cache, v_cache, ln_gain, ln_bias, w_qkv, b_qkv, w_dense, b_dense, w_up, b_up, w_down, b_down):
        shape = k_cache.shape
        flat = (2, NB, SLOTS * KVL, HD)
        k_cache = k_cache.reshape(flat)
        v_cache = v_cache.reshape(flat)
        half = HD // 2
        inv_freq = ROPE_THETA ** (-jnp.arange(half).astype(f32) * (2.0 / HD))
        angles = positions.astype(f32)[:, None] * inv_freq[None, :]
        cos_part = jnp.cos(angles)
        sin_part = jnp.sin(angles)
        cos = jnp.concatenate([cos_part, cos_part], axis=1)
        sin = jnp.concatenate([-sin_part, sin_part], axis=1)
        caches = None
        for layer in range(2):
            msg, *caches = attn_call(layer, positions, hidden, cos, sin, ln_gain, ln_bias, b_qkv, w_qkv, k_cache, v_cache, caches)
            hidden = rest_call(layer, msg, hidden, ln_gain, ln_bias, b_dense, b_up, b_down, w_dense, w_up, w_down)
        return hidden, caches[0].reshape(shape), caches[1].reshape(shape)

    return jax.shard_map(device_step, mesh=mesh, in_specs=in_specs, out_specs=out_specs, check_vma=False)
```

```python
import functools
import math

import jax
import jax.numpy as jnp
from jax import lax
from jax.experimental import pallas as pl
from jax.experimental.pallas import tpu as pltpu
from jax.sharding import PartitionSpec as P

BLOCK_SIZE = 64
LOCAL_BLOCKS = 16
VERT_STRIDE = 8
ROPE_THETA = 1000000.0
GELU_LIMIT = 20.0
NORM_EPS = 0.00001
MASKED = -1e30
MESH = pl.DeviceIdType.MESH

NB = 64
D = 3072
HD = 128
KVL = 4
GRP = 3
SLOTS = 64
QW = KVL * (GRP + 2) * HD
QROWS = 16
KCH = 6
KCS = D // KCH
G = 8
NG = NB // G
HALF = NB // 2
HPC = 6
MSG = HPC * HALF + 8
ROWS = HALF // 2
F_LOC = 4096
M_LOC = F_LOC // 2
NCH = 4
CW = D // NCH
DR = HPC * HD
LAG = 2
VMEM_BYTES = 52 * 1024 * 1024

f32 = jnp.float32
bf16 = jnp.bfloat16


def norm_rows(rows, gain, shift):
    mean = jnp.mean(rows, axis=-1, keepdims=True)
    cent = rows - mean
    var = jnp.mean(jnp.square(cent), axis=-1, keepdims=True)
    return (cent * lax.rsqrt(var + NORM_EPS)) * gain + shift


def rope_tables(pos):
    half = HD // 2
    row = lax.broadcasted_iota(jnp.int32, (8, HD), 0)
    lane = lax.broadcasted_iota(jnp.int32, (NB, HD), 1)
    groups = []
    for i in range(NB // 8):
        at = jnp.zeros((8, HD), jnp.int32)
        for r in range(8):
            at = jnp.where(row == r, pos[i * 8 + r], at)
        groups.append(at)
    where = jnp.concatenate(groups, axis=0).astype(f32)
    power = (lane % half).astype(f32) * (2.0 / HD)
    angles = where * jnp.exp(power * -math.log(ROPE_THETA))
    sin = jnp.sin(angles)
    return jnp.cos(angles), jnp.where(lane < half, -sin, sin)


def attn_kernel(layer, pos, x, gain, shift, b_qkv, w_hbm, kc_hbm, vc_hbm, *rest):
    if layer == 1:
        rest = rest[2:]
    (msg, ko_hbm, vo_hbm, w, kbuf, vbuf, u, acc, qs, kns, vns, os, ms, ls, wsem, ksem, vsem, osem) = rest[:18]
    sp = lax.axis_index('sp')
    tp = lax.axis_index('tp')
    base = sp * SLOTS

    def w_copy(i):
        return pltpu.make_async_copy(w_hbm.at[layer, pl.ds(i * KCS, KCS), :], w.at[i], wsem.at[i])

    def in_copy(hbm, buf, sem, i):
        return pltpu.make_async_copy(hbm.at[layer, pl.ds(i * G, G)], buf.at[pl.ds(i * G, G)], sem.at[i])

    def out_copy(buf, hbm, j, i):
        return pltpu.make_async_copy(buf.at[pl.ds(i * G, G)], hbm.at[layer, pl.ds(i * G, G)], osem.at[j, i])

    if layer == 0:
        places, small_sem = rest[18:23], rest[23]
        small = [pltpu.make_async_copy(src, dst, small_sem.at[i]) for i, (src, dst) in enumerate(zip((pos, x, gain, shift, b_qkv), places))]
        for copy in small:
            copy.start()
        pos, x, gain, shift, b_qkv = places
    for i in range(KCH):
        w_copy(i).start(priority=i % 2)
    for i in range(NG):
        in_copy(kc_hbm, kbuf, ksem, i).start(priority=0)
        in_copy(vc_hbm, vbuf, vsem, i).start(priority=1)
    if layer == 0:
        for copy in small:
            copy.wait()

    g_row = gain[layer, 0:1, :].astype(f32)
    s_row = shift[layer, 0:1, :].astype(f32)
    for i in range(NB // 16):
        rows = x[pl.ds(i * 16, 16), :].astype(f32)
        normed = norm_rows(rows, g_row, s_row).astype(bf16)
        for j in range(KCH):
            u[j, pl.ds(i * 16, 16), :] = normed[:, j * KCS:(j + 1) * KCS]
    acc[...] = jnp.broadcast_to(b_qkv[layer:layer + 1, :].astype(f32), (NB, QW))
    qs[...] = jnp.zeros_like(qs)

    cos_t, sin_t = rope_tables(pos)

    def qkv_step(i, carry):
        w_copy(i).wait()
        acc[...] += jnp.dot(u[i], w[i], preferred_element_type=f32)
        return carry

    lax.fori_loop(0, KCH, qkv_step, 0)

    for c in range(KVL):
        for j in range(GRP + 2):
            col = (c * (GRP + 2) + j) * HD
            tile = acc[:, col:col + HD]
            if j <= GRP:
                tile = tile * cos_t + pltpu.roll(tile, HD // 2, 1) * sin_t
            for i in range(NB // 8):
                part = tile[i * 8:(i + 1) * 8]
                if j < GRP:
                    qs[pl.ds(i * 8 * QROWS + c * GRP + j, 8, stride=QROWS), :] = part
                else:
                    dst = kns if j == GRP else vns
                    dst[pl.ds(i * 64 + c, 8, stride=8), :] = part
                    dst[pl.ds(i * 64 + c + 4, 8, stride=8), :] = part

    row_h = lax.broadcasted_iota(jnp.int32, (QROWS, SLOTS * KVL), 0)
    col_i = lax.broadcasted_iota(jnp.int32, (QROWS, SLOTS * KVL), 1)
    slot_of = jnp.where(row_h // GRP == col_i % KVL, col_i // KVL, 1 << 20)
    head_id = tp * KVL * GRP + row_h
    vertical = (sp + head_id + 1) % VERT_STRIDE == 0
    sub_row = lax.broadcasted_iota(jnp.int32, (16, HD), 0) // KVL

    def attn_step(i, carry):
        in_copy(kc_hbm, kbuf, ksem, i).wait()
        in_copy(vc_hbm, vbuf, vsem, i).wait()
        limits = []
        for bi in range(G):
            b = i * G + bi
            p = pos[b]
            pl_ = p - base
            pc = jnp.clip(pl_, 0, SLOTS - 1)
            hit = jnp.logical_and(pl_ >= 0, pl_ < SLOTS)
            sub = jnp.where(hit, pc % KVL, -1)
            r0 = pl.multiple_of((pc // KVL) * 16, 16)
            put = sub_row == sub
            for buf, new in ((kbuf, kns), (vbuf, vns)):
                new8 = new[pl.ds(pl.multiple_of(b * 8, 8), 8), :]
                new16 = jnp.concatenate([new8, new8], axis=0)
                old = buf[b, pl.ds(r0, 16), :].astype(f32)
                buf[b, pl.ds(r0, 16), :] = jnp.where(put, new16, old).astype(bf16)
            if layer == 0:
                near = p // BLOCK_SIZE - sp < LOCAL_BLOCKS
                limits.append(jnp.where(vertical, pl_, jnp.where(near, pl_, -1)))
            else:
                limits.append(pl_)
        scores = []
        for bi in range(G):
            b = i * G + bi
            q = qs[pl.ds(pl.multiple_of(b * QROWS, QROWS), QROWS), :].astype(bf16)
            scores.append(lax.dot_general(q, kbuf[b], (((1,), (1,)), ((), ())), preferred_element_type=f32))
        keeps = [slot_of <= limit for limit in limits]
        scores = [jnp.where(keep, s * (1.0 / HD), MASKED) for keep, s in zip(keeps, scores)]
        peaks = [jnp.max(s, axis=1, keepdims=True) for s in scores]
        weights = [jnp.where(keep, jnp.exp(s - peak), 0.0) for keep, s, peak in zip(keeps, scores, peaks)]
        outs = [jnp.dot(wt.astype(bf16), vbuf[i * G + bi], preferred_element_type=f32) for bi, wt in enumerate(weights)]
        sums = [jnp.sum(wt, axis=1, keepdims=True) for wt in weights]
        for bi in range(G):
            rows = pl.ds(pl.multiple_of((i * G + bi) * QROWS, QROWS), QROWS)
            ms[rows, :] = jnp.broadcast_to(peaks[bi], (QROWS, HD))
            ls[rows, :] = jnp.broadcast_to(sums[bi], (QROWS, HD))
            os[rows, :] = outs[bi]

        @pl.when(i > 0)
        def _():
            out_copy(kbuf, ko_hbm, 0, i - 1).start()
            out_copy(vbuf, vo_hbm, 1, i - 1).start(priority=1)

        return carry

    lax.fori_loop(0, NG, attn_step, 0)

    lane = lax.broadcasted_iota(jnp.int32, (8, HD), 1)
    for half in range(2):
        for c in range(2):
            stat = jnp.zeros((8, HD), f32)
            for g in range(HPC):
                for i in range(HALF // 8):
                    rows = pl.ds((half * HALF + i * 8) * QROWS + c * HPC + g, 8, stride=QROWS)
                    at = 2 * (g * (HALF // 8) + i)
                    msg[half * 2 + c, pl.ds(g * HALF + i * 8, 8), :] = os[rows, :]
                    stat = jnp.where(lane == at, ms[rows, :], stat)
                    stat = jnp.where(lane == at + 1, ls[rows, :], stat)
            msg[half * 2 + c, pl.ds(HPC * HALF, 8), :] = stat
    out_copy(kbuf, ko_hbm, 0, NG - 1).start()
    out_copy(vbuf, vo_hbm, 1, NG - 1).start(priority=1)
    for i in range(NG):
        out_copy(kbuf, ko_hbm, 0, i).wait()
        out_copy(vbuf, vo_hbm, 1, i).wait()


def attn_call(layer, pos, x, gain, shift, b_qkv, w_qkv, k_cache, v_cache, prev):
    vm = pl.BlockSpec(memory_space=pltpu.VMEM)
    hbm = pl.BlockSpec(memory_space=pltpu.HBM)
    args = [pos, x, gain, shift, b_qkv, w_qkv, k_cache, v_cache]
    if layer == 0:
        specs = [hbm] * 8
        alias = {}
        small = [pltpu.SMEM(pos.shape, jnp.int32)] + [pltpu.VMEM(arr.shape, bf16) for arr in (x, gain, shift, b_qkv)]
        small.append(pltpu.SemaphoreType.DMA((5,)))
        limit = 60 * 1024 * 1024
    else:
        args += list(prev)
        specs = [pl.BlockSpec(memory_space=pltpu.SMEM)] + [vm] * 4 + [hbm] * 5
        alias = {8: 1, 9: 2}
        small = []
        limit = VMEM_BYTES
    cache = jax.ShapeDtypeStruct(k_cache.shape, bf16)
    return pl.pallas_call(
        functools.partial(attn_kernel, layer),
        out_shape=(jax.ShapeDtypeStruct((KVL, MSG, HD), f32), cache, cache),
        in_specs=specs,
        out_specs=(vm, hbm, hbm),
        scratch_shapes=[
            pltpu.VMEM((KCH, KCS, QW), bf16),
            pltpu.VMEM((NB, SLOTS * KVL, HD), bf16),
            pltpu.VMEM((NB, SLOTS * KVL, HD), bf16),
            pltpu.VMEM((KCH, NB, KCS), bf16),
            pltpu.VMEM((NB, QW), f32),
            pltpu.VMEM((NB * QROWS, HD), f32),
            pltpu.VMEM((NB * 8, HD), f32),
            pltpu.VMEM((NB * 8, HD), f32),
            pltpu.VMEM((NB * QROWS, HD), f32),
            pltpu.VMEM((NB * QROWS, HD), f32),
            pltpu.VMEM((NB * QROWS, HD), f32),
            pltpu.SemaphoreType.DMA((KCH,)),
            pltpu.SemaphoreType.DMA((NG,)),
            pltpu.SemaphoreType.DMA((NG,)),
            pltpu.SemaphoreType.DMA((2, NG)),
            *small,
        ],
        input_output_aliases=alias,
        compiler_params=pltpu.CompilerParams(vmem_limit_bytes=limit),
        name=f'attn{layer}',
    )(*args)


def rest_kernel(layer, msg, x, gain, shift, b_dense, b_up, b_down, wd_hbm, wu_hbm, wn_hbm, out,
                wd, wu, wn, got, sent, o_buf, part, pair, sums, other, ag, full, xrow, up, mbuf,
                wsem, a_sem, d_sem, y_sem, g_sem, x_sem):
    dp = lax.axis_index('dp')
    tp = lax.axis_index('tp')
    sp = lax.axis_index('sp')
    core = sp % 2
    cx = sp // 2
    ox = 1 - cx
    mate = (dp, tp, cx * 2 + 1 - core)
    x_dev = (dp, tp, ox * 2 + core)
    y_dev = (dp, 1 - tp, sp)

    def load(src, dst, i):
        return pltpu.make_async_copy(src, dst, wsem.at[i])

    wd_copy = load(wd_hbm.at[layer, pl.ds(pl.multiple_of(core * DR, DR), DR), :], wd, 0)

    def wu_copy(i):
        return load(wu_hbm.at[layer, pl.ds(i * CW, CW), pl.ds(pl.multiple_of(core * F_LOC, F_LOC), F_LOC)], wu.at[i], 1 + i)

    wn_copy = load(wn_hbm.at[layer, pl.ds(pl.multiple_of(core * M_LOC, M_LOC), M_LOC), :], wn, 1 + NCH)

    barrier = pltpu.get_barrier_semaphore()
    for peer in (mate, x_dev, y_dev):
        pl.semaphore_signal(barrier, inc=1, device_id=peer, device_id_type=MESH)
    wd_copy.start()
    for i in range(NCH):
        wu_copy(i).start()
    wn_copy.start()
    pl.semaphore_wait(barrier, 3)

    def remote(src, dst, sems, idx, peer):
        return pltpu.make_async_remote_copy(
            src_ref=src, dst_ref=dst, send_sem=sems.at[(0,) + idx], recv_sem=sems.at[(1,) + idx],
            device_id=peer, device_id_type=MESH)

    near = cx * 2 + core
    far = ox * 2 + core
    swap = [remote(msg.at[ox * 2 + 1 - core], got.at[0], a_sem, (0,), mate),
            remote(msg.at[cx * 2 + 1 - core], got.at[1], a_sem, (1,), mate)]
    for copy in swap:
        copy.start()

    gain1 = gain[layer, 1:2, :].astype(f32)
    shift1 = shift[layer, 1:2, :].astype(f32)
    own = pl.ds(pl.multiple_of(core * ROWS, ROWS), ROWS)
    theirs = pl.ds(pl.multiple_of((1 - core) * ROWS, ROWS), ROWS)

    def all_rows(x_, c_):
        return pl.ds(pl.multiple_of(x_ * HALF + c_ * ROWS, ROWS), ROWS)

    xrow[...] = x[all_rows(cx, core), :].astype(f32)
    lane = lax.broadcasted_iota(jnp.int32, (8, HD), 1)

    def merge(one, two, put, stat_out=None):
        stats = [ref[pl.ds(HPC * HALF, 8), :] for ref in (one, two)]
        new_stat = jnp.zeros((8, HD), f32)
        for g in range(HPC):
            for i in range(HALF // 8):
                at = 2 * (g * (HALF // 8) + i)
                peaks = [jnp.broadcast_to(st[:, at:at + 1], (8, HD)) for st in stats]
                tots = [jnp.broadcast_to(st[:, at + 1:at + 2], (8, HD)) for st in stats]
                top = jnp.maximum(peaks[0], peaks[1])
                scale = [jnp.exp(p - top) for p in peaks]
                rows = pl.ds(g * HALF + i * 8, 8)
                num = one[rows, :] * scale[0] + two[rows, :] * scale[1]
                den = tots[0] * scale[0] + tots[1] * scale[1]
                put(g, i, num, den)
                if stat_out is not None:
                    new_stat = jnp.where(lane == at, top, new_stat)
                    new_stat = jnp.where(lane == at + 1, den, new_stat)
        if stat_out is not None:
            stat_out[pl.ds(HPC * HALF, 8), :] = new_stat

    def put_part(ref):
        def put(g, i, num, den):
            ref[pl.ds(g * HALF + i * 8, 8), :] = num
        return put

    def put_out(g, i, num, den):
        o_buf[pl.ds(i * 8, 8), g * HD:(g + 1) * HD] = num / den

    swap[0].wait_recv()
    merge(msg.at[far], got.at[0], put_part(sent.at[0]), sent.at[0])
    cross = remote(sent.at[0], got.at[2], a_sem, (2,), x_dev)
    cross.start()
    swap[1].wait_recv()
    merge(msg.at[near], got.at[1], put_part(sent.at[1]), sent.at[1])
    cross.wait_recv()
    merge(sent.at[1], got.at[2], put_out)
    for copy in swap + [cross]:
        copy.wait_send()

    def reduce(ph, product, finish):
        first = [remote(part.at[ph, n, theirs, :], pair.at[ph, n], d_sem, (ph, n), mate) for n in range(NCH)]
        second = [remote(sums.at[ph, n], other.at[ph, n], y_sem, (ph, n), y_dev) for n in range(NCH)]
        for step in range(NCH + LAG):
            if step < NCH:
                part[ph, step] = product(step)
                first[step].start()
            if step >= LAG:
                n = step - LAG
                first[n].wait_recv()
                sums[ph, n] = part[ph, n, own, :] + pair[ph, n]
                second[n].start()
        for n in range(NCH):
            second[n].wait_recv()
            finish(n, sums[ph, n] + other[ph, n])
        return first + second

    def residual(n, total, bias):
        cols = slice(n * CW, (n + 1) * CW)
        v = xrow[:, cols] + total + bias[layer:layer + 1, cols].astype(f32)
        xrow[:, cols] = v.astype(bf16).astype(f32)

    wd_copy.wait()
    o = o_buf[...].astype(bf16)
    sends = reduce(0, lambda n: jnp.dot(o, wd[:, n * CW:(n + 1) * CW], preferred_element_type=f32),
                   lambda n, total: residual(n, total, b_dense))

    normed = norm_rows(xrow[...], gain1, shift1).astype(bf16).astype(f32)
    swap = []
    for n in range(NCH):
        ag[n, own, :] = normed[:, n * CW:(n + 1) * CW]
        here = ag.at[n, own, :]
        swap.append(remote(here, here, g_sem, (n,), mate))
        swap[n].start()
    cols_up = pl.ds(pl.multiple_of(core * F_LOC, F_LOC), F_LOC)
    up[...] = jnp.broadcast_to(b_up[layer:layer + 1, cols_up].astype(f32), (HALF, F_LOC))
    for n in range(NCH):
        wu_copy(n).wait()
        swap[n].wait_recv()
        up[...] += jnp.dot(ag[n].astype(bf16), wu[n], preferred_element_type=f32)

    pick = (lax.broadcasted_iota(jnp.int32, (256, 128), 0) == 2 * lax.broadcasted_iota(jnp.int32, (256, 128), 1))
    pick = jnp.where(pick, 1.0, 0.0).astype(bf16)
    for k in range(F_LOC // 256):
        a = up[:, k * 256:(k + 1) * 256]
        z = jnp.minimum(a, GELU_LIMIT)
        gate = z * jax.nn.sigmoid(1.702 * z)
        lin = jnp.clip(a, -GELU_LIMIT, GELU_LIMIT) + 1.0
        prod = (gate * pltpu.roll(lin, 255, 1)).astype(bf16)
        mbuf[:, k * 128:(k + 1) * 128] = jnp.dot(prod, pick, preferred_element_type=f32).astype(bf16)
    wn_copy.wait()
    m = mbuf[...]
    sends += swap

    def spread(n, total):
        residual(n, total, b_down)
        full[n, all_rows(cx, core), :] = xrow[:, n * CW:(n + 1) * CW]
        here = full.at[n, all_rows(cx, core), :]
        for k, peer in enumerate((x_dev, mate)):
            copy = remote(here, here, x_sem, (k, n), peer)
            copy.start()
            sends.append(copy)

    sends += reduce(1, lambda n: jnp.dot(m, wn[:, n * CW:(n + 1) * CW], preferred_element_type=f32), spread)
    for n in range(NCH):
        there = full.at[n, all_rows(ox, core), :]
        remote(there, there, x_sem, (0, n), x_dev).wait_recv()
        copy = remote(there, there, x_sem, (2, n), mate)
        copy.start()
        sends.append(copy)
    for n in range(NCH):
        for k, x_ in ((1, cx), (2, ox)):
            there = full.at[n, all_rows(x_, 1 - core), :]
            remote(there, there, x_sem, (k, n), mate).wait_recv()
        out[:, n * CW:(n + 1) * CW] = full[n].astype(bf16)
    for copy in sends:
        copy.wait_send()


def rest_call(layer, msg, x, gain, shift, b_dense, b_up, b_down, w_dense, w_up, w_down):
    vm = pl.BlockSpec(memory_space=pltpu.VMEM)
    hbm = pl.BlockSpec(memory_space=pltpu.HBM)
    return pl.pallas_call(
        functools.partial(rest_kernel, layer),
        out_shape=jax.ShapeDtypeStruct((NB, D), bf16),
        in_specs=[vm] * 7 + [hbm] * 3,
        out_specs=vm,
        scratch_shapes=[
            pltpu.VMEM((DR, D), bf16),
            pltpu.VMEM((NCH, CW, F_LOC), bf16),
            pltpu.VMEM((M_LOC, D), bf16),
            pltpu.VMEM((3, MSG, HD), f32),
            pltpu.VMEM((2, MSG, HD), f32),
            pltpu.VMEM((HALF, DR), f32),
            pltpu.VMEM((2, NCH, HALF, CW), f32),
            pltpu.VMEM((2, NCH, ROWS, CW), f32),
            pltpu.VMEM((2, NCH, ROWS, CW), f32),
            pltpu.VMEM((2, NCH, ROWS, CW), f32),
            pltpu.VMEM((NCH, HALF, CW), f32),
            pltpu.VMEM((NCH, NB, CW), f32),
            pltpu.VMEM((ROWS, D), f32),
            pltpu.VMEM((HALF, F_LOC), f32),
            pltpu.VMEM((HALF, M_LOC), bf16),
            pltpu.SemaphoreType.DMA((2 + NCH,)),
            pltpu.SemaphoreType.DMA((2, 3)),
            pltpu.SemaphoreType.DMA((2, 2, NCH)),
            pltpu.SemaphoreType.DMA((2, 2, NCH)),
            pltpu.SemaphoreType.DMA((2, NCH)),
            pltpu.SemaphoreType.DMA((2, 3, NCH)),
        ],
        compiler_params=pltpu.CompilerParams(vmem_limit_bytes=VMEM_BYTES, collective_id=layer, has_side_effects=True),
        name=f'rest{layer}',
    )(msg, x, gain, shift, b_dense, b_up, b_down, w_dense, w_up, w_down)


def solution(mesh):
    cache_spec = P(None, 'dp', 'sp', 'tp', None)
    in_specs = (P('dp', None), P('dp'), cache_spec, cache_spec, P(), P(), P(None, None, 'tp'), P(None, 'tp'), P(None, 'tp', None), P(), P(None, None, 'tp'), P(None, 'tp'), P(None, 'tp', None), P())
    out_specs = (P('dp', None), cache_spec, cache_spec)

    def device_step(hidden, positions, k_cache, v_cache, ln_gain, ln_bias, w_qkv, b_qkv, w_dense, b_dense, w_up, b_up, w_down, b_down):
        shape = k_cache.shape
        flat = (2, NB, SLOTS * KVL, HD)
        k_cache = k_cache.reshape(flat)
        v_cache = v_cache.reshape(flat)
        caches = None
        for layer in range(2):
            msg, *caches = attn_call(layer, positions, hidden, ln_gain, ln_bias, b_qkv, w_qkv, k_cache, v_cache, caches)
            hidden = rest_call(layer, msg, hidden, ln_gain, ln_bias, b_dense, b_up, b_down, w_dense, w_up, w_down)
        return hidden, caches[0].reshape(shape), caches[1].reshape(shape)

    return jax.shard_map(device_step, mesh=mesh, in_specs=in_specs, out_specs=out_specs, check_vma=False)
```

```python
import functools
import math

import jax
import jax.numpy as jnp
from jax import lax
from jax.experimental import pallas as pl
from jax.experimental.pallas import tpu as pltpu
from jax.sharding import PartitionSpec as P

BLOCK_SIZE = 64
LOCAL_BLOCKS = 16
VERT_STRIDE = 8
ROPE_THETA = 1000000.0
GELU_LIMIT = 20.0
NORM_EPS = 0.00001
MASKED = -1e30
MESH = pl.DeviceIdType.MESH

NB = 64
D = 3072
HD = 128
KVL = 4
GRP = 3
SLOTS = 64
QW = KVL * (GRP + 2) * HD
QROWS = 16
KCH = 6
KCS = D // KCH
G = 8
NG = NB // G
HALF = NB // 2
HPC = 6
MSG = HPC * HALF + 8
ROWS = HALF // 2
F_LOC = 4096
M_LOC = F_LOC // 2
NCH = 4
CW = D // NCH
QC = QW // NCH
DR = HPC * HD
LAG = 2
VMEM_BYTES = 52 * 1024 * 1024

f32 = jnp.float32
bf16 = jnp.bfloat16


def norm_rows(rows, gain, shift):
    mean = jnp.mean(rows, axis=-1, keepdims=True)
    cent = rows - mean
    var = jnp.mean(jnp.square(cent), axis=-1, keepdims=True)
    return (cent * lax.rsqrt(var + NORM_EPS)) * gain + shift


def rope_tables(pos):
    half = HD // 2
    row = lax.broadcasted_iota(jnp.int32, (8, HD), 0)
    lane = lax.broadcasted_iota(jnp.int32, (NB, HD), 1)
    groups = []
    for i in range(NB // 8):
        at = jnp.zeros((8, HD), jnp.int32)
        for r in range(8):
            at = jnp.where(row == r, pos[i * 8 + r], at)
        groups.append(at)
    where = jnp.concatenate(groups, axis=0).astype(f32)
    power = (lane % half).astype(f32) * (2.0 / HD)
    angles = where * jnp.exp(power * -math.log(ROPE_THETA))
    sin = jnp.sin(angles)
    return jnp.cos(angles), jnp.where(lane < half, -sin, sin)


def attn_kernel(layer, pos, *rest):
    if layer == 0:
        x, gain, shift, b_qkv, w_hbm, kc_hbm, vc_hbm, *rest = rest
    else:
        acc, kc_hbm, vc_hbm, _, _, *rest = rest
    msg, ko_hbm, vo_hbm, kbuf, vbuf, qs, kns, vns, os, ms, ls, ksem, vsem, osem, *rest = rest
    sp = lax.axis_index('sp')
    tp = lax.axis_index('tp')
    base = sp * SLOTS

    def in_copy(hbm, buf, sem, i):
        return pltpu.make_async_copy(hbm.at[layer, pl.ds(i * G, G)], buf.at[pl.ds(i * G, G)], sem.at[i])

    def out_copy(buf, hbm, j, i):
        return pltpu.make_async_copy(buf.at[pl.ds(i * G, G)], hbm.at[layer, pl.ds(i * G, G)], osem.at[j, i])

    def fetch_cache():
        for i in range(NG):
            in_copy(kc_hbm, kbuf, ksem, i).start(priority=0)
            in_copy(vc_hbm, vbuf, vsem, i).start(priority=1)

    if layer == 0:
        w, u, acc, wsem, *places, small_sem = rest
        small = [pltpu.make_async_copy(src, dst, small_sem.at[i]) for i, (src, dst) in enumerate(zip((pos, x, gain, shift, b_qkv), places))]
        for copy in small:
            copy.start()
        pos, x, gain, shift, b_qkv = places

        def w_copy(i):
            return pltpu.make_async_copy(w_hbm.at[layer, pl.ds(i * KCS, KCS), :], w.at[i], wsem.at[i])

        for i in range(KCH):
            w_copy(i).start(priority=i % 2)
        fetch_cache()
        for copy in small:
            copy.wait()
        g_row = gain[layer, 0:1, :].astype(f32)
        s_row = shift[layer, 0:1, :].astype(f32)
        for i in range(NB // 16):
            rows = x[pl.ds(i * 16, 16), :].astype(f32)
            normed = norm_rows(rows, g_row, s_row).astype(bf16)
            for j in range(KCH):
                u[j, pl.ds(i * 16, 16), :] = normed[:, j * KCS:(j + 1) * KCS]
        acc[...] = jnp.broadcast_to(b_qkv[layer:layer + 1, :].astype(f32), (NB, QW))
    else:
        fetch_cache()
    qs[...] = jnp.zeros_like(qs)
    cos_t, sin_t = rope_tables(pos)
    if layer == 0:
        def qkv_step(i, carry):
            w_copy(i).wait()
            acc[...] += jnp.dot(u[i], w[i], preferred_element_type=f32)
            return carry

        lax.fori_loop(0, KCH, qkv_step, 0)

    for c in range(KVL):
        for j in range(GRP + 2):
            if layer == 0:
                col = (c * (GRP + 2) + j) * HD
                tile = acc[:, col:col + HD]
            else:
                tile = acc[c, :, j * HD:(j + 1) * HD]
            if j <= GRP:
                tile = tile * cos_t + pltpu.roll(tile, HD // 2, 1) * sin_t
            for i in range(NB // 8):
                part = tile[i * 8:(i + 1) * 8]
                if j < GRP:
                    qs[pl.ds(i * 8 * QROWS + c * GRP + j, 8, stride=QROWS), :] = part
                else:
                    dst = kns if j == GRP else vns
                    dst[pl.ds(i * 64 + c, 8, stride=8), :] = part
                    dst[pl.ds(i * 64 + c + 4, 8, stride=8), :] = part

    row_h = lax.broadcasted_iota(jnp.int32, (QROWS, SLOTS * KVL), 0)
    col_i = lax.broadcasted_iota(jnp.int32, (QROWS, SLOTS * KVL), 1)
    slot_of = jnp.where(row_h // GRP == col_i % KVL, col_i // KVL, 1 << 20)
    head_id = tp * KVL * GRP + row_h
    vertical = (sp + head_id + 1) % VERT_STRIDE == 0
    sub_row = lax.broadcasted_iota(jnp.int32, (16, HD), 0) // KVL

    def attn_step(i, carry):
        in_copy(kc_hbm, kbuf, ksem, i).wait()
        in_copy(vc_hbm, vbuf, vsem, i).wait()
        limits = []
        for bi in range(G):
            b = i * G + bi
            p = pos[b]
            pl_ = p - base
            pc = jnp.clip(pl_, 0, SLOTS - 1)
            hit = jnp.logical_and(pl_ >= 0, pl_ < SLOTS)
            sub = jnp.where(hit, pc % KVL, -1)
            r0 = pl.multiple_of((pc // KVL) * 16, 16)
            put = sub_row == sub
            for buf, new in ((kbuf, kns), (vbuf, vns)):
                new8 = new[pl.ds(pl.multiple_of(b * 8, 8), 8), :]
                new16 = jnp.concatenate([new8, new8], axis=0)
                old = buf[b, pl.ds(r0, 16), :].astype(f32)
                buf[b, pl.ds(r0, 16), :] = jnp.where(put, new16, old).astype(bf16)
            if layer == 0:
                near = p // BLOCK_SIZE - sp < LOCAL_BLOCKS
                limits.append(jnp.where(vertical, pl_, jnp.where(near, pl_, -1)))
            else:
                limits.append(pl_)
        scores = []
        for bi in range(G):
            b = i * G + bi
            q = qs[pl.ds(pl.multiple_of(b * QROWS, QROWS), QROWS), :].astype(bf16)
            scores.append(lax.dot_general(q, kbuf[b], (((1,), (1,)), ((), ())), preferred_element_type=f32))
        keeps = [slot_of <= limit for limit in limits]
        scores = [jnp.where(keep, s * (1.0 / HD), MASKED) for keep, s in zip(keeps, scores)]
        peaks = [jnp.max(s, axis=1, keepdims=True) for s in scores]
        weights = [jnp.where(keep, jnp.exp(s - peak), 0.0) for keep, s, peak in zip(keeps, scores, peaks)]
        outs = [jnp.dot(wt.astype(bf16), vbuf[i * G + bi], preferred_element_type=f32) for bi, wt in enumerate(weights)]
        sums = [jnp.sum(wt, axis=1, keepdims=True) for wt in weights]
        for bi in range(G):
            rows = pl.ds(pl.multiple_of((i * G + bi) * QROWS, QROWS), QROWS)
            ms[rows, :] = jnp.broadcast_to(peaks[bi], (QROWS, HD))
            ls[rows, :] = jnp.broadcast_to(sums[bi], (QROWS, HD))
            os[rows, :] = outs[bi]

        @pl.when(i > 0)
        def _():
            out_copy(kbuf, ko_hbm, 0, i - 1).start()
            out_copy(vbuf, vo_hbm, 1, i - 1).start(priority=1)

        return carry

    lax.fori_loop(0, NG, attn_step, 0)

    lane = lax.broadcasted_iota(jnp.int32, (8, HD), 1)
    for half in range(2):
        for c in range(2):
            stat = jnp.zeros((8, HD), f32)
            for g in range(HPC):
                for i in range(HALF // 8):
                    rows = pl.ds((half * HALF + i * 8) * QROWS + c * HPC + g, 8, stride=QROWS)
                    at = 2 * (g * (HALF // 8) + i)
                    msg[half * 2 + c, pl.ds(g * HALF + i * 8, 8), :] = os[rows, :]
                    stat = jnp.where(lane == at, ms[rows, :], stat)
                    stat = jnp.where(lane == at + 1, ls[rows, :], stat)
            msg[half * 2 + c, pl.ds(HPC * HALF, 8), :] = stat
    out_copy(kbuf, ko_hbm, 0, NG - 1).start()
    out_copy(vbuf, vo_hbm, 1, NG - 1).start(priority=1)
    for i in range(NG):
        out_copy(kbuf, ko_hbm, 0, i).wait()
        out_copy(vbuf, vo_hbm, 1, i).wait()


def attn_call(layer, pos, operands, k_cache, v_cache, prev):
    vm = pl.BlockSpec(memory_space=pltpu.VMEM)
    hbm = pl.BlockSpec(memory_space=pltpu.HBM)
    args = [pos, *operands, k_cache, v_cache]
    if layer == 0:
        specs = [hbm] * 8
        alias = {}
        extra = [
            pltpu.VMEM((KCH, KCS, QW), bf16),
            pltpu.VMEM((KCH, NB, KCS), bf16),
            pltpu.VMEM((NB, QW), f32),
            pltpu.SemaphoreType.DMA((KCH,)),
            pltpu.SMEM(pos.shape, jnp.int32),
            *[pltpu.VMEM(arr.shape, bf16) for arr in operands[:4]],
            pltpu.SemaphoreType.DMA((5,)),
        ]
        limit = 60 * 1024 * 1024
    else:
        args += list(prev)
        specs = [pl.BlockSpec(memory_space=pltpu.SMEM), vm] + [hbm] * 4
        alias = {4: 1, 5: 2}
        extra = []
        limit = VMEM_BYTES
    cache = jax.ShapeDtypeStruct(k_cache.shape, bf16)
    return pl.pallas_call(
        functools.partial(attn_kernel, layer),
        out_shape=(jax.ShapeDtypeStruct((KVL, MSG, HD), f32), cache, cache),
        in_specs=specs,
        out_specs=(vm, hbm, hbm),
        scratch_shapes=[
            pltpu.VMEM((NB, SLOTS * KVL, HD), bf16),
            pltpu.VMEM((NB, SLOTS * KVL, HD), bf16),
            pltpu.VMEM((NB * QROWS, HD), f32),
            pltpu.VMEM((NB * 8, HD), f32),
            pltpu.VMEM((NB * 8, HD), f32),
            pltpu.VMEM((NB * QROWS, HD), f32),
            pltpu.VMEM((NB * QROWS, HD), f32),
            pltpu.VMEM((NB * QROWS, HD), f32),
            pltpu.SemaphoreType.DMA((NG,)),
            pltpu.SemaphoreType.DMA((NG,)),
            pltpu.SemaphoreType.DMA((2, NG)),
            *extra,
        ],
        input_output_aliases=alias,
        compiler_params=pltpu.CompilerParams(vmem_limit_bytes=limit),
        name=f'attn{layer}',
    )(*args)


def rest_kernel(layer, msg, x, gain, shift, b_dense, b_up, b_down, wd_hbm, wu_hbm, wn_hbm, *rest):
    if layer == 0:
        b_qkv, wq_hbm, x_out, out, *rest = rest
    else:
        out, *rest = rest
    (wd, wu, wn, got, sent, o_buf, part, pair, sums, other, ag, full, xrow, up, mbuf,
     wsem, a_sem, d_sem, y_sem, g_sem, x_sem) = rest
    dp = lax.axis_index('dp')
    tp = lax.axis_index('tp')
    sp = lax.axis_index('sp')
    core = sp % 2
    cx = sp // 2
    ox = 1 - cx
    mate = (dp, tp, cx * 2 + 1 - core)
    x_dev = (dp, tp, ox * 2 + core)
    y_dev = (dp, 1 - tp, sp)

    def load(src, dst, i):
        return pltpu.make_async_copy(src, dst, wsem.at[i])

    wd_copy = load(wd_hbm.at[layer, pl.ds(pl.multiple_of(core * DR, DR), DR), :], wd, 0)

    def wu_copy(i):
        return load(wu_hbm.at[layer, pl.ds(i * CW, CW), pl.ds(pl.multiple_of(core * F_LOC, F_LOC), F_LOC)], wu.at[i], 1 + i)

    wn_copy = load(wn_hbm.at[layer, pl.ds(pl.multiple_of(core * M_LOC, M_LOC), M_LOC), :], wn, 1 + NCH)

    def wq_copy(i):
        return load(wq_hbm.at[1, pl.ds(i * CW, CW), :], wu.at[i, :, pl.ds(0, QW)], 2 + NCH + i)

    barrier = pltpu.get_barrier_semaphore()
    for peer in (mate, x_dev, y_dev):
        pl.semaphore_signal(barrier, inc=1, device_id=peer, device_id_type=MESH)
    wd_copy.start()
    for i in range(NCH):
        wu_copy(i).start()
    wn_copy.start()
    pl.semaphore_wait(barrier, 3)

    def remote(src, dst, sems, idx, peer):
        return pltpu.make_async_remote_copy(
            src_ref=src, dst_ref=dst, send_sem=sems.at[(0,) + idx], recv_sem=sems.at[(1,) + idx],
            device_id=peer, device_id_type=MESH)

    near = cx * 2 + core
    far = ox * 2 + core
    swap = [remote(msg.at[ox * 2 + 1 - core], got.at[0], a_sem, (0,), mate),
            remote(msg.at[cx * 2 + 1 - core], got.at[1], a_sem, (1,), mate)]
    for copy in swap:
        copy.start()

    gain1 = gain[layer, 1:2, :].astype(f32)
    shift1 = shift[layer, 1:2, :].astype(f32)
    own = pl.ds(pl.multiple_of(core * ROWS, ROWS), ROWS)
    theirs = pl.ds(pl.multiple_of((1 - core) * ROWS, ROWS), ROWS)

    def all_rows(x_, c_):
        return pl.ds(pl.multiple_of(x_ * HALF + c_ * ROWS, ROWS), ROWS)

    xrow[...] = x[all_rows(cx, core), :].astype(f32) if layer == 0 else x[...]
    lane = lax.broadcasted_iota(jnp.int32, (8, HD), 1)

    def merge(one, two, put, stat_out=None):
        stats = [ref[pl.ds(HPC * HALF, 8), :] for ref in (one, two)]
        new_stat = jnp.zeros((8, HD), f32)
        for g in range(HPC):
            for i in range(HALF // 8):
                at = 2 * (g * (HALF // 8) + i)
                peaks = [jnp.broadcast_to(st[:, at:at + 1], (8, HD)) for st in stats]
                tots = [jnp.broadcast_to(st[:, at + 1:at + 2], (8, HD)) for st in stats]
                top = jnp.maximum(peaks[0], peaks[1])
                scale = [jnp.exp(p - top) for p in peaks]
                rows = pl.ds(g * HALF + i * 8, 8)
                num = one[rows, :] * scale[0] + two[rows, :] * scale[1]
                den = tots[0] * scale[0] + tots[1] * scale[1]
                put(g, i, num, den)
                if stat_out is not None:
                    new_stat = jnp.where(lane == at, top, new_stat)
                    new_stat = jnp.where(lane == at + 1, den, new_stat)
        if stat_out is not None:
            stat_out[pl.ds(HPC * HALF, 8), :] = new_stat

    def put_part(ref):
        def put(g, i, num, den):
            ref[pl.ds(g * HALF + i * 8, 8), :] = num
        return put

    def put_out(g, i, num, den):
        o_buf[pl.ds(i * 8, 8), g * HD:(g + 1) * HD] = num / den

    swap[0].wait_recv()
    merge(msg.at[far], got.at[0], put_part(sent.at[0]), sent.at[0])
    cross = remote(sent.at[0], got.at[2], a_sem, (2,), x_dev)
    cross.start()
    swap[1].wait_recv()
    merge(msg.at[near], got.at[1], put_part(sent.at[1]), sent.at[1])
    cross.wait_recv()
    merge(sent.at[1], got.at[2], put_out)
    for copy in swap + [cross]:
        copy.wait_send()

    def reduce(ph, product, finish):
        first = [remote(part.at[ph, n, theirs, :], pair.at[ph, n], d_sem, (ph, n), mate) for n in range(NCH)]
        second = [remote(sums.at[ph, n], other.at[ph, n], y_sem, (ph, n), y_dev) for n in range(NCH)]
        for step in range(NCH + LAG):
            if step < NCH:
                part[ph, step] = product(step)
                first[step].start()
            if step >= LAG:
                n = step - LAG
                first[n].wait_recv()
                sums[ph, n] = part[ph, n, own, :] + pair[ph, n]
                second[n].start()
        for n in range(NCH):
            second[n].wait_recv()
            finish(n, sums[ph, n] + other[ph, n])
        return first + second

    def residual(n, total, bias):
        cols = slice(n * CW, (n + 1) * CW)
        v = xrow[:, cols] + total + bias[layer:layer + 1, cols].astype(f32)
        xrow[:, cols] = v.astype(bf16).astype(f32)

    wd_copy.wait()
    o = o_buf[...].astype(bf16)
    sends = reduce(0, lambda n: jnp.dot(o, wd[:, n * CW:(n + 1) * CW], preferred_element_type=f32),
                   lambda n, total: residual(n, total, b_dense))

    normed = norm_rows(xrow[...], gain1, shift1).astype(bf16).astype(f32)
    swap = []
    for n in range(NCH):
        ag[n, own, :] = normed[:, n * CW:(n + 1) * CW]
        here = ag.at[n, own, :]
        swap.append(remote(here, here, g_sem, (n,), mate))
        swap[n].start()
    cols_up = pl.ds(pl.multiple_of(core * F_LOC, F_LOC), F_LOC)
    up[...] = jnp.broadcast_to(b_up[layer:layer + 1, cols_up].astype(f32), (HALF, F_LOC))
    for n in range(NCH):
        wu_copy(n).wait()
        swap[n].wait_recv()
        up[...] += jnp.dot(ag[n].astype(bf16), wu[n], preferred_element_type=f32)
        if layer == 0:
            wq_copy(n).start()

    pick = (lax.broadcasted_iota(jnp.int32, (256, 128), 0) == 2 * lax.broadcasted_iota(jnp.int32, (256, 128), 1))
    pick = jnp.where(pick, 1.0, 0.0).astype(bf16)
    for k in range(F_LOC // 256):
        a = up[:, k * 256:(k + 1) * 256]
        z = jnp.minimum(a, GELU_LIMIT)
        gate = z * jax.nn.sigmoid(1.702 * z)
        lin = jnp.clip(a, -GELU_LIMIT, GELU_LIMIT) + 1.0
        prod = (gate * pltpu.roll(lin, 255, 1)).astype(bf16)
        mbuf[:, k * 128:(k + 1) * 128] = jnp.dot(prod, pick, preferred_element_type=f32).astype(bf16)
    wn_copy.wait()
    m = mbuf[...]
    sends += swap

    def spread(n, value):
        full[n, all_rows(cx, core), :] = value
        here = full.at[n, all_rows(cx, core), :]
        for k, peer in enumerate((x_dev, mate)):
            copy = remote(here, here, x_sem, (k, n), peer)
            copy.start()
            sends.append(copy)

    def collect(use):
        for n in range(NCH):
            there = full.at[n, all_rows(ox, core), :]
            remote(there, there, x_sem, (0, n), x_dev).wait_recv()
            copy = remote(there, there, x_sem, (2, n), mate)
            copy.start()
            sends.append(copy)
        for n in range(NCH):
            for k, x_ in ((1, cx), (2, ox)):
                there = full.at[n, all_rows(x_, 1 - core), :]
                remote(there, there, x_sem, (k, n), mate).wait_recv()
            use(n)

    def take_down(n, total):
        residual(n, total, b_down)
        if layer == 1:
            spread(n, xrow[:, n * CW:(n + 1) * CW])

    sends += reduce(1, lambda n: jnp.dot(m, wn[:, n * CW:(n + 1) * CW], preferred_element_type=f32), take_down)
    if layer == 0:
        x_out[...] = xrow[...]
        u = norm_rows(xrow[...], gain[1, 0:1, :].astype(f32), shift[1, 0:1, :].astype(f32)).astype(bf16)
        for i in range(NCH):
            wq_copy(i).wait()
        for n in range(NCH):
            cols = slice(n * QC, (n + 1) * QC)
            r = jnp.broadcast_to(b_qkv[1:2, cols].astype(f32), (ROWS, QC))
            for i in range(NCH):
                r += jnp.dot(u[:, i * CW:(i + 1) * CW], wu[i, :, cols], preferred_element_type=f32)
            spread(n, r)

        def use(n):
            out[n] = full[n]
    else:
        def use(n):
            out[:, n * CW:(n + 1) * CW] = full[n].astype(bf16)

    collect(use)
    for copy in sends:
        copy.wait_send()


def rest_call(layer, msg, x, gain, shift, b_dense, b_up, b_down, w_dense, w_up, w_down, *qkv):
    vm = pl.BlockSpec(memory_space=pltpu.VMEM)
    hbm = pl.BlockSpec(memory_space=pltpu.HBM)
    if layer == 0:
        in_specs = [vm] * 7 + [hbm] * 3 + [vm, hbm]
        out_shape = (jax.ShapeDtypeStruct((ROWS, D), f32), jax.ShapeDtypeStruct((NCH, NB, QC), f32))
        out_specs = (vm, vm)
    else:
        in_specs = [vm] * 7 + [hbm] * 3
        out_shape = jax.ShapeDtypeStruct((NB, D), bf16)
        out_specs = vm
    return pl.pallas_call(
        functools.partial(rest_kernel, layer),
        out_shape=out_shape,
        in_specs=in_specs,
        out_specs=out_specs,
        scratch_shapes=[
            pltpu.VMEM((DR, D), bf16),
            pltpu.VMEM((NCH, CW, F_LOC), bf16),
            pltpu.VMEM((M_LOC, D), bf16),
            pltpu.VMEM((3, MSG, HD), f32),
            pltpu.VMEM((2, MSG, HD), f32),
            pltpu.VMEM((HALF, DR), f32),
            pltpu.VMEM((2, NCH, HALF, CW), f32),
            pltpu.VMEM((2, NCH, ROWS, CW), f32),
            pltpu.VMEM((2, NCH, ROWS, CW), f32),
            pltpu.VMEM((2, NCH, ROWS, CW), f32),
            pltpu.VMEM((NCH, HALF, CW), f32),
            pltpu.VMEM((NCH, NB, QC if layer == 0 else CW), f32),
            pltpu.VMEM((ROWS, D), f32),
            pltpu.VMEM((HALF, F_LOC), f32),
            pltpu.VMEM((HALF, M_LOC), bf16),
            pltpu.SemaphoreType.DMA((2 + 2 * NCH,)),
            pltpu.SemaphoreType.DMA((2, 3)),
            pltpu.SemaphoreType.DMA((2, 2, NCH)),
            pltpu.SemaphoreType.DMA((2, 2, NCH)),
            pltpu.SemaphoreType.DMA((2, NCH)),
            pltpu.SemaphoreType.DMA((2, 3, NCH)),
        ],
        compiler_params=pltpu.CompilerParams(vmem_limit_bytes=VMEM_BYTES, collective_id=layer, has_side_effects=True),
        name=f'rest{layer}',
    )(msg, x, gain, shift, b_dense, b_up, b_down, w_dense, w_up, w_down, *qkv)


def solution(mesh):
    cache_spec = P(None, 'dp', 'sp', 'tp', None)
    in_specs = (P('dp', None), P('dp'), cache_spec, cache_spec, P(), P(), P(None, None, 'tp'), P(None, 'tp'), P(None, 'tp', None), P(), P(None, None, 'tp'), P(None, 'tp'), P(None, 'tp', None), P())
    out_specs = (P('dp', None), cache_spec, cache_spec)

    def device_step(hidden, positions, k_cache, v_cache, ln_gain, ln_bias, w_qkv, b_qkv, w_dense, b_dense, w_up, b_up, w_down, b_down):
        shape = k_cache.shape
        flat = (2, NB, SLOTS * KVL, HD)
        k_cache = k_cache.reshape(flat)
        v_cache = v_cache.reshape(flat)
        shared = (ln_gain, ln_bias, b_dense, b_up, b_down, w_dense, w_up, w_down)
        msg, *caches = attn_call(0, positions, (hidden, ln_gain, ln_bias, b_qkv, w_qkv), k_cache, v_cache, None)
        rows, qkv = rest_call(0, msg, hidden, *shared, b_qkv, w_qkv)
        msg, *caches = attn_call(1, positions, (qkv,), k_cache, v_cache, caches)
        hidden = rest_call(1, msg, rows, *shared)
        return hidden, caches[0].reshape(shape), caches[1].reshape(shape)

    return jax.shard_map(device_step, mesh=mesh, in_specs=in_specs, out_specs=out_specs, check_vma=False)
```

```python
import functools
import math

import jax
import jax.numpy as jnp
from jax import lax
from jax.experimental import pallas as pl
from jax.experimental.pallas import tpu as pltpu
from jax.sharding import PartitionSpec as P

BLOCK_SIZE = 64
LOCAL_BLOCKS = 16
VERT_STRIDE = 8
ROPE_THETA = 1000000.0
GELU_LIMIT = 20.0
NORM_EPS = 0.00001
MASKED = -1e30
MESH = pl.DeviceIdType.MESH

NB = 64
D = 3072
HD = 128
KVL = 4
GRP = 3
SLOTS = 64
QW = KVL * (GRP + 2) * HD
QROWS = 16
KCH = 6
KCS = D // KCH
G = 8
NG = NB // G
HALF = NB // 2
HPC = 6
MSG = HPC * HALF + 8
ROWS = HALF // 2
F_LOC = 4096
M_LOC = F_LOC // 2
NCH = 6
CW = D // NCH
QCH = 4
QC = QW // QCH
DR = HPC * HD
LAG = 2
VMEM_BYTES = 52 * 1024 * 1024

f32 = jnp.float32
bf16 = jnp.bfloat16


def norm_rows(rows, gain, shift):
    mean = jnp.mean(rows, axis=-1, keepdims=True)
    cent = rows - mean
    var = jnp.mean(jnp.square(cent), axis=-1, keepdims=True)
    return (cent * lax.rsqrt(var + NORM_EPS)) * gain + shift


def rope_tables(pos):
    half = HD // 2
    row = lax.broadcasted_iota(jnp.int32, (8, HD), 0)
    lane = lax.broadcasted_iota(jnp.int32, (NB, HD), 1)
    groups = []
    for i in range(NB // 8):
        at = jnp.zeros((8, HD), jnp.int32)
        for r in range(8):
            at = jnp.where(row == r, pos[i * 8 + r], at)
        groups.append(at)
    where = jnp.concatenate(groups, axis=0).astype(f32)
    power = (lane % half).astype(f32) * (2.0 / HD)
    angles = where * jnp.exp(power * -math.log(ROPE_THETA))
    sin = jnp.sin(angles)
    return jnp.cos(angles), jnp.where(lane < half, -sin, sin)


def attn_kernel(layer, pos, *rest):
    if layer == 0:
        x, gain, shift, b_qkv, w_hbm, kc_hbm, vc_hbm, *rest = rest
    else:
        acc, kc_hbm, vc_hbm, _, _, *rest = rest
    msg, ko_hbm, vo_hbm, kbuf, vbuf, qs, kns, vns, os, ms, ls, ksem, vsem, osem, *rest = rest
    sp = lax.axis_index('sp')
    tp = lax.axis_index('tp')
    base = sp * SLOTS

    def in_copy(hbm, buf, sem, i):
        return pltpu.make_async_copy(hbm.at[layer, pl.ds(i * G, G)], buf.at[pl.ds(i * G, G)], sem.at[i])

    def out_copy(buf, hbm, j, i):
        return pltpu.make_async_copy(buf.at[pl.ds(i * G, G)], hbm.at[layer, pl.ds(i * G, G)], osem.at[j, i])

    def fetch_cache():
        for i in range(NG):
            in_copy(kc_hbm, kbuf, ksem, i).start(priority=0)
            in_copy(vc_hbm, vbuf, vsem, i).start(priority=1)

    if layer == 0:
        w, u, acc, wsem, *places, small_sem = rest
        small = [pltpu.make_async_copy(src, dst, small_sem.at[i]) for i, (src, dst) in enumerate(zip((pos, x, gain, shift, b_qkv), places))]
        for copy in small:
            copy.start()
        pos, x, gain, shift, b_qkv = places

        def w_copy(i):
            return pltpu.make_async_copy(w_hbm.at[layer, pl.ds(i * KCS, KCS), :], w.at[i], wsem.at[i])

        for i in range(KCH):
            w_copy(i).start(priority=i % 2)
        fetch_cache()
        for copy in small:
            copy.wait()
        g_row = gain[layer, 0:1, :].astype(f32)
        s_row = shift[layer, 0:1, :].astype(f32)
        for i in range(NB // 16):
            rows = x[pl.ds(i * 16, 16), :].astype(f32)
            normed = norm_rows(rows, g_row, s_row).astype(bf16)
            for j in range(KCH):
                u[j, pl.ds(i * 16, 16), :] = normed[:, j * KCS:(j + 1) * KCS]
        acc[...] = jnp.broadcast_to(b_qkv[layer:layer + 1, :].astype(f32), (NB, QW))
    else:
        fetch_cache()
    qs[...] = jnp.zeros_like(qs)
    cos_t, sin_t = rope_tables(pos)
    if layer == 0:
        def qkv_step(i, carry):
            w_copy(i).wait()
            acc[...] += jnp.dot(u[i], w[i], preferred_element_type=f32)
            return carry

        lax.fori_loop(0, KCH, qkv_step, 0)

    for c in range(KVL):
        for j in range(GRP + 2):
            if layer == 0:
                col = (c * (GRP + 2) + j) * HD
                tile = acc[:, col:col + HD]
            else:
                tile = acc[c, :, j * HD:(j + 1) * HD]
            if j <= GRP:
                tile = tile * cos_t + pltpu.roll(tile, HD // 2, 1) * sin_t
            for i in range(NB // 8):
                part = tile[i * 8:(i + 1) * 8]
                if j < GRP:
                    qs[pl.ds(i * 8 * QROWS + c * GRP + j, 8, stride=QROWS), :] = part
                else:
                    dst = kns if j == GRP else vns
                    dst[pl.ds(i * 64 + c, 8, stride=8), :] = part
                    dst[pl.ds(i * 64 + c + 4, 8, stride=8), :] = part

    row_h = lax.broadcasted_iota(jnp.int32, (QROWS, SLOTS * KVL), 0)
    col_i = lax.broadcasted_iota(jnp.int32, (QROWS, SLOTS * KVL), 1)
    slot_of = jnp.where(row_h // GRP == col_i % KVL, col_i // KVL, 1 << 20)
    head_id = tp * KVL * GRP + row_h
    vertical = (sp + head_id + 1) % VERT_STRIDE == 0
    sub_row = lax.broadcasted_iota(jnp.int32, (16, HD), 0) // KVL

    def attn_step(i, carry):
        in_copy(kc_hbm, kbuf, ksem, i).wait()
        in_copy(vc_hbm, vbuf, vsem, i).wait()
        limits = []
        for bi in range(G):
            b = i * G + bi
            p = pos[b]
            pl_ = p - base
            pc = jnp.clip(pl_, 0, SLOTS - 1)
            hit = jnp.logical_and(pl_ >= 0, pl_ < SLOTS)
            sub = jnp.where(hit, pc % KVL, -1)
            r0 = pl.multiple_of((pc // KVL) * 16, 16)
            put = sub_row == sub
            for buf, new in ((kbuf, kns), (vbuf, vns)):
                new8 = new[pl.ds(pl.multiple_of(b * 8, 8), 8), :]
                new16 = jnp.concatenate([new8, new8], axis=0)
                old = buf[b, pl.ds(r0, 16), :].astype(f32)
                buf[b, pl.ds(r0, 16), :] = jnp.where(put, new16, old).astype(bf16)
            if layer == 0:
                near = p // BLOCK_SIZE - sp < LOCAL_BLOCKS
                limits.append(jnp.where(vertical, pl_, jnp.where(near, pl_, -1)))
            else:
                limits.append(pl_)
        scores = []
        for bi in range(G):
            b = i * G + bi
            q = qs[pl.ds(pl.multiple_of(b * QROWS, QROWS), QROWS), :].astype(bf16)
            scores.append(lax.dot_general(q, kbuf[b], (((1,), (1,)), ((), ())), preferred_element_type=f32))
        keeps = [slot_of <= limit for limit in limits]
        scores = [jnp.where(keep, s * (1.0 / HD), MASKED) for keep, s in zip(keeps, scores)]
        peaks = [jnp.max(s, axis=1, keepdims=True) for s in scores]
        weights = [jnp.where(keep, jnp.exp(s - peak), 0.0) for keep, s, peak in zip(keeps, scores, peaks)]
        outs = [jnp.dot(wt.astype(bf16), vbuf[i * G + bi], preferred_element_type=f32) for bi, wt in enumerate(weights)]
        sums = [jnp.sum(wt, axis=1, keepdims=True) for wt in weights]
        for bi in range(G):
            rows = pl.ds(pl.multiple_of((i * G + bi) * QROWS, QROWS), QROWS)
            ms[rows, :] = jnp.broadcast_to(peaks[bi], (QROWS, HD))
            ls[rows, :] = jnp.broadcast_to(sums[bi], (QROWS, HD))
            os[rows, :] = outs[bi]

        out_copy(kbuf, ko_hbm, 0, i).start()
        out_copy(vbuf, vo_hbm, 1, i).start(priority=1)
        return carry

    lax.fori_loop(0, NG, attn_step, 0)

    lane = lax.broadcasted_iota(jnp.int32, (8, HD), 1)
    for half in range(2):
        for c in range(2):
            stat = jnp.zeros((8, HD), f32)
            for g in range(HPC):
                for i in range(HALF // 8):
                    rows = pl.ds((half * HALF + i * 8) * QROWS + c * HPC + g, 8, stride=QROWS)
                    at = 2 * (g * (HALF // 8) + i)
                    msg[half * 2 + c, pl.ds(g * HALF + i * 8, 8), :] = os[rows, :]
                    stat = jnp.where(lane == at, ms[rows, :], stat)
                    stat = jnp.where(lane == at + 1, ls[rows, :], stat)
            msg[half * 2 + c, pl.ds(HPC * HALF, 8), :] = stat
    for i in range(NG):
        out_copy(kbuf, ko_hbm, 0, i).wait()
        out_copy(vbuf, vo_hbm, 1, i).wait()


def attn_call(layer, pos, operands, k_cache, v_cache, prev):
    vm = pl.BlockSpec(memory_space=pltpu.VMEM)
    hbm = pl.BlockSpec(memory_space=pltpu.HBM)
    args = [pos, *operands, k_cache, v_cache]
    if layer == 0:
        specs = [hbm] * 8
        alias = {}
        extra = [
            pltpu.VMEM((KCH, KCS, QW), bf16),
            pltpu.VMEM((KCH, NB, KCS), bf16),
            pltpu.VMEM((NB, QW), f32),
            pltpu.SemaphoreType.DMA((KCH,)),
            pltpu.SMEM(pos.shape, jnp.int32),
            *[pltpu.VMEM(arr.shape, bf16) for arr in operands[:4]],
            pltpu.SemaphoreType.DMA((5,)),
        ]
        limit = 60 * 1024 * 1024
    else:
        args += list(prev)
        specs = [pl.BlockSpec(memory_space=pltpu.SMEM), vm] + [hbm] * 4
        alias = {4: 1, 5: 2}
        extra = []
        limit = VMEM_BYTES
    cache = jax.ShapeDtypeStruct(k_cache.shape, bf16)
    return pl.pallas_call(
        functools.partial(attn_kernel, layer),
        out_shape=(jax.ShapeDtypeStruct((KVL, MSG, HD), f32), cache, cache),
        in_specs=specs,
        out_specs=(vm, hbm, hbm),
        scratch_shapes=[
            pltpu.VMEM((NB, SLOTS * KVL, HD), bf16),
            pltpu.VMEM((NB, SLOTS * KVL, HD), bf16),
            pltpu.VMEM((NB * QROWS, HD), f32),
            pltpu.VMEM((NB * 8, HD), f32),
            pltpu.VMEM((NB * 8, HD), f32),
            pltpu.VMEM((NB * QROWS, HD), f32),
            pltpu.VMEM((NB * QROWS, HD), f32),
            pltpu.VMEM((NB * QROWS, HD), f32),
            pltpu.SemaphoreType.DMA((NG,)),
            pltpu.SemaphoreType.DMA((NG,)),
            pltpu.SemaphoreType.DMA((2, NG)),
            *extra,
        ],
        input_output_aliases=alias,
        compiler_params=pltpu.CompilerParams(vmem_limit_bytes=limit),
        name=f'attn{layer}',
    )(*args)


def rest_kernel(layer, msg, x, gain, shift, b_dense, b_up, b_down, wd_hbm, wu_hbm, wn_hbm, *rest):
    if layer == 0:
        b_qkv, wq_hbm, x_out, out, *rest = rest
    else:
        out, *rest = rest
    (wd, wu, wn, got, sent, o_buf, part, pair, sums, other, ag, full, xrow, up, mbuf,
     wsem, a_sem, d_sem, y_sem, g_sem, x_sem) = rest
    dp = lax.axis_index('dp')
    tp = lax.axis_index('tp')
    sp = lax.axis_index('sp')
    core = sp % 2
    cx = sp // 2
    ox = 1 - cx
    mate = (dp, tp, cx * 2 + 1 - core)
    x_dev = (dp, tp, ox * 2 + core)
    y_dev = (dp, 1 - tp, sp)

    def load(src, dst, i):
        return pltpu.make_async_copy(src, dst, wsem.at[i])

    wd_copy = load(wd_hbm.at[layer, pl.ds(pl.multiple_of(core * DR, DR), DR), :], wd, 0)

    def wu_copy(i):
        return load(wu_hbm.at[layer, pl.ds(i * CW, CW), pl.ds(pl.multiple_of(core * F_LOC, F_LOC), F_LOC)], wu.at[i], 1 + i)

    wn_copy = load(wn_hbm.at[layer, pl.ds(pl.multiple_of(core * M_LOC, M_LOC), M_LOC), :], wn, 1 + NCH)

    def wq_copy(i):
        return load(wq_hbm.at[1, pl.ds(i * CW, CW), :], wu.at[i, :, pl.ds(0, QW)], 2 + NCH + i)

    barrier = pltpu.get_barrier_semaphore()
    for peer in (mate, x_dev, y_dev):
        pl.semaphore_signal(barrier, inc=1, device_id=peer, device_id_type=MESH)
    wd_copy.start()
    for i in range(NCH):
        wu_copy(i).start()
    wn_copy.start()
    pl.semaphore_wait(barrier, 3)

    def remote(src, dst, sems, idx, peer):
        return pltpu.make_async_remote_copy(
            src_ref=src, dst_ref=dst, send_sem=sems.at[(0,) + idx], recv_sem=sems.at[(1,) + idx],
            device_id=peer, device_id_type=MESH)

    near = cx * 2 + core
    far = ox * 2 + core
    swap = [remote(msg.at[ox * 2 + 1 - core], got.at[0], a_sem, (0,), mate),
            remote(msg.at[cx * 2 + 1 - core], got.at[1], a_sem, (1,), mate)]
    for copy in swap:
        copy.start()

    gain1 = gain[layer, 1:2, :].astype(f32)
    shift1 = shift[layer, 1:2, :].astype(f32)
    own = pl.ds(pl.multiple_of(core * ROWS, ROWS), ROWS)
    theirs = pl.ds(pl.multiple_of((1 - core) * ROWS, ROWS), ROWS)

    def all_rows(x_, c_):
        return pl.ds(pl.multiple_of(x_ * HALF + c_ * ROWS, ROWS), ROWS)

    xrow[...] = x[all_rows(cx, core), :].astype(f32) if layer == 0 else x[...]
    lane = lax.broadcasted_iota(jnp.int32, (8, HD), 1)

    def merge(one, two, put, stat_out=None):
        stats = [ref[pl.ds(HPC * HALF, 8), :] for ref in (one, two)]
        new_stat = jnp.zeros((8, HD), f32)
        for g in range(HPC):
            for i in range(HALF // 8):
                at = 2 * (g * (HALF // 8) + i)
                peaks = [jnp.broadcast_to(st[:, at:at + 1], (8, HD)) for st in stats]
                tots = [jnp.broadcast_to(st[:, at + 1:at + 2], (8, HD)) for st in stats]
                top = jnp.maximum(peaks[0], peaks[1])
                scale = [jnp.exp(p - top) for p in peaks]
                rows = pl.ds(g * HALF + i * 8, 8)
                num = one[rows, :] * scale[0] + two[rows, :] * scale[1]
                den = tots[0] * scale[0] + tots[1] * scale[1]
                put(g, i, num, den)
                if stat_out is not None:
                    new_stat = jnp.where(lane == at, top, new_stat)
                    new_stat = jnp.where(lane == at + 1, den, new_stat)
        if stat_out is not None:
            stat_out[pl.ds(HPC * HALF, 8), :] = new_stat

    def put_part(ref):
        def put(g, i, num, den):
            ref[pl.ds(g * HALF + i * 8, 8), :] = num
        return put

    def put_out(g, i, num, den):
        o_buf[pl.ds(i * 8, 8), g * HD:(g + 1) * HD] = num / den

    swap[0].wait_recv()
    merge(msg.at[far], got.at[0], put_part(sent.at[0]), sent.at[0])
    cross = remote(sent.at[0], got.at[2], a_sem, (2,), x_dev)
    cross.start()
    swap[1].wait_recv()
    merge(msg.at[near], got.at[1], put_part(sent.at[1]), sent.at[1])
    cross.wait_recv()
    merge(sent.at[1], got.at[2], put_out)
    sends = swap + [cross]

    def reduce(ph, product, finish):
        first = [remote(part.at[ph, n, theirs, :], pair.at[ph, n], d_sem, (ph, n), mate) for n in range(NCH)]
        second = [remote(sums.at[ph, n], other.at[ph, n], y_sem, (ph, n), y_dev) for n in range(NCH)]
        for step in range(NCH + LAG):
            if step < NCH:
                part[ph, step] = product(step)
                first[step].start()
            if step >= LAG:
                n = step - LAG
                first[n].wait_recv()
                sums[ph, n] = part[ph, n, own, :] + pair[ph, n]
                second[n].start()
        for n in range(NCH):
            second[n].wait_recv()
            finish(n, sums[ph, n] + other[ph, n])
        return first + second

    def residual(n, total, bias):
        cols = slice(n * CW, (n + 1) * CW)
        v = xrow[:, cols] + total + bias[layer:layer + 1, cols].astype(f32)
        xrow[:, cols] = v.astype(bf16).astype(f32)

    wd_copy.wait()
    o = o_buf[...].astype(bf16)
    sends += reduce(0, lambda n: jnp.dot(o, wd[:, n * CW:(n + 1) * CW], preferred_element_type=f32),
                   lambda n, total: residual(n, total, b_dense))

    normed = norm_rows(xrow[...], gain1, shift1).astype(bf16).astype(f32)
    swap = []
    for n in range(NCH):
        ag[n, own, :] = normed[:, n * CW:(n + 1) * CW]
        here = ag.at[n, own, :]
        swap.append(remote(here, here, g_sem, (n,), mate))
        swap[n].start()
    cols_up = pl.ds(pl.multiple_of(core * F_LOC, F_LOC), F_LOC)
    up[...] = jnp.broadcast_to(b_up[layer:layer + 1, cols_up].astype(f32), (HALF, F_LOC))
    for n in range(NCH):
        wu_copy(n).wait()
        swap[n].wait_recv()
        up[...] += jnp.dot(ag[n].astype(bf16), wu[n], preferred_element_type=f32)
        if layer == 0:
            wq_copy(n).start()

    pick = (lax.broadcasted_iota(jnp.int32, (256, 128), 0) == 2 * lax.broadcasted_iota(jnp.int32, (256, 128), 1))
    pick = jnp.where(pick, 1.0, 0.0).astype(bf16)
    for k in range(F_LOC // 256):
        a = up[:, k * 256:(k + 1) * 256]
        z = jnp.minimum(a, GELU_LIMIT)
        gate = z * jax.nn.sigmoid(1.702 * z)
        lin = jnp.clip(a, -GELU_LIMIT, GELU_LIMIT) + 1.0
        prod = (gate * pltpu.roll(lin, 255, 1)).astype(bf16)
        mbuf[:, k * 128:(k + 1) * 128] = jnp.dot(prod, pick, preferred_element_type=f32).astype(bf16)
    wn_copy.wait()
    m = mbuf[...]
    sends += swap

    def spread(n, value):
        full[n, all_rows(cx, core), :] = value
        here = full.at[n, all_rows(cx, core), :]
        for k, peer in enumerate((x_dev, mate)):
            copy = remote(here, here, x_sem, (k, n), peer)
            copy.start()
            sends.append(copy)

    def collect(chunks, use):
        for n in range(chunks):
            there = full.at[n, all_rows(ox, core), :]
            remote(there, there, x_sem, (0, n), x_dev).wait_recv()
            copy = remote(there, there, x_sem, (2, n), mate)
            copy.start()
            sends.append(copy)
        for n in range(chunks):
            for k, x_ in ((1, cx), (2, ox)):
                there = full.at[n, all_rows(x_, 1 - core), :]
                remote(there, there, x_sem, (k, n), mate).wait_recv()
            use(n)

    def take_down(n, total):
        residual(n, total, b_down)
        if layer == 1:
            spread(n, xrow[:, n * CW:(n + 1) * CW])

    sends += reduce(1, lambda n: jnp.dot(m, wn[:, n * CW:(n + 1) * CW], preferred_element_type=f32), take_down)
    if layer == 0:
        x_out[...] = xrow[...]
        u = norm_rows(xrow[...], gain[1, 0:1, :].astype(f32), shift[1, 0:1, :].astype(f32)).astype(bf16)
        for i in range(NCH):
            wq_copy(i).wait()
        for n in range(QCH):
            cols = slice(n * QC, (n + 1) * QC)
            r = jnp.broadcast_to(b_qkv[1:2, cols].astype(f32), (ROWS, QC))
            for i in range(NCH):
                r += jnp.dot(u[:, i * CW:(i + 1) * CW], wu[i, :, cols], preferred_element_type=f32)
            spread(n, r)

        def use(n):
            out[n] = full[n]
    else:
        def use(n):
            out[:, n * CW:(n + 1) * CW] = full[n].astype(bf16)

    collect(QCH if layer == 0 else NCH, use)
    for copy in sends:
        copy.wait_send()


def rest_call(layer, msg, x, gain, shift, b_dense, b_up, b_down, w_dense, w_up, w_down, *qkv):
    vm = pl.BlockSpec(memory_space=pltpu.VMEM)
    hbm = pl.BlockSpec(memory_space=pltpu.HBM)
    if layer == 0:
        in_specs = [vm] * 7 + [hbm] * 3 + [vm, hbm]
        out_shape = (jax.ShapeDtypeStruct((ROWS, D), f32), jax.ShapeDtypeStruct((QCH, NB, QC), f32))
        out_specs = (vm, vm)
    else:
        in_specs = [vm] * 7 + [hbm] * 3
        out_shape = jax.ShapeDtypeStruct((NB, D), bf16)
        out_specs = vm
    return pl.pallas_call(
        functools.partial(rest_kernel, layer),
        out_shape=out_shape,
        in_specs=in_specs,
        out_specs=out_specs,
        scratch_shapes=[
            pltpu.VMEM((DR, D), bf16),
            pltpu.VMEM((NCH, CW, F_LOC), bf16),
            pltpu.VMEM((M_LOC, D), bf16),
            pltpu.VMEM((3, MSG, HD), f32),
            pltpu.VMEM((2, MSG, HD), f32),
            pltpu.VMEM((HALF, DR), f32),
            pltpu.VMEM((2, NCH, HALF, CW), f32),
            pltpu.VMEM((2, NCH, ROWS, CW), f32),
            pltpu.VMEM((2, NCH, ROWS, CW), f32),
            pltpu.VMEM((2, NCH, ROWS, CW), f32),
            pltpu.VMEM((NCH, HALF, CW), f32),
            pltpu.VMEM((QCH, NB, QC) if layer == 0 else (NCH, NB, CW), f32),
            pltpu.VMEM((ROWS, D), f32),
            pltpu.VMEM((HALF, F_LOC), f32),
            pltpu.VMEM((HALF, M_LOC), bf16),
            pltpu.SemaphoreType.DMA((2 + 2 * NCH,)),
            pltpu.SemaphoreType.DMA((2, 3)),
            pltpu.SemaphoreType.DMA((2, 2, NCH)),
            pltpu.SemaphoreType.DMA((2, 2, NCH)),
            pltpu.SemaphoreType.DMA((2, NCH)),
            pltpu.SemaphoreType.DMA((2, 3, NCH)),
        ],
        compiler_params=pltpu.CompilerParams(vmem_limit_bytes=VMEM_BYTES, collective_id=layer, has_side_effects=True),
        name=f'rest{layer}',
    )(msg, x, gain, shift, b_dense, b_up, b_down, w_dense, w_up, w_down, *qkv)


def solution(mesh):
    cache_spec = P(None, 'dp', 'sp', 'tp', None)
    in_specs = (P('dp', None), P('dp'), cache_spec, cache_spec, P(), P(), P(None, None, 'tp'), P(None, 'tp'), P(None, 'tp', None), P(), P(None, None, 'tp'), P(None, 'tp'), P(None, 'tp', None), P())
    out_specs = (P('dp', None), cache_spec, cache_spec)

    def device_step(hidden, positions, k_cache, v_cache, ln_gain, ln_bias, w_qkv, b_qkv, w_dense, b_dense, w_up, b_up, w_down, b_down):
        shape = k_cache.shape
        flat = (2, NB, SLOTS * KVL, HD)
        k_cache = k_cache.reshape(flat)
        v_cache = v_cache.reshape(flat)
        shared = (ln_gain, ln_bias, b_dense, b_up, b_down, w_dense, w_up, w_down)
        msg, *caches = attn_call(0, positions, (hidden, ln_gain, ln_bias, b_qkv, w_qkv), k_cache, v_cache, None)
        rows, qkv = rest_call(0, msg, hidden, *shared, b_qkv, w_qkv)
        msg, *caches = attn_call(1, positions, (qkv,), k_cache, v_cache, caches)
        hidden = rest_call(1, msg, rows, *shared)
        return hidden, caches[0].reshape(shape), caches[1].reshape(shape)

    return jax.shard_map(device_step, mesh=mesh, in_specs=in_specs, out_specs=out_specs, check_vma=False)
```

```python
import functools
import math

import jax
import jax.numpy as jnp
from jax import lax
from jax.experimental import pallas as pl
from jax.experimental.pallas import tpu as pltpu
from jax.sharding import PartitionSpec as P

BLOCK_SIZE = 64
LOCAL_BLOCKS = 16
VERT_STRIDE = 8
ROPE_THETA = 1000000.0
GELU_LIMIT = 20.0
NORM_EPS = 0.00001
MASKED = -1e30
MESH = pl.DeviceIdType.MESH

NB = 64
D = 3072
HD = 128
KVL = 4
GRP = 3
SLOTS = 64
QW = KVL * (GRP + 2) * HD
QROWS = 16
KCH = 6
KCS = D // KCH
G = 8
NG = NB // G
GS = 16
HALF = NB // 2
HPC = 6
MSG = HPC * HALF + 8
ROWS = HALF // 2
F_LOC = 4096
M_LOC = F_LOC // 2
NCH = 6
CW = D // NCH
QCH = 4
QC = QW // QCH
DR = HPC * HD
RCH = 12
RW = D // RCH
LAG = 5
VMEM_BYTES = 52 * 1024 * 1024

f32 = jnp.float32
bf16 = jnp.bfloat16


def norm_rows(rows, gain, shift):
    mean = jnp.mean(rows, axis=-1, keepdims=True)
    cent = rows - mean
    var = jnp.mean(jnp.square(cent), axis=-1, keepdims=True)
    return (cent * lax.rsqrt(var + NORM_EPS)) * gain + shift


def rope_tables(pos):
    half = HD // 2
    row = lax.broadcasted_iota(jnp.int32, (8, HD), 0)
    lane = lax.broadcasted_iota(jnp.int32, (NB, HD), 1)
    groups = []
    for i in range(NB // 8):
        at = jnp.zeros((8, HD), jnp.int32)
        for r in range(8):
            at = jnp.where(row == r, pos[i * 8 + r], at)
        groups.append(at)
    where = jnp.concatenate(groups, axis=0).astype(f32)
    power = (lane % half).astype(f32) * (2.0 / HD)
    angles = where * jnp.exp(power * -math.log(ROPE_THETA))
    sin = jnp.sin(angles)
    return jnp.cos(angles), jnp.where(lane < half, -sin, sin)


def attn_kernel(layer, pos, *rest):
    if layer == 0:
        x, gain, shift, b_qkv, w_hbm, kc_hbm, vc_hbm, *rest = rest
    else:
        acc, kc_hbm, vc_hbm, _, _, *rest = rest
    msg, ko_hbm, vo_hbm, kbuf, vbuf, qs, kns, vns, os, ms, ls, ksem, vsem, osem, *rest = rest
    sp = lax.axis_index('sp')
    tp = lax.axis_index('tp')
    base = sp * SLOTS

    def in_copy(hbm, buf, sem, i):
        return pltpu.make_async_copy(hbm.at[layer, pl.ds(i * G, G)], buf.at[pl.ds(i * G, G)], sem.at[i])

    def out_copy(buf, hbm, j, i):
        return pltpu.make_async_copy(buf.at[pl.ds(i * G, G)], hbm.at[layer, pl.ds(i * G, G)], osem.at[j, i])

    def fetch_cache():
        for i in range(NG):
            in_copy(kc_hbm, kbuf, ksem, i).start(priority=0)
            in_copy(vc_hbm, vbuf, vsem, i).start(priority=1)

    if layer == 0:
        w, u, acc, wsem, *places, small_sem = rest
        small = [pltpu.make_async_copy(src, dst, small_sem.at[i]) for i, (src, dst) in enumerate(zip((pos, x, gain, shift, b_qkv), places))]
        for copy in small:
            copy.start()
        pos, x, gain, shift, b_qkv = places

        def w_copy(i):
            return pltpu.make_async_copy(w_hbm.at[layer, pl.ds(i * KCS, KCS), :], w.at[i], wsem.at[i])

        for i in range(KCH):
            w_copy(i).start(priority=i % 2)
        fetch_cache()
        for copy in small:
            copy.wait()
        g_row = gain[layer, 0:1, :].astype(f32)
        s_row = shift[layer, 0:1, :].astype(f32)
        for i in range(NB // 16):
            rows = x[pl.ds(i * 16, 16), :].astype(f32)
            normed = norm_rows(rows, g_row, s_row).astype(bf16)
            for j in range(KCH):
                u[j, pl.ds(i * 16, 16), :] = normed[:, j * KCS:(j + 1) * KCS]
        acc[...] = jnp.broadcast_to(b_qkv[layer:layer + 1, :].astype(f32), (NB, QW))
    else:
        fetch_cache()
    qs[...] = jnp.zeros_like(qs)
    cos_t, sin_t = rope_tables(pos)
    if layer == 0:
        def qkv_step(i, carry):
            w_copy(i).wait()
            acc[...] += jnp.dot(u[i], w[i], preferred_element_type=f32)
            return carry

        lax.fori_loop(0, KCH, qkv_step, 0)

    for c in range(KVL):
        for j in range(GRP + 2):
            if layer == 0:
                col = (c * (GRP + 2) + j) * HD
                tile = acc[:, col:col + HD]
            else:
                tile = acc[c, :, j * HD:(j + 1) * HD]
            if j <= GRP:
                tile = tile * cos_t + pltpu.roll(tile, HD // 2, 1) * sin_t
            for i in range(NB // 8):
                part = tile[i * 8:(i + 1) * 8]
                if j < GRP:
                    qs[pl.ds(i * 8 * QROWS + c * GRP + j, 8, stride=QROWS), :] = part
                else:
                    dst = kns if j == GRP else vns
                    dst[pl.ds(i * 64 + c, 8, stride=8), :] = part
                    dst[pl.ds(i * 64 + c + 4, 8, stride=8), :] = part

    row_h = lax.broadcasted_iota(jnp.int32, (QROWS, SLOTS * KVL), 0)
    col_i = lax.broadcasted_iota(jnp.int32, (QROWS, SLOTS * KVL), 1)
    slot_of = jnp.where(row_h // GRP == col_i % KVL, col_i // KVL, 1 << 20)
    head_id = tp * KVL * GRP + row_h
    vertical = (sp + head_id + 1) % VERT_STRIDE == 0
    sub_row = lax.broadcasted_iota(jnp.int32, (16, HD), 0) // KVL

    def attn_step(i, carry):
        copies = [i * (GS // G) + j for j in range(GS // G)]
        for j in copies:
            in_copy(kc_hbm, kbuf, ksem, j).wait()
            in_copy(vc_hbm, vbuf, vsem, j).wait()
        limits = []
        for bi in range(GS):
            b = i * GS + bi
            p = pos[b]
            pl_ = p - base
            pc = jnp.clip(pl_, 0, SLOTS - 1)
            hit = jnp.logical_and(pl_ >= 0, pl_ < SLOTS)
            sub = jnp.where(hit, pc % KVL, -1)
            r0 = pl.multiple_of((pc // KVL) * 16, 16)
            put = sub_row == sub
            for buf, new in ((kbuf, kns), (vbuf, vns)):
                new8 = new[pl.ds(pl.multiple_of(b * 8, 8), 8), :]
                new16 = jnp.concatenate([new8, new8], axis=0)
                old = buf[b, pl.ds(r0, 16), :].astype(f32)
                buf[b, pl.ds(r0, 16), :] = jnp.where(put, new16, old).astype(bf16)
            if layer == 0:
                near = p // BLOCK_SIZE - sp < LOCAL_BLOCKS
                limits.append(jnp.where(vertical, pl_, jnp.where(near, pl_, -1)))
            else:
                limits.append(pl_)
        scores = []
        for bi in range(GS):
            b = i * GS + bi
            q = qs[pl.ds(pl.multiple_of(b * QROWS, QROWS), QROWS), :].astype(bf16)
            scores.append(lax.dot_general(q, kbuf[b], (((1,), (1,)), ((), ())), preferred_element_type=f32))
        keeps = [slot_of <= limit for limit in limits]
        scores = [jnp.where(keep, s * (1.0 / HD), MASKED) for keep, s in zip(keeps, scores)]
        peaks = [jnp.max(s, axis=1, keepdims=True) for s in scores]
        weights = [jnp.where(keep, jnp.exp(s - peak), 0.0) for keep, s, peak in zip(keeps, scores, peaks)]
        outs = [jnp.dot(wt.astype(bf16), vbuf[i * GS + bi], preferred_element_type=f32) for bi, wt in enumerate(weights)]
        sums = [jnp.sum(wt, axis=1, keepdims=True) for wt in weights]
        for bi in range(GS):
            rows = pl.ds(pl.multiple_of((i * GS + bi) * QROWS, QROWS), QROWS)
            ms[rows, :] = jnp.broadcast_to(peaks[bi], (QROWS, HD))
            ls[rows, :] = jnp.broadcast_to(sums[bi], (QROWS, HD))
            os[rows, :] = outs[bi]

        for j in copies:
            out_copy(kbuf, ko_hbm, 0, j).start()
            out_copy(vbuf, vo_hbm, 1, j).start(priority=1)
        return carry

    lax.fori_loop(0, NB // GS, attn_step, 0)

    lane = lax.broadcasted_iota(jnp.int32, (8, HD), 1)
    for half in range(2):
        for c in range(2):
            stat = jnp.zeros((8, HD), f32)
            for g in range(HPC):
                for i in range(HALF // 8):
                    rows = pl.ds((half * HALF + i * 8) * QROWS + c * HPC + g, 8, stride=QROWS)
                    at = 2 * (g * (HALF // 8) + i)
                    msg[half * 2 + c, pl.ds(g * HALF + i * 8, 8), :] = os[rows, :]
                    stat = jnp.where(lane == at, ms[rows, :], stat)
                    stat = jnp.where(lane == at + 1, ls[rows, :], stat)
            msg[half * 2 + c, pl.ds(HPC * HALF, 8), :] = stat
    for i in range(NG):
        out_copy(kbuf, ko_hbm, 0, i).wait()
        out_copy(vbuf, vo_hbm, 1, i).wait()


def attn_call(layer, pos, operands, k_cache, v_cache, prev):
    vm = pl.BlockSpec(memory_space=pltpu.VMEM)
    hbm = pl.BlockSpec(memory_space=pltpu.HBM)
    args = [pos, *operands, k_cache, v_cache]
    if layer == 0:
        specs = [hbm] * 8
        alias = {}
        extra = [
            pltpu.VMEM((KCH, KCS, QW), bf16),
            pltpu.VMEM((KCH, NB, KCS), bf16),
            pltpu.VMEM((NB, QW), f32),
            pltpu.SemaphoreType.DMA((KCH,)),
            pltpu.SMEM(pos.shape, jnp.int32),
            *[pltpu.VMEM(arr.shape, bf16) for arr in operands[:4]],
            pltpu.SemaphoreType.DMA((5,)),
        ]
        limit = 60 * 1024 * 1024
    else:
        args += list(prev)
        specs = [pl.BlockSpec(memory_space=pltpu.SMEM), vm] + [hbm] * 4
        alias = {4: 1, 5: 2}
        extra = []
        limit = VMEM_BYTES
    cache = jax.ShapeDtypeStruct(k_cache.shape, bf16)
    return pl.pallas_call(
        functools.partial(attn_kernel, layer),
        out_shape=(jax.ShapeDtypeStruct((KVL, MSG, HD), f32), cache, cache),
        in_specs=specs,
        out_specs=(vm, hbm, hbm),
        scratch_shapes=[
            pltpu.VMEM((NB, SLOTS * KVL, HD), bf16),
            pltpu.VMEM((NB, SLOTS * KVL, HD), bf16),
            pltpu.VMEM((NB * QROWS, HD), f32),
            pltpu.VMEM((NB * 8, HD), f32),
            pltpu.VMEM((NB * 8, HD), f32),
            pltpu.VMEM((NB * QROWS, HD), f32),
            pltpu.VMEM((NB * QROWS, HD), f32),
            pltpu.VMEM((NB * QROWS, HD), f32),
            pltpu.SemaphoreType.DMA((NG,)),
            pltpu.SemaphoreType.DMA((NG,)),
            pltpu.SemaphoreType.DMA((2, NG)),
            *extra,
        ],
        input_output_aliases=alias,
        compiler_params=pltpu.CompilerParams(vmem_limit_bytes=limit),
        name=f'attn{layer}',
    )(*args)


def rest_kernel(layer, msg, x, gain, shift, b_dense, b_up, b_down, wd_hbm, wu_hbm, wn_hbm, *rest):
    if layer == 0:
        b_qkv, wq_hbm, x_out, out, *rest = rest
    else:
        out, *rest = rest
    (wd, wu, wn, got, sent, o_buf, part, pair, sums, other, ag, full, xrow, up, mbuf,
     wsem, a_sem, d_sem, y_sem, g_sem, x_sem) = rest
    dp = lax.axis_index('dp')
    tp = lax.axis_index('tp')
    sp = lax.axis_index('sp')
    core = sp % 2
    cx = sp // 2
    ox = 1 - cx
    mate = (dp, tp, cx * 2 + 1 - core)
    x_dev = (dp, tp, ox * 2 + core)
    y_dev = (dp, 1 - tp, sp)

    def load(src, dst, i):
        return pltpu.make_async_copy(src, dst, wsem.at[i])

    wd_copy = load(wd_hbm.at[layer, pl.ds(pl.multiple_of(core * DR, DR), DR), :], wd, 0)

    def wu_copy(i):
        return load(wu_hbm.at[layer, pl.ds(i * CW, CW), pl.ds(pl.multiple_of(core * F_LOC, F_LOC), F_LOC)], wu.at[i], 1 + i)

    wn_copy = load(wn_hbm.at[layer, pl.ds(pl.multiple_of(core * M_LOC, M_LOC), M_LOC), :], wn, 1 + NCH)

    def wq_copy(i):
        return load(wq_hbm.at[1, pl.ds(i * CW, CW), :], wu.at[i, :, pl.ds(0, QW)], 2 + NCH + i)

    barrier = pltpu.get_barrier_semaphore()
    for peer in (mate, x_dev, y_dev):
        pl.semaphore_signal(barrier, inc=1, device_id=peer, device_id_type=MESH)
    wd_copy.start()
    for i in range(NCH):
        wu_copy(i).start()
    wn_copy.start()
    pl.semaphore_wait(barrier, 3)

    def remote(src, dst, sems, idx, peer):
        return pltpu.make_async_remote_copy(
            src_ref=src, dst_ref=dst, send_sem=sems.at[(0,) + idx], recv_sem=sems.at[(1,) + idx],
            device_id=peer, device_id_type=MESH)

    near = cx * 2 + core
    far = ox * 2 + core
    swap = [remote(msg.at[ox * 2 + 1 - core], got.at[0], a_sem, (0,), mate),
            remote(msg.at[cx * 2 + 1 - core], got.at[1], a_sem, (1,), mate)]
    for copy in swap:
        copy.start()

    gain1 = gain[layer, 1:2, :].astype(f32)
    shift1 = shift[layer, 1:2, :].astype(f32)
    own = pl.ds(pl.multiple_of(core * ROWS, ROWS), ROWS)
    theirs = pl.ds(pl.multiple_of((1 - core) * ROWS, ROWS), ROWS)

    def all_rows(x_, c_):
        return pl.ds(pl.multiple_of(x_ * HALF + c_ * ROWS, ROWS), ROWS)

    xrow[...] = x[all_rows(cx, core), :].astype(f32) if layer == 0 else x[...]
    lane = lax.broadcasted_iota(jnp.int32, (8, HD), 1)

    def merge(one, two, put, stat_out=None):
        stats = [ref[pl.ds(HPC * HALF, 8), :] for ref in (one, two)]
        new_stat = jnp.zeros((8, HD), f32)
        for g in range(HPC):
            for i in range(HALF // 8):
                at = 2 * (g * (HALF // 8) + i)
                peaks = [jnp.broadcast_to(st[:, at:at + 1], (8, HD)) for st in stats]
                tots = [jnp.broadcast_to(st[:, at + 1:at + 2], (8, HD)) for st in stats]
                top = jnp.maximum(peaks[0], peaks[1])
                scale = [jnp.exp(p - top) for p in peaks]
                rows = pl.ds(g * HALF + i * 8, 8)
                num = one[rows, :] * scale[0] + two[rows, :] * scale[1]
                den = tots[0] * scale[0] + tots[1] * scale[1]
                put(g, i, num, den)
                if stat_out is not None:
                    new_stat = jnp.where(lane == at, top, new_stat)
                    new_stat = jnp.where(lane == at + 1, den, new_stat)
        if stat_out is not None:
            stat_out[pl.ds(HPC * HALF, 8), :] = new_stat

    def put_part(ref):
        def put(g, i, num, den):
            ref[pl.ds(g * HALF + i * 8, 8), :] = num
        return put

    def put_out(g, i, num, den):
        o_buf[pl.ds(i * 8, 8), g * HD:(g + 1) * HD] = num / den

    swap[0].wait_recv()
    merge(msg.at[far], got.at[0], put_part(sent.at[0]), sent.at[0])
    cross = remote(sent.at[0], got.at[2], a_sem, (2,), x_dev)
    cross.start()
    swap[1].wait_recv()
    merge(msg.at[near], got.at[1], put_part(sent.at[1]), sent.at[1])
    cross.wait_recv()
    merge(sent.at[1], got.at[2], put_out)
    sends = swap + [cross]

    def reduce(ph, product, finish):
        first = [remote(part.at[ph, n, theirs, :], pair.at[ph, n], d_sem, (ph, n), mate) for n in range(RCH)]
        second = [remote(sums.at[ph, n], other.at[ph, n], y_sem, (ph, n), y_dev) for n in range(RCH)]
        for step in range(RCH + LAG):
            if step < RCH:
                part[ph, step] = product(step)
                first[step].start()
            if step >= LAG:
                n = step - LAG
                first[n].wait_recv()
                sums[ph, n] = part[ph, n, own, :] + pair[ph, n]
                second[n].start()
        for n in range(RCH):
            second[n].wait_recv()
            finish(n, sums[ph, n] + other[ph, n])
        return first + second

    def residual(n, total, bias):
        cols = slice(n * RW, (n + 1) * RW)
        v = xrow[:, cols] + total + bias[layer:layer + 1, cols].astype(f32)
        xrow[:, cols] = v.astype(bf16).astype(f32)

    wd_copy.wait()
    o = o_buf[...].astype(bf16)
    sends += reduce(0, lambda n: jnp.dot(o, wd[:, n * RW:(n + 1) * RW], preferred_element_type=f32),
                   lambda n, total: residual(n, total, b_dense))

    normed = norm_rows(xrow[...], gain1, shift1).astype(bf16).astype(f32)
    swap = []
    for n in range(NCH):
        ag[n, own, :] = normed[:, n * CW:(n + 1) * CW]
        here = ag.at[n, own, :]
        swap.append(remote(here, here, g_sem, (n,), mate))
        swap[n].start()
    cols_up = pl.ds(pl.multiple_of(core * F_LOC, F_LOC), F_LOC)
    up[...] = jnp.broadcast_to(b_up[layer:layer + 1, cols_up].astype(f32), (HALF, F_LOC))
    for n in range(NCH):
        wu_copy(n).wait()
        swap[n].wait_recv()
        up[...] += jnp.dot(ag[n].astype(bf16), wu[n], preferred_element_type=f32)
        if layer == 0:
            wq_copy(n).start()

    pick = (lax.broadcasted_iota(jnp.int32, (256, 128), 0) == 2 * lax.broadcasted_iota(jnp.int32, (256, 128), 1))
    pick = jnp.where(pick, 1.0, 0.0).astype(bf16)
    for k in range(F_LOC // 256):
        a = up[:, k * 256:(k + 1) * 256]
        z = jnp.minimum(a, GELU_LIMIT)
        gate = z * jax.nn.sigmoid(1.702 * z)
        lin = jnp.clip(a, -GELU_LIMIT, GELU_LIMIT) + 1.0
        prod = (gate * pltpu.roll(lin, 255, 1)).astype(bf16)
        mbuf[:, k * 128:(k + 1) * 128] = jnp.dot(prod, pick, preferred_element_type=f32).astype(bf16)
    wn_copy.wait()
    m = mbuf[...]
    sends += swap

    def spread(n, value):
        full[n, all_rows(cx, core), :] = value
        here = full.at[n, all_rows(cx, core), :]
        for k, peer in enumerate((x_dev, mate)):
            copy = remote(here, here, x_sem, (k, n), peer)
            copy.start()
            sends.append(copy)

    def collect(chunks, use):
        for n in range(chunks):
            there = full.at[n, all_rows(ox, core), :]
            remote(there, there, x_sem, (0, n), x_dev).wait_recv()
            copy = remote(there, there, x_sem, (2, n), mate)
            copy.start()
            sends.append(copy)
        for n in range(chunks):
            for k, x_ in ((1, cx), (2, ox)):
                there = full.at[n, all_rows(x_, 1 - core), :]
                remote(there, there, x_sem, (k, n), mate).wait_recv()
            use(n)

    def take_down(n, total):
        residual(n, total, b_down)
        if layer == 1:
            spread(n, xrow[:, n * RW:(n + 1) * RW])

    sends += reduce(1, lambda n: jnp.dot(m, wn[:, n * RW:(n + 1) * RW], preferred_element_type=f32), take_down)
    if layer == 0:
        x_out[...] = xrow[...]
        u = norm_rows(xrow[...], gain[1, 0:1, :].astype(f32), shift[1, 0:1, :].astype(f32)).astype(bf16)
        for i in range(NCH):
            wq_copy(i).wait()
        for n in range(QCH):
            cols = slice(n * QC, (n + 1) * QC)
            r = jnp.broadcast_to(b_qkv[1:2, cols].astype(f32), (ROWS, QC))
            for i in range(NCH):
                r += jnp.dot(u[:, i * CW:(i + 1) * CW], wu[i, :, cols], preferred_element_type=f32)
            spread(n, r)

        def use(n):
            out[n] = full[n]
    else:
        def use(n):
            out[:, n * RW:(n + 1) * RW] = full[n].astype(bf16)

    collect(QCH if layer == 0 else RCH, use)
    for copy in sends:
        copy.wait_send()


def rest_call(layer, msg, x, gain, shift, b_dense, b_up, b_down, w_dense, w_up, w_down, *qkv):
    vm = pl.BlockSpec(memory_space=pltpu.VMEM)
    hbm = pl.BlockSpec(memory_space=pltpu.HBM)
    if layer == 0:
        in_specs = [vm] * 7 + [hbm] * 3 + [vm, hbm]
        out_shape = (jax.ShapeDtypeStruct((ROWS, D), f32), jax.ShapeDtypeStruct((QCH, NB, QC), f32))
        out_specs = (vm, vm)
    else:
        in_specs = [vm] * 7 + [hbm] * 3
        out_shape = jax.ShapeDtypeStruct((NB, D), bf16)
        out_specs = vm
    return pl.pallas_call(
        functools.partial(rest_kernel, layer),
        out_shape=out_shape,
        in_specs=in_specs,
        out_specs=out_specs,
        scratch_shapes=[
            pltpu.VMEM((DR, D), bf16),
            pltpu.VMEM((NCH, CW, F_LOC), bf16),
            pltpu.VMEM((M_LOC, D), bf16),
            pltpu.VMEM((3, MSG, HD), f32),
            pltpu.VMEM((2, MSG, HD), f32),
            pltpu.VMEM((HALF, DR), f32),
            pltpu.VMEM((2, RCH, HALF, RW), f32),
            pltpu.VMEM((2, RCH, ROWS, RW), f32),
            pltpu.VMEM((2, RCH, ROWS, RW), f32),
            pltpu.VMEM((2, RCH, ROWS, RW), f32),
            pltpu.VMEM((NCH, HALF, CW), f32),
            pltpu.VMEM((QCH, NB, QC) if layer == 0 else (RCH, NB, RW), f32),
            pltpu.VMEM((ROWS, D), f32),
            pltpu.VMEM((HALF, F_LOC), f32),
            pltpu.VMEM((HALF, M_LOC), bf16),
            pltpu.SemaphoreType.DMA((2 + 2 * NCH,)),
            pltpu.SemaphoreType.DMA((2, 3)),
            pltpu.SemaphoreType.DMA((2, 2, RCH)),
            pltpu.SemaphoreType.DMA((2, 2, RCH)),
            pltpu.SemaphoreType.DMA((2, NCH)),
            pltpu.SemaphoreType.DMA((2, 3, RCH)),
        ],
        compiler_params=pltpu.CompilerParams(vmem_limit_bytes=VMEM_BYTES, collective_id=layer, has_side_effects=True),
        name=f'rest{layer}',
    )(msg, x, gain, shift, b_dense, b_up, b_down, w_dense, w_up, w_down, *qkv)


def solution(mesh):
    cache_spec = P(None, 'dp', 'sp', 'tp', None)
    in_specs = (P('dp', None), P('dp'), cache_spec, cache_spec, P(), P(), P(None, None, 'tp'), P(None, 'tp'), P(None, 'tp', None), P(), P(None, None, 'tp'), P(None, 'tp'), P(None, 'tp', None), P())
    out_specs = (P('dp', None), cache_spec, cache_spec)

    def device_step(hidden, positions, k_cache, v_cache, ln_gain, ln_bias, w_qkv, b_qkv, w_dense, b_dense, w_up, b_up, w_down, b_down):
        shape = k_cache.shape
        flat = (2, NB, SLOTS * KVL, HD)
        k_cache = k_cache.reshape(flat)
        v_cache = v_cache.reshape(flat)
        shared = (ln_gain, ln_bias, b_dense, b_up, b_down, w_dense, w_up, w_down)
        msg, *caches = attn_call(0, positions, (hidden, ln_gain, ln_bias, b_qkv, w_qkv), k_cache, v_cache, None)
        rows, qkv = rest_call(0, msg, hidden, *shared, b_qkv, w_qkv)
        msg, *caches = attn_call(1, positions, (qkv,), k_cache, v_cache, caches)
        hidden = rest_call(1, msg, rows, *shared)
        return hidden, caches[0].reshape(shape), caches[1].reshape(shape)

    return jax.shard_map(device_step, mesh=mesh, in_specs=in_specs, out_specs=out_specs, check_vma=False)
```

```python
import functools
import math

import jax
import jax.numpy as jnp
from jax import lax
from jax.experimental import pallas as pl
from jax.experimental.pallas import tpu as pltpu
from jax.sharding import PartitionSpec as P

BLOCK_SIZE = 64
LOCAL_BLOCKS = 16
VERT_STRIDE = 8
ROPE_THETA = 1000000.0
GELU_LIMIT = 20.0
NORM_EPS = 0.00001
MASKED = -1e30
MESH = pl.DeviceIdType.MESH

NB = 64
D = 3072
HD = 128
KVL = 4
GRP = 3
SLOTS = 64
QW = KVL * (GRP + 2) * HD
QROWS = 16
KCH = 6
KCS = D // KCH
G = 8
NG = NB // G
GS = 32
HALF = NB // 2
HPC = 6
MSG = HPC * HALF + 8
ROWS = HALF // 2
F_LOC = 4096
M_LOC = F_LOC // 2
NCH = 6
CW = D // NCH
QCH = 4
QC = QW // QCH
DR = HPC * HD
RCH = 6
RW = D // RCH
LAG = 2
VMEM_BYTES = 52 * 1024 * 1024

f32 = jnp.float32
bf16 = jnp.bfloat16


def norm_rows(rows, gain, shift):
    mean = jnp.mean(rows, axis=-1, keepdims=True)
    cent = rows - mean
    var = jnp.mean(jnp.square(cent), axis=-1, keepdims=True)
    return (cent * lax.rsqrt(var + NORM_EPS)) * gain + shift


def rope_tables(pos):
    half = HD // 2
    row = lax.broadcasted_iota(jnp.int32, (8, HD), 0)
    lane = lax.broadcasted_iota(jnp.int32, (NB, HD), 1)
    groups = []
    for i in range(NB // 8):
        at = jnp.zeros((8, HD), jnp.int32)
        for r in range(8):
            at = jnp.where(row == r, pos[i * 8 + r], at)
        groups.append(at)
    where = jnp.concatenate(groups, axis=0).astype(f32)
    power = (lane % half).astype(f32) * (2.0 / HD)
    angles = where * jnp.exp(power * -math.log(ROPE_THETA))
    sin = jnp.sin(angles)
    return jnp.cos(angles), jnp.where(lane < half, -sin, sin)


def attn_kernel(layer, pos, *rest):
    if layer == 0:
        x, gain, shift, b_qkv, w_hbm, kc_hbm, vc_hbm, *rest = rest
    else:
        acc, kc_hbm, vc_hbm, _, _, *rest = rest
    msg, ko_hbm, vo_hbm, kbuf, vbuf, qs, kns, vns, os, ms, ls, ksem, vsem, osem, *rest = rest
    sp = lax.axis_index('sp')
    tp = lax.axis_index('tp')
    base = sp * SLOTS

    def in_copy(hbm, buf, sem, i):
        return pltpu.make_async_copy(hbm.at[layer, pl.ds(i * G, G)], buf.at[pl.ds(i * G, G)], sem.at[i])

    def out_copy(buf, hbm, j, i):
        return pltpu.make_async_copy(buf.at[pl.ds(i * G, G)], hbm.at[layer, pl.ds(i * G, G)], osem.at[j, i])

    def fetch_cache():
        for i in range(NG):
            in_copy(kc_hbm, kbuf, ksem, i).start(priority=0)
            in_copy(vc_hbm, vbuf, vsem, i).start(priority=1)

    if layer == 0:
        w, u, acc, wsem, *places, small_sem = rest
        small = [pltpu.make_async_copy(src, dst, small_sem.at[i]) for i, (src, dst) in enumerate(zip((pos, x, gain, shift, b_qkv), places))]
        for copy in small:
            copy.start()
        pos, x, gain, shift, b_qkv = places

        def w_copy(i):
            return pltpu.make_async_copy(w_hbm.at[layer, pl.ds(i * KCS, KCS), :], w.at[i], wsem.at[i])

        for i in range(KCH):
            w_copy(i).start(priority=i % 2)
        fetch_cache()
        for copy in small:
            copy.wait()
        g_row = gain[layer, 0:1, :].astype(f32)
        s_row = shift[layer, 0:1, :].astype(f32)
        for i in range(NB // 16):
            rows = x[pl.ds(i * 16, 16), :].astype(f32)
            normed = norm_rows(rows, g_row, s_row).astype(bf16)
            for j in range(KCH):
                u[j, pl.ds(i * 16, 16), :] = normed[:, j * KCS:(j + 1) * KCS]
        acc[...] = jnp.broadcast_to(b_qkv[layer:layer + 1, :].astype(f32), (NB, QW))
    else:
        fetch_cache()
    qs[...] = jnp.zeros_like(qs)
    cos_t, sin_t = rope_tables(pos)
    if layer == 0:
        def qkv_step(i, carry):
            w_copy(i).wait()
            acc[...] += jnp.dot(u[i], w[i], preferred_element_type=f32)
            return carry

        lax.fori_loop(0, KCH, qkv_step, 0)

    for c in range(KVL):
        for j in range(GRP + 2):
            if layer == 0:
                col = (c * (GRP + 2) + j) * HD
                tile = acc[:, col:col + HD]
            else:
                tile = acc[c, :, j * HD:(j + 1) * HD]
            if j <= GRP:
                tile = tile * cos_t + pltpu.roll(tile, HD // 2, 1) * sin_t
            for i in range(NB // 8):
                part = tile[i * 8:(i + 1) * 8]
                if j < GRP:
                    qs[pl.ds(i * 8 * QROWS + c * GRP + j, 8, stride=QROWS), :] = part
                else:
                    dst = kns if j == GRP else vns
                    dst[pl.ds(i * 64 + c, 8, stride=8), :] = part
                    dst[pl.ds(i * 64 + c + 4, 8, stride=8), :] = part

    row_h = lax.broadcasted_iota(jnp.int32, (QROWS, SLOTS * KVL), 0)
    col_i = lax.broadcasted_iota(jnp.int32, (QROWS, SLOTS * KVL), 1)
    slot_of = jnp.where(row_h // GRP == col_i % KVL, col_i // KVL, 1 << 20)
    head_id = tp * KVL * GRP + row_h
    vertical = (sp + head_id + 1) % VERT_STRIDE == 0
    sub_row = lax.broadcasted_iota(jnp.int32, (16, HD), 0) // KVL

    def attn_step(i, carry):
        copies = [i * (GS // G) + j for j in range(GS // G)]
        for j in copies:
            in_copy(kc_hbm, kbuf, ksem, j).wait()
            in_copy(vc_hbm, vbuf, vsem, j).wait()
        limits = []
        for bi in range(GS):
            b = i * GS + bi
            p = pos[b]
            pl_ = p - base
            pc = jnp.clip(pl_, 0, SLOTS - 1)
            hit = jnp.logical_and(pl_ >= 0, pl_ < SLOTS)
            sub = jnp.where(hit, pc % KVL, -1)
            r0 = pl.multiple_of((pc // KVL) * 16, 16)
            put = sub_row == sub
            for buf, new in ((kbuf, kns), (vbuf, vns)):
                new8 = new[pl.ds(pl.multiple_of(b * 8, 8), 8), :]
                new16 = jnp.concatenate([new8, new8], axis=0)
                old = buf[b, pl.ds(r0, 16), :].astype(f32)
                buf[b, pl.ds(r0, 16), :] = jnp.where(put, new16, old).astype(bf16)
            if layer == 0:
                near = p // BLOCK_SIZE - sp < LOCAL_BLOCKS
                limits.append(jnp.where(vertical, pl_, jnp.where(near, pl_, -1)))
            else:
                limits.append(pl_)
        scores = []
        for bi in range(GS):
            b = i * GS + bi
            q = qs[pl.ds(pl.multiple_of(b * QROWS, QROWS), QROWS), :].astype(bf16)
            scores.append(lax.dot_general(q, kbuf[b], (((1,), (1,)), ((), ())), preferred_element_type=f32))
        keeps = [slot_of <= limit for limit in limits]
        scores = [jnp.where(keep, s * (1.0 / HD), MASKED) for keep, s in zip(keeps, scores)]
        peaks = [jnp.max(s, axis=1, keepdims=True) for s in scores]
        weights = [jnp.where(keep, jnp.exp(s - peak), 0.0) for keep, s, peak in zip(keeps, scores, peaks)]
        outs = [jnp.dot(wt.astype(bf16), vbuf[i * GS + bi], preferred_element_type=f32) for bi, wt in enumerate(weights)]
        sums = [jnp.sum(wt, axis=1, keepdims=True) for wt in weights]
        for bi in range(GS):
            rows = pl.ds(pl.multiple_of((i * GS + bi) * QROWS, QROWS), QROWS)
            ms[rows, :] = jnp.broadcast_to(peaks[bi], (QROWS, HD))
            ls[rows, :] = jnp.broadcast_to(sums[bi], (QROWS, HD))
            os[rows, :] = outs[bi]

        for j in copies:
            out_copy(kbuf, ko_hbm, 0, j).start()
            out_copy(vbuf, vo_hbm, 1, j).start(priority=1)
        return carry

    lax.fori_loop(0, NB // GS, attn_step, 0)

    lane = lax.broadcasted_iota(jnp.int32, (8, HD), 1)
    for half in range(2):
        for c in range(2):
            stat = jnp.zeros((8, HD), f32)
            for g in range(HPC):
                for i in range(HALF // 8):
                    rows = pl.ds((half * HALF + i * 8) * QROWS + c * HPC + g, 8, stride=QROWS)
                    at = 2 * (g * (HALF // 8) + i)
                    msg[half * 2 + c, pl.ds(g * HALF + i * 8, 8), :] = os[rows, :]
                    stat = jnp.where(lane == at, ms[rows, :], stat)
                    stat = jnp.where(lane == at + 1, ls[rows, :], stat)
            msg[half * 2 + c, pl.ds(HPC * HALF, 8), :] = stat
    for i in range(NG):
        out_copy(kbuf, ko_hbm, 0, i).wait()
        out_copy(vbuf, vo_hbm, 1, i).wait()


def attn_call(layer, pos, operands, k_cache, v_cache, prev):
    vm = pl.BlockSpec(memory_space=pltpu.VMEM)
    hbm = pl.BlockSpec(memory_space=pltpu.HBM)
    args = [pos, *operands, k_cache, v_cache]
    if layer == 0:
        specs = [hbm] * 8
        alias = {}
        extra = [
            pltpu.VMEM((KCH, KCS, QW), bf16),
            pltpu.VMEM((KCH, NB, KCS), bf16),
            pltpu.VMEM((NB, QW), f32),
            pltpu.SemaphoreType.DMA((KCH,)),
            pltpu.SMEM(pos.shape, jnp.int32),
            *[pltpu.VMEM(arr.shape, bf16) for arr in operands[:4]],
            pltpu.SemaphoreType.DMA((5,)),
        ]
        limit = 60 * 1024 * 1024
    else:
        args += list(prev)
        specs = [pl.BlockSpec(memory_space=pltpu.SMEM), vm] + [hbm] * 4
        alias = {4: 1, 5: 2}
        extra = []
        limit = VMEM_BYTES
    cache = jax.ShapeDtypeStruct(k_cache.shape, bf16)
    return pl.pallas_call(
        functools.partial(attn_kernel, layer),
        out_shape=(jax.ShapeDtypeStruct((KVL, MSG, HD), f32), cache, cache),
        in_specs=specs,
        out_specs=(vm, hbm, hbm),
        scratch_shapes=[
            pltpu.VMEM((NB, SLOTS * KVL, HD), bf16),
            pltpu.VMEM((NB, SLOTS * KVL, HD), bf16),
            pltpu.VMEM((NB * QROWS, HD), f32),
            pltpu.VMEM((NB * 8, HD), f32),
            pltpu.VMEM((NB * 8, HD), f32),
            pltpu.VMEM((NB * QROWS, HD), f32),
            pltpu.VMEM((NB * QROWS, HD), f32),
            pltpu.VMEM((NB * QROWS, HD), f32),
            pltpu.SemaphoreType.DMA((NG,)),
            pltpu.SemaphoreType.DMA((NG,)),
            pltpu.SemaphoreType.DMA((2, NG)),
            *extra,
        ],
        input_output_aliases=alias,
        compiler_params=pltpu.CompilerParams(vmem_limit_bytes=limit),
        name=f'attn{layer}',
    )(*args)


def rest_kernel(layer, msg, x, gain, shift, b_dense, b_up, b_down, wd_hbm, wu_hbm, wn_hbm, *rest):
    if layer == 0:
        b_qkv, wq_hbm, x_out, out, *rest = rest
    else:
        out, *rest = rest
    (wd, wu, wn, got, sent, o_buf, part, pair, sums, other, ag, full, xrow, up, mbuf,
     wsem, a_sem, d_sem, y_sem, g_sem, x_sem) = rest
    dp = lax.axis_index('dp')
    tp = lax.axis_index('tp')
    sp = lax.axis_index('sp')
    core = sp % 2
    cx = sp // 2
    ox = 1 - cx
    mate = (dp, tp, cx * 2 + 1 - core)
    x_dev = (dp, tp, ox * 2 + core)
    y_dev = (dp, 1 - tp, sp)

    def load(src, dst, i):
        return pltpu.make_async_copy(src, dst, wsem.at[i])

    wd_copy = load(wd_hbm.at[layer, pl.ds(pl.multiple_of(core * DR, DR), DR), :], wd, 0)

    def wu_copy(i):
        return load(wu_hbm.at[layer, pl.ds(i * CW, CW), pl.ds(pl.multiple_of(core * F_LOC, F_LOC), F_LOC)], wu.at[i], 1 + i)

    wn_copy = load(wn_hbm.at[layer, pl.ds(pl.multiple_of(core * M_LOC, M_LOC), M_LOC), :], wn, 1 + NCH)

    def wq_copy(i):
        return load(wq_hbm.at[1, pl.ds(i * CW, CW), :], wu.at[i, :, pl.ds(0, QW)], 2 + NCH + i)

    barrier = pltpu.get_barrier_semaphore()
    for peer in (mate, x_dev, y_dev):
        pl.semaphore_signal(barrier, inc=1, device_id=peer, device_id_type=MESH)
    wd_copy.start()
    for i in range(NCH):
        wu_copy(i).start()
    wn_copy.start()
    pl.semaphore_wait(barrier, 3)

    def remote(src, dst, sems, idx, peer):
        return pltpu.make_async_remote_copy(
            src_ref=src, dst_ref=dst, send_sem=sems.at[(0,) + idx], recv_sem=sems.at[(1,) + idx],
            device_id=peer, device_id_type=MESH)

    near = cx * 2 + core
    far = ox * 2 + core
    swap = [remote(msg.at[ox * 2 + 1 - core], got.at[0], a_sem, (0,), mate),
            remote(msg.at[cx * 2 + 1 - core], got.at[1], a_sem, (1,), mate)]
    for copy in swap:
        copy.start()

    gain1 = gain[layer, 1:2, :].astype(f32)
    shift1 = shift[layer, 1:2, :].astype(f32)
    own = pl.ds(pl.multiple_of(core * ROWS, ROWS), ROWS)
    theirs = pl.ds(pl.multiple_of((1 - core) * ROWS, ROWS), ROWS)

    def all_rows(x_, c_):
        return pl.ds(pl.multiple_of(x_ * HALF + c_ * ROWS, ROWS), ROWS)

    xrow[...] = x[all_rows(cx, core), :].astype(f32) if layer == 0 else x[...]
    lane = lax.broadcasted_iota(jnp.int32, (8, HD), 1)

    def merge(one, two, put, stat_out=None):
        stats = [ref[pl.ds(HPC * HALF, 8), :] for ref in (one, two)]
        new_stat = jnp.zeros((8, HD), f32)
        for g in range(HPC):
            for i in range(HALF // 8):
                at = 2 * (g * (HALF // 8) + i)
                peaks = [jnp.broadcast_to(st[:, at:at + 1], (8, HD)) for st in stats]
                tots = [jnp.broadcast_to(st[:, at + 1:at + 2], (8, HD)) for st in stats]
                top = jnp.maximum(peaks[0], peaks[1])
                scale = [jnp.exp(p - top) for p in peaks]
                rows = pl.ds(g * HALF + i * 8, 8)
                num = one[rows, :] * scale[0] + two[rows, :] * scale[1]
                den = tots[0] * scale[0] + tots[1] * scale[1]
                put(g, i, num, den)
                if stat_out is not None:
                    new_stat = jnp.where(lane == at, top, new_stat)
                    new_stat = jnp.where(lane == at + 1, den, new_stat)
        if stat_out is not None:
            stat_out[pl.ds(HPC * HALF, 8), :] = new_stat

    def put_part(ref):
        def put(g, i, num, den):
            ref[pl.ds(g * HALF + i * 8, 8), :] = num
        return put

    def put_out(g, i, num, den):
        o_buf[pl.ds(i * 8, 8), g * HD:(g + 1) * HD] = num / den

    swap[0].wait_recv()
    merge(msg.at[far], got.at[0], put_part(sent.at[0]), sent.at[0])
    cross = remote(sent.at[0], got.at[2], a_sem, (2,), x_dev)
    cross.start()
    swap[1].wait_recv()
    merge(msg.at[near], got.at[1], put_part(sent.at[1]), sent.at[1])
    cross.wait_recv()
    merge(sent.at[1], got.at[2], put_out)
    sends = swap + [cross]

    def reduce(ph, product, finish):
        first = [remote(part.at[ph, n, theirs, :], pair.at[ph, n], d_sem, (ph, n), mate) for n in range(RCH)]
        second = [remote(sums.at[ph, n], other.at[ph, n], y_sem, (ph, n), y_dev) for n in range(RCH)]
        for step in range(RCH + LAG):
            if step < RCH:
                part[ph, step] = product(step)
                first[step].start()
            if step >= LAG:
                n = step - LAG
                first[n].wait_recv()
                sums[ph, n] = part[ph, n, own, :] + pair[ph, n]
                second[n].start()
        for n in range(RCH):
            second[n].wait_recv()
            finish(n, sums[ph, n] + other[ph, n])
        return first + second

    def residual(n, total, bias):
        cols = slice(n * RW, (n + 1) * RW)
        v = xrow[:, cols] + total + bias[layer:layer + 1, cols].astype(f32)
        xrow[:, cols] = v.astype(bf16).astype(f32)

    wd_copy.wait()
    o = o_buf[...].astype(bf16)
    sends += reduce(0, lambda n: jnp.dot(o, wd[:, n * RW:(n + 1) * RW], preferred_element_type=f32),
                   lambda n, total: residual(n, total, b_dense))

    normed = norm_rows(xrow[...], gain1, shift1).astype(bf16).astype(f32)
    swap = []
    for n in range(NCH):
        ag[n, own, :] = normed[:, n * CW:(n + 1) * CW]
        here = ag.at[n, own, :]
        swap.append(remote(here, here, g_sem, (n,), mate))
        swap[n].start()
    cols_up = pl.ds(pl.multiple_of(core * F_LOC, F_LOC), F_LOC)
    up[...] = jnp.broadcast_to(b_up[layer:layer + 1, cols_up].astype(f32), (HALF, F_LOC))
    for n in range(NCH):
        wu_copy(n).wait()
        swap[n].wait_recv()
        up[...] += jnp.dot(ag[n].astype(bf16), wu[n], preferred_element_type=f32)
        if layer == 0:
            wq_copy(n).start()

    pick = (lax.broadcasted_iota(jnp.int32, (256, 128), 0) == 2 * lax.broadcasted_iota(jnp.int32, (256, 128), 1))
    pick = jnp.where(pick, 1.0, 0.0).astype(bf16)
    for k in range(F_LOC // 256):
        a = up[:, k * 256:(k + 1) * 256]
        z = jnp.minimum(a, GELU_LIMIT)
        gate = z * jax.nn.sigmoid(1.702 * z)
        lin = jnp.clip(a, -GELU_LIMIT, GELU_LIMIT) + 1.0
        prod = (gate * pltpu.roll(lin, 255, 1)).astype(bf16)
        mbuf[:, k * 128:(k + 1) * 128] = jnp.dot(prod, pick, preferred_element_type=f32).astype(bf16)
    wn_copy.wait()
    m = mbuf[...]
    sends += swap

    def spread(n, value):
        full[n, all_rows(cx, core), :] = value
        here = full.at[n, all_rows(cx, core), :]
        for k, peer in enumerate((x_dev, mate)):
            copy = remote(here, here, x_sem, (k, n), peer)
            copy.start()
            sends.append(copy)

    def collect(chunks, use):
        for n in range(chunks):
            there = full.at[n, all_rows(ox, core), :]
            remote(there, there, x_sem, (0, n), x_dev).wait_recv()
            copy = remote(there, there, x_sem, (2, n), mate)
            copy.start()
            sends.append(copy)
        for n in range(chunks):
            for k, x_ in ((1, cx), (2, ox)):
                there = full.at[n, all_rows(x_, 1 - core), :]
                remote(there, there, x_sem, (k, n), mate).wait_recv()
            use(n)

    def take_down(n, total):
        residual(n, total, b_down)
        if layer == 1:
            spread(n, xrow[:, n * RW:(n + 1) * RW])

    sends += reduce(1, lambda n: jnp.dot(m, wn[:, n * RW:(n + 1) * RW], preferred_element_type=f32), take_down)
    if layer == 0:
        x_out[...] = xrow[...]
        u = norm_rows(xrow[...], gain[1, 0:1, :].astype(f32), shift[1, 0:1, :].astype(f32)).astype(bf16)
        for i in range(NCH):
            wq_copy(i).wait()
        for n in range(QCH):
            cols = slice(n * QC, (n + 1) * QC)
            r = jnp.broadcast_to(b_qkv[1:2, cols].astype(f32), (ROWS, QC))
            for i in range(NCH):
                r += jnp.dot(u[:, i * CW:(i + 1) * CW], wu[i, :, cols], preferred_element_type=f32)
            spread(n, r)

        def use(n):
            out[n] = full[n]
    else:
        def use(n):
            out[:, n * RW:(n + 1) * RW] = full[n].astype(bf16)

    collect(QCH if layer == 0 else RCH, use)
    for copy in sends:
        copy.wait_send()


def rest_call(layer, msg, x, gain, shift, b_dense, b_up, b_down, w_dense, w_up, w_down, *qkv):
    vm = pl.BlockSpec(memory_space=pltpu.VMEM)
    hbm = pl.BlockSpec(memory_space=pltpu.HBM)
    if layer == 0:
        in_specs = [vm] * 7 + [hbm] * 3 + [vm, hbm]
        out_shape = (jax.ShapeDtypeStruct((ROWS, D), f32), jax.ShapeDtypeStruct((QCH, NB, QC), f32))
        out_specs = (vm, vm)
    else:
        in_specs = [vm] * 7 + [hbm] * 3
        out_shape = jax.ShapeDtypeStruct((NB, D), bf16)
        out_specs = vm
    return pl.pallas_call(
        functools.partial(rest_kernel, layer),
        out_shape=out_shape,
        in_specs=in_specs,
        out_specs=out_specs,
        scratch_shapes=[
            pltpu.VMEM((DR, D), bf16),
            pltpu.VMEM((NCH, CW, F_LOC), bf16),
            pltpu.VMEM((M_LOC, D), bf16),
            pltpu.VMEM((3, MSG, HD), f32),
            pltpu.VMEM((2, MSG, HD), f32),
            pltpu.VMEM((HALF, DR), f32),
            pltpu.VMEM((2, RCH, HALF, RW), f32),
            pltpu.VMEM((2, RCH, ROWS, RW), f32),
            pltpu.VMEM((2, RCH, ROWS, RW), f32),
            pltpu.VMEM((2, RCH, ROWS, RW), f32),
            pltpu.VMEM((NCH, HALF, CW), f32),
            pltpu.VMEM((QCH, NB, QC) if layer == 0 else (RCH, NB, RW), f32),
            pltpu.VMEM((ROWS, D), f32),
            pltpu.VMEM((HALF, F_LOC), f32),
            pltpu.VMEM((HALF, M_LOC), bf16),
            pltpu.SemaphoreType.DMA((2 + 2 * NCH,)),
            pltpu.SemaphoreType.DMA((2, 3)),
            pltpu.SemaphoreType.DMA((2, 2, RCH)),
            pltpu.SemaphoreType.DMA((2, 2, RCH)),
            pltpu.SemaphoreType.DMA((2, NCH)),
            pltpu.SemaphoreType.DMA((2, 3, RCH)),
        ],
        compiler_params=pltpu.CompilerParams(vmem_limit_bytes=VMEM_BYTES, collective_id=layer, has_side_effects=True),
        name=f'rest{layer}',
    )(msg, x, gain, shift, b_dense, b_up, b_down, w_dense, w_up, w_down, *qkv)


def solution(mesh):
    cache_spec = P(None, 'dp', 'sp', 'tp', None)
    in_specs = (P('dp', None), P('dp'), cache_spec, cache_spec, P(), P(), P(None, None, 'tp'), P(None, 'tp'), P(None, 'tp', None), P(), P(None, None, 'tp'), P(None, 'tp'), P(None, 'tp', None), P())
    out_specs = (P('dp', None), cache_spec, cache_spec)

    def device_step(hidden, positions, k_cache, v_cache, ln_gain, ln_bias, w_qkv, b_qkv, w_dense, b_dense, w_up, b_up, w_down, b_down):
        shape = k_cache.shape
        flat = (2, NB, SLOTS * KVL, HD)
        k_cache = k_cache.reshape(flat)
        v_cache = v_cache.reshape(flat)
        shared = (ln_gain, ln_bias, b_dense, b_up, b_down, w_dense, w_up, w_down)
        msg, *caches = attn_call(0, positions, (hidden, ln_gain, ln_bias, b_qkv, w_qkv), k_cache, v_cache, None)
        rows, qkv = rest_call(0, msg, hidden, *shared, b_qkv, w_qkv)
        msg, *caches = attn_call(1, positions, (qkv,), k_cache, v_cache, caches)
        hidden = rest_call(1, msg, rows, *shared)
        return hidden, caches[0].reshape(shape), caches[1].reshape(shape)

    return jax.shard_map(device_step, mesh=mesh, in_specs=in_specs, out_specs=out_specs, check_vma=False)
```

```python
import functools
import math

import jax
import jax.numpy as jnp
from jax import lax
from jax.experimental import pallas as pl
from jax.experimental.pallas import tpu as pltpu
from jax.sharding import PartitionSpec as P

BLOCK_SIZE = 64
LOCAL_BLOCKS = 16
VERT_STRIDE = 8
ROPE_THETA = 1000000.0
GELU_LIMIT = 20.0
NORM_EPS = 0.00001
MASKED = -1e30
MESH = pl.DeviceIdType.MESH

NB = 64
D = 3072
HD = 128
KVL = 4
GRP = 3
SLOTS = 64
QW = KVL * (GRP + 2) * HD
QROWS = 16
KCH = 12
KCS = D // KCH
G = 8
NG = NB // G
GS = 16
HALF = NB // 2
HPC = 6
MSG = HPC * HALF + 8
ROWS = HALF // 2
F_LOC = 4096
M_LOC = F_LOC // 2
NCH = 6
CW = D // NCH
QCH = 4
QC = QW // QCH
DR = HPC * HD
RCH = 6
RW = D // RCH
LAG = 2
VMEM_BYTES = 52 * 1024 * 1024

f32 = jnp.float32
bf16 = jnp.bfloat16


def norm_rows(rows, gain, shift):
    mean = jnp.mean(rows, axis=-1, keepdims=True)
    cent = rows - mean
    var = jnp.mean(jnp.square(cent), axis=-1, keepdims=True)
    return (cent * lax.rsqrt(var + NORM_EPS)) * gain + shift


def rope_tables(pos):
    half = HD // 2
    row = lax.broadcasted_iota(jnp.int32, (8, HD), 0)
    lane = lax.broadcasted_iota(jnp.int32, (NB, HD), 1)
    groups = []
    for i in range(NB // 8):
        at = jnp.zeros((8, HD), jnp.int32)
        for r in range(8):
            at = jnp.where(row == r, pos[i * 8 + r], at)
        groups.append(at)
    where = jnp.concatenate(groups, axis=0).astype(f32)
    power = (lane % half).astype(f32) * (2.0 / HD)
    angles = where * jnp.exp(power * -math.log(ROPE_THETA))
    sin = jnp.sin(angles)
    return jnp.cos(angles), jnp.where(lane < half, -sin, sin)


def attn_kernel(layer, pos, *rest):
    if layer == 0:
        x, gain, shift, b_qkv, w_hbm, kc_hbm, vc_hbm, *rest = rest
    else:
        acc, kc_hbm, vc_hbm, _, _, *rest = rest
    msg, ko_hbm, vo_hbm, kbuf, vbuf, qs, kns, vns, os, ms, ls, ksem, vsem, osem, *rest = rest
    sp = lax.axis_index('sp')
    tp = lax.axis_index('tp')
    base = sp * SLOTS

    def in_copy(hbm, buf, sem, i):
        return pltpu.make_async_copy(hbm.at[layer, pl.ds(i * G, G)], buf.at[pl.ds(i * G, G)], sem.at[i])

    def out_copy(buf, hbm, j, i):
        return pltpu.make_async_copy(buf.at[pl.ds(i * G, G)], hbm.at[layer, pl.ds(i * G, G)], osem.at[j, i])

    def fetch_cache():
        for i in range(NG):
            in_copy(kc_hbm, kbuf, ksem, i).start(priority=0)
            in_copy(vc_hbm, vbuf, vsem, i).start(priority=1)

    if layer == 0:
        w, u, acc, wsem, *places, msg_buf, small_sem = rest
        msg_hbm, msg = msg, msg_buf
        small = [pltpu.make_async_copy(src, dst, small_sem.at[i]) for i, (src, dst) in enumerate(zip((pos, x, gain, shift, b_qkv), places))]
        for copy in small:
            copy.start()
        pos, x, gain, shift, b_qkv = places

        def w_copy(i):
            return pltpu.make_async_copy(w_hbm.at[layer, pl.ds(i * KCS, KCS), :], w.at[i], wsem.at[i])

        for i in range(KCH):
            w_copy(i).start(priority=i % 2)
        fetch_cache()
        for copy in small:
            copy.wait()
        g_row = gain[layer, 0:1, :].astype(f32)
        s_row = shift[layer, 0:1, :].astype(f32)
        for i in range(NB // 16):
            rows = x[pl.ds(i * 16, 16), :].astype(f32)
            normed = norm_rows(rows, g_row, s_row).astype(bf16)
            for j in range(KCH):
                u[j, pl.ds(i * 16, 16), :] = normed[:, j * KCS:(j + 1) * KCS]
        acc[...] = jnp.broadcast_to(b_qkv[layer:layer + 1, :].astype(f32), (NB, QW))
    else:
        fetch_cache()
    qs[...] = jnp.zeros_like(qs)
    cos_t, sin_t = rope_tables(pos)
    if layer == 0:
        def qkv_step(i, carry):
            w_copy(i).wait()
            acc[...] += jnp.dot(u[i], w[i], preferred_element_type=f32)
            return carry

        lax.fori_loop(0, KCH, qkv_step, 0)

    for c in range(KVL):
        for j in range(GRP + 2):
            if layer == 0:
                col = (c * (GRP + 2) + j) * HD
                tile = acc[:, col:col + HD]
            else:
                tile = acc[c, :, j * HD:(j + 1) * HD]
            if j <= GRP:
                tile = tile * cos_t + pltpu.roll(tile, HD // 2, 1) * sin_t
            for i in range(NB // 8):
                part = tile[i * 8:(i + 1) * 8]
                if j < GRP:
                    qs[pl.ds(i * 8 * QROWS + c * GRP + j, 8, stride=QROWS), :] = part
                else:
                    dst = kns if j == GRP else vns
                    dst[pl.ds(i * 64 + c, 8, stride=8), :] = part
                    dst[pl.ds(i * 64 + c + 4, 8, stride=8), :] = part

    row_h = lax.broadcasted_iota(jnp.int32, (QROWS, SLOTS * KVL), 0)
    col_i = lax.broadcasted_iota(jnp.int32, (QROWS, SLOTS * KVL), 1)
    slot_of = jnp.where(row_h // GRP == col_i % KVL, col_i // KVL, 1 << 20)
    head_id = tp * KVL * GRP + row_h
    vertical = (sp + head_id + 1) % VERT_STRIDE == 0
    sub_row = lax.broadcasted_iota(jnp.int32, (16, HD), 0) // KVL

    def patch(buf, new, b):
        at = pos[b] - base
        atc = jnp.clip(at, 0, SLOTS - 1)
        hit = jnp.logical_and(at >= 0, at < SLOTS)
        put = sub_row == jnp.where(hit, atc % KVL, -1)
        r0 = pl.multiple_of((atc // KVL) * 16, 16)
        new8 = new[b * 8:b * 8 + 8, :]
        new16 = jnp.concatenate([new8, new8], axis=0)
        old = buf[b, pl.ds(r0, 16), :].astype(f32)
        buf[b, pl.ds(r0, 16), :] = jnp.where(put, new16, old).astype(bf16)

    def score(step):
        seqs = range(step * GS, (step + 1) * GS)
        for b in seqs:
            patch(kbuf, kns, b)
        return [lax.dot_general(qs[b * QROWS:(b + 1) * QROWS, :].astype(bf16), kbuf[b], (((1,), (1,)), ((), ())),
                                preferred_element_type=f32) for b in seqs]

    def keep_of(b):
        at = pos[b] - base
        if layer == 0:
            near = pos[b] // BLOCK_SIZE - sp < LOCAL_BLOCKS
            return slot_of <= jnp.where(vertical, at, jnp.where(near, at, -1))
        return slot_of <= at

    def mix(step, scores):
        seqs = range(step * GS, (step + 1) * GS)
        for b in seqs:
            patch(vbuf, vns, b)
        keeps = [keep_of(b) for b in seqs]
        scores = [jnp.where(keep, s * (1.0 / HD), MASKED) for keep, s in zip(keeps, scores)]
        peaks = [jnp.max(s, axis=1, keepdims=True) for s in scores]
        weights = [jnp.where(keep, jnp.exp(s - peak), 0.0) for keep, s, peak in zip(keeps, scores, peaks)]
        outs = [jnp.dot(wt.astype(bf16), vbuf[b], preferred_element_type=f32) for b, wt in zip(seqs, weights)]
        sums = [jnp.sum(wt, axis=1, keepdims=True) for wt in weights]
        for j, b in enumerate(seqs):
            rows = slice(b * QROWS, (b + 1) * QROWS)
            ms[rows, :] = jnp.broadcast_to(peaks[j], (QROWS, HD))
            ls[rows, :] = jnp.broadcast_to(sums[j], (QROWS, HD))
            os[rows, :] = outs[j]

    per = GS // G
    steps = NB // GS
    for j in range(per):
        in_copy(kc_hbm, kbuf, ksem, j).wait()
    scores = score(0)
    for step in range(steps):
        for j in range(step * per, (step + 1) * per):
            in_copy(vc_hbm, vbuf, vsem, j).wait()
            if step + 1 < steps:
                in_copy(kc_hbm, kbuf, ksem, j + per).wait()
        later = score(step + 1) if step + 1 < steps else None
        mix(step, scores)
        scores = later
        for j in range(step * per, (step + 1) * per):
            out_copy(kbuf, ko_hbm, 0, j).start()
            out_copy(vbuf, vo_hbm, 1, j).start(priority=1)

    lane = lax.broadcasted_iota(jnp.int32, (8, HD), 1)
    for half in range(2):
        for c in range(2):
            stat = jnp.zeros((8, HD), f32)
            for g in range(HPC):
                for i in range(HALF // 8):
                    rows = pl.ds((half * HALF + i * 8) * QROWS + c * HPC + g, 8, stride=QROWS)
                    at = 2 * (g * (HALF // 8) + i)
                    msg[half * 2 + c, pl.ds(g * HALF + i * 8, 8), :] = os[rows, :]
                    stat = jnp.where(lane == at, ms[rows, :], stat)
                    stat = jnp.where(lane == at + 1, ls[rows, :], stat)
            msg[half * 2 + c, pl.ds(HPC * HALF, 8), :] = stat
    if layer == 0:
        send = pltpu.make_async_copy(msg, msg_hbm, small_sem.at[5])
        send.start()
    for i in range(NG):
        out_copy(kbuf, ko_hbm, 0, i).wait()
        out_copy(vbuf, vo_hbm, 1, i).wait()
    if layer == 0:
        send.wait()


def attn_call(layer, pos, operands, k_cache, v_cache, prev):
    vm = pl.BlockSpec(memory_space=pltpu.VMEM)
    hbm = pl.BlockSpec(memory_space=pltpu.HBM)
    args = [pos, *operands, k_cache, v_cache]
    if layer == 0:
        specs = [hbm] * 8
        alias = {}
        extra = [
            pltpu.VMEM((KCH, KCS, QW), bf16),
            pltpu.VMEM((KCH, NB, KCS), bf16),
            pltpu.VMEM((NB, QW), f32),
            pltpu.SemaphoreType.DMA((KCH,)),
            pltpu.SMEM(pos.shape, jnp.int32),
            *[pltpu.VMEM(arr.shape, bf16) for arr in operands[:4]],
            pltpu.VMEM((KVL, MSG, HD), f32),
            pltpu.SemaphoreType.DMA((6,)),
        ]
        limit = 60 * 1024 * 1024
    else:
        args += list(prev)
        specs = [pl.BlockSpec(memory_space=pltpu.SMEM), vm] + [hbm] * 4
        alias = {4: 1, 5: 2}
        extra = []
        limit = VMEM_BYTES
    cache = jax.ShapeDtypeStruct(k_cache.shape, bf16)
    return pl.pallas_call(
        functools.partial(attn_kernel, layer),
        out_shape=(jax.ShapeDtypeStruct((KVL, MSG, HD), f32), cache, cache),
        in_specs=specs,
        out_specs=(hbm if layer == 0 else vm, hbm, hbm),
        scratch_shapes=[
            pltpu.VMEM((NB, SLOTS * KVL, HD), bf16),
            pltpu.VMEM((NB, SLOTS * KVL, HD), bf16),
            pltpu.VMEM((NB * QROWS, HD), f32),
            pltpu.VMEM((NB * 8, HD), f32),
            pltpu.VMEM((NB * 8, HD), f32),
            pltpu.VMEM((NB * QROWS, HD), f32),
            pltpu.VMEM((NB * QROWS, HD), f32),
            pltpu.VMEM((NB * QROWS, HD), f32),
            pltpu.SemaphoreType.DMA((NG,)),
            pltpu.SemaphoreType.DMA((NG,)),
            pltpu.SemaphoreType.DMA((2, NG)),
            *extra,
        ],
        input_output_aliases=alias,
        compiler_params=pltpu.CompilerParams(vmem_limit_bytes=limit),
        name=f'attn{layer}',
    )(*args)


def rest_kernel(layer, msg, x, gain, shift, b_dense, b_up, b_down, wd_hbm, wu_hbm, wn_hbm, *rest):
    if layer == 0:
        b_qkv, wq_hbm, x_out, out, *rest = rest
    else:
        out, *rest = rest
    (wd, wu, wn, got, sent, o_buf, part, pair, sums, other, ag, full, xrow, up, mbuf,
     wsem, a_sem, d_sem, y_sem, g_sem, x_sem) = rest
    dp = lax.axis_index('dp')
    tp = lax.axis_index('tp')
    sp = lax.axis_index('sp')
    core = sp % 2
    cx = sp // 2
    ox = 1 - cx
    mate = (dp, tp, cx * 2 + 1 - core)
    x_dev = (dp, tp, ox * 2 + core)
    y_dev = (dp, 1 - tp, sp)

    def load(src, dst, i):
        return pltpu.make_async_copy(src, dst, wsem.at[i])

    wd_copy = load(wd_hbm.at[layer, pl.ds(pl.multiple_of(core * DR, DR), DR), :], wd, 0)

    def wu_copy(i):
        return load(wu_hbm.at[layer, pl.ds(i * CW, CW), pl.ds(pl.multiple_of(core * F_LOC, F_LOC), F_LOC)], wu.at[i], 1 + i)

    wn_copy = load(wn_hbm.at[layer, pl.ds(pl.multiple_of(core * M_LOC, M_LOC), M_LOC), :], wn, 1 + NCH)

    def wq_copy(i):
        return load(wq_hbm.at[1, pl.ds(i * CW, CW), :], wu.at[i, :, pl.ds(0, QW)], 2 + NCH + i)

    barrier = pltpu.get_barrier_semaphore()
    for peer in (mate, x_dev, y_dev):
        pl.semaphore_signal(barrier, inc=1, device_id=peer, device_id_type=MESH)
    wd_copy.start()
    for i in range(NCH):
        wu_copy(i).start()
    wn_copy.start()
    pl.semaphore_wait(barrier, 3)

    def remote(src, dst, sems, idx, peer):
        return pltpu.make_async_remote_copy(
            src_ref=src, dst_ref=dst, send_sem=sems.at[(0,) + idx], recv_sem=sems.at[(1,) + idx],
            device_id=peer, device_id_type=MESH)

    near = cx * 2 + core
    far = ox * 2 + core
    swap = [remote(msg.at[ox * 2 + 1 - core], got.at[0], a_sem, (0,), mate),
            remote(msg.at[cx * 2 + 1 - core], got.at[1], a_sem, (1,), mate)]
    for copy in swap:
        copy.start()

    gain1 = gain[layer, 1:2, :].astype(f32)
    shift1 = shift[layer, 1:2, :].astype(f32)
    own = pl.ds(pl.multiple_of(core * ROWS, ROWS), ROWS)
    theirs = pl.ds(pl.multiple_of((1 - core) * ROWS, ROWS), ROWS)

    def all_rows(x_, c_):
        return pl.ds(pl.multiple_of(x_ * HALF + c_ * ROWS, ROWS), ROWS)

    xrow[...] = x[all_rows(cx, core), :].astype(f32) if layer == 0 else x[...]
    lane = lax.broadcasted_iota(jnp.int32, (8, HD), 1)

    def merge(one, two, put, stat_out=None):
        stats = [ref[pl.ds(HPC * HALF, 8), :] for ref in (one, two)]
        new_stat = jnp.zeros((8, HD), f32)
        for g in range(HPC):
            for i in range(HALF // 8):
                at = 2 * (g * (HALF // 8) + i)
                peaks = [jnp.broadcast_to(st[:, at:at + 1], (8, HD)) for st in stats]
                tots = [jnp.broadcast_to(st[:, at + 1:at + 2], (8, HD)) for st in stats]
                top = jnp.maximum(peaks[0], peaks[1])
                scale = [jnp.exp(p - top) for p in peaks]
                rows = pl.ds(g * HALF + i * 8, 8)
                num = one[rows, :] * scale[0] + two[rows, :] * scale[1]
                den = tots[0] * scale[0] + tots[1] * scale[1]
                put(g, i, num, den)
                if stat_out is not None:
                    new_stat = jnp.where(lane == at, top, new_stat)
                    new_stat = jnp.where(lane == at + 1, den, new_stat)
        if stat_out is not None:
            stat_out[pl.ds(HPC * HALF, 8), :] = new_stat

    def put_part(ref):
        def put(g, i, num, den):
            ref[pl.ds(g * HALF + i * 8, 8), :] = num
        return put

    def put_out(g, i, num, den):
        o_buf[pl.ds(i * 8, 8), g * HD:(g + 1) * HD] = num / den

    swap[0].wait_recv()
    merge(msg.at[far], got.at[0], put_part(sent.at[0]), sent.at[0])
    cross = remote(sent.at[0], got.at[2], a_sem, (2,), x_dev)
    cross.start()
    swap[1].wait_recv()
    merge(msg.at[near], got.at[1], put_part(sent.at[1]), sent.at[1])
    cross.wait_recv()
    merge(sent.at[1], got.at[2], put_out)
    sends = swap + [cross]

    def reduce(ph, product, finish):
        first = [remote(part.at[ph, n, theirs, :], pair.at[ph, n], d_sem, (ph, n), mate) for n in range(RCH)]
        second = [remote(sums.at[ph, n], other.at[ph, n], y_sem, (ph, n), y_dev) for n in range(RCH)]
        for step in range(RCH + LAG):
            if step < RCH:
                part[ph, step] = product(step)
                first[step].start()
            if step >= LAG:
                n = step - LAG
                first[n].wait_recv()
                sums[ph, n] = part[ph, n, own, :] + pair[ph, n]
                second[n].start()
        for n in range(RCH):
            second[n].wait_recv()
            finish(n, sums[ph, n] + other[ph, n])
        return first + second

    def residual(n, total, bias):
        cols = slice(n * RW, (n + 1) * RW)
        v = xrow[:, cols] + total + bias[layer:layer + 1, cols].astype(f32)
        xrow[:, cols] = v.astype(bf16).astype(f32)

    wd_copy.wait()
    o = o_buf[...].astype(bf16)
    sends += reduce(0, lambda n: jnp.dot(o, wd[:, n * RW:(n + 1) * RW], preferred_element_type=f32),
                   lambda n, total: residual(n, total, b_dense))

    normed = norm_rows(xrow[...], gain1, shift1).astype(bf16).astype(f32)
    swap = []
    for n in range(NCH):
        ag[n, own, :] = normed[:, n * CW:(n + 1) * CW]
        here = ag.at[n, own, :]
        swap.append(remote(here, here, g_sem, (n,), mate))
        swap[n].start()
    cols_up = pl.ds(pl.multiple_of(core * F_LOC, F_LOC), F_LOC)
    up[...] = jnp.broadcast_to(b_up[layer:layer + 1, cols_up].astype(f32), (HALF, F_LOC))
    for n in range(NCH):
        wu_copy(n).wait()
        swap[n].wait_recv()
        up[...] += jnp.dot(ag[n].astype(bf16), wu[n], preferred_element_type=f32)
        if layer == 0:
            wq_copy(n).start()

    pick = (lax.broadcasted_iota(jnp.int32, (256, 128), 0) == 2 * lax.broadcasted_iota(jnp.int32, (256, 128), 1))
    pick = jnp.where(pick, 1.0, 0.0).astype(bf16)
    for k in range(F_LOC // 256):
        a = up[:, k * 256:(k + 1) * 256]
        z = jnp.minimum(a, GELU_LIMIT)
        gate = z * jax.nn.sigmoid(1.702 * z)
        lin = jnp.clip(a, -GELU_LIMIT, GELU_LIMIT) + 1.0
        prod = (gate * pltpu.roll(lin, 255, 1)).astype(bf16)
        mbuf[:, k * 128:(k + 1) * 128] = jnp.dot(prod, pick, preferred_element_type=f32).astype(bf16)
    wn_copy.wait()
    m = mbuf[...]
    sends += swap

    def spread(n, value):
        full[n, all_rows(cx, core), :] = value
        here = full.at[n, all_rows(cx, core), :]
        for k, peer in enumerate((x_dev, mate)):
            copy = remote(here, here, x_sem, (k, n), peer)
            copy.start()
            sends.append(copy)

    def collect(chunks, use):
        for n in range(chunks):
            there = full.at[n, all_rows(ox, core), :]
            remote(there, there, x_sem, (0, n), x_dev).wait_recv()
            copy = remote(there, there, x_sem, (2, n), mate)
            copy.start()
            sends.append(copy)
        for n in range(chunks):
            for k, x_ in ((1, cx), (2, ox)):
                there = full.at[n, all_rows(x_, 1 - core), :]
                remote(there, there, x_sem, (k, n), mate).wait_recv()
            use(n)

    def take_down(n, total):
        residual(n, total, b_down)
        if layer == 1:
            spread(n, xrow[:, n * RW:(n + 1) * RW])

    sends += reduce(1, lambda n: jnp.dot(m, wn[:, n * RW:(n + 1) * RW], preferred_element_type=f32), take_down)
    if layer == 0:
        x_out[...] = xrow[...]
        u = norm_rows(xrow[...], gain[1, 0:1, :].astype(f32), shift[1, 0:1, :].astype(f32)).astype(bf16)
        for i in range(NCH):
            wq_copy(i).wait()
        for n in range(QCH):
            cols = slice(n * QC, (n + 1) * QC)
            r = jnp.broadcast_to(b_qkv[1:2, cols].astype(f32), (ROWS, QC))
            for i in range(NCH):
                r += jnp.dot(u[:, i * CW:(i + 1) * CW], wu[i, :, cols], preferred_element_type=f32)
            spread(n, r)

        def use(n):
            out[n] = full[n]
    else:
        def use(n):
            out[:, n * RW:(n + 1) * RW] = full[n].astype(bf16)

    collect(QCH if layer == 0 else RCH, use)
    for copy in sends:
        copy.wait_send()


def rest_call(layer, msg, x, gain, shift, b_dense, b_up, b_down, w_dense, w_up, w_down, *qkv):
    vm = pl.BlockSpec(memory_space=pltpu.VMEM)
    hbm = pl.BlockSpec(memory_space=pltpu.HBM)
    if layer == 0:
        in_specs = [vm] * 7 + [hbm] * 3 + [vm, hbm]
        out_shape = (jax.ShapeDtypeStruct((ROWS, D), f32), jax.ShapeDtypeStruct((QCH, NB, QC), f32))
        out_specs = (vm, vm)
    else:
        in_specs = [vm] * 7 + [hbm] * 3
        out_shape = jax.ShapeDtypeStruct((NB, D), bf16)
        out_specs = vm
    return pl.pallas_call(
        functools.partial(rest_kernel, layer),
        out_shape=out_shape,
        in_specs=in_specs,
        out_specs=out_specs,
        scratch_shapes=[
            pltpu.VMEM((DR, D), bf16),
            pltpu.VMEM((NCH, CW, F_LOC), bf16),
            pltpu.VMEM((M_LOC, D), bf16),
            pltpu.VMEM((3, MSG, HD), f32),
            pltpu.VMEM((2, MSG, HD), f32),
            pltpu.VMEM((HALF, DR), f32),
            pltpu.VMEM((2, RCH, HALF, RW), f32),
            pltpu.VMEM((2, RCH, ROWS, RW), f32),
            pltpu.VMEM((2, RCH, ROWS, RW), f32),
            pltpu.VMEM((2, RCH, ROWS, RW), f32),
            pltpu.VMEM((NCH, HALF, CW), f32),
            pltpu.VMEM((QCH, NB, QC) if layer == 0 else (RCH, NB, RW), f32),
            pltpu.VMEM((ROWS, D), f32),
            pltpu.VMEM((HALF, F_LOC), f32),
            pltpu.VMEM((HALF, M_LOC), bf16),
            pltpu.SemaphoreType.DMA((2 + 2 * NCH,)),
            pltpu.SemaphoreType.DMA((2, 3)),
            pltpu.SemaphoreType.DMA((2, 2, RCH)),
            pltpu.SemaphoreType.DMA((2, 2, RCH)),
            pltpu.SemaphoreType.DMA((2, NCH)),
            pltpu.SemaphoreType.DMA((2, 3, RCH)),
        ],
        compiler_params=pltpu.CompilerParams(vmem_limit_bytes=VMEM_BYTES, collective_id=layer, has_side_effects=True),
        name=f'rest{layer}',
    )(msg, x, gain, shift, b_dense, b_up, b_down, w_dense, w_up, w_down, *qkv)


def solution(mesh):
    cache_spec = P(None, 'dp', 'sp', 'tp', None)
    in_specs = (P('dp', None), P('dp'), cache_spec, cache_spec, P(), P(), P(None, None, 'tp'), P(None, 'tp'), P(None, 'tp', None), P(), P(None, None, 'tp'), P(None, 'tp'), P(None, 'tp', None), P())
    out_specs = (P('dp', None), cache_spec, cache_spec)

    def device_step(hidden, positions, k_cache, v_cache, ln_gain, ln_bias, w_qkv, b_qkv, w_dense, b_dense, w_up, b_up, w_down, b_down):
        shape = k_cache.shape
        flat = (2, NB, SLOTS * KVL, HD)
        k_cache = k_cache.reshape(flat)
        v_cache = v_cache.reshape(flat)
        shared = (ln_gain, ln_bias, b_dense, b_up, b_down, w_dense, w_up, w_down)
        msg, *caches = attn_call(0, positions, (hidden, ln_gain, ln_bias, b_qkv, w_qkv), k_cache, v_cache, None)
        rows, qkv = rest_call(0, msg, hidden, *shared, b_qkv, w_qkv)
        msg, *caches = attn_call(1, positions, (qkv,), k_cache, v_cache, caches)
        hidden = rest_call(1, msg, rows, *shared)
        return hidden, caches[0].reshape(shape), caches[1].reshape(shape)

    return jax.shard_map(device_step, mesh=mesh, in_specs=in_specs, out_specs=out_specs, check_vma=False)
```

```python
import functools
import math

import jax
import jax.numpy as jnp
from jax import lax
from jax.experimental import pallas as pl
from jax.experimental.pallas import tpu as pltpu
from jax.sharding import PartitionSpec as P

BLOCK_SIZE = 64
LOCAL_BLOCKS = 16
VERT_STRIDE = 8
ROPE_THETA = 1000000.0
GELU_LIMIT = 20.0
NORM_EPS = 0.00001
MASKED = -1e30
MESH = pl.DeviceIdType.MESH

NB = 64
D = 3072
HD = 128
KVL = 4
GRP = 3
SLOTS = 64
QW = KVL * (GRP + 2) * HD
QROWS = 16
KCH = 6
KCS = D // KCH
G = 8
NG = NB // G
GS = 16
HALF = NB // 2
HPC = 6
MSG = HPC * HALF + 8
MSG_ROOM = 160
ROWS = HALF // 2
F_LOC = 4096
M_LOC = F_LOC // 2
NCH = 6
CW = D // NCH
QCH = 4
QC = QW // QCH
DR = HPC * HD
RCH = 6
RW = D // RCH
LAG = 2
VMEM_BYTES = 52 * 1024 * 1024

f32 = jnp.float32
bf16 = jnp.bfloat16


def norm_rows(rows, gain, shift):
    mean = jnp.mean(rows, axis=-1, keepdims=True)
    cent = rows - mean
    var = jnp.mean(jnp.square(cent), axis=-1, keepdims=True)
    return (cent * lax.rsqrt(var + NORM_EPS)) * gain + shift


def rope_tables(pos):
    half = HD // 2
    row = lax.broadcasted_iota(jnp.int32, (8, HD), 0)
    lane = lax.broadcasted_iota(jnp.int32, (NB, HD), 1)
    groups = []
    for i in range(NB // 8):
        at = jnp.zeros((8, HD), jnp.int32)
        for r in range(8):
            at = jnp.where(row == r, pos[i * 8 + r], at)
        groups.append(at)
    where = jnp.concatenate(groups, axis=0).astype(f32)
    power = (lane % half).astype(f32) * (2.0 / HD)
    angles = where * jnp.exp(power * -math.log(ROPE_THETA))
    sin = jnp.sin(angles)
    return jnp.cos(angles), jnp.where(lane < half, -sin, sin)


def attn_kernel(layer, pos, *rest):
    if layer == 0:
        x, gain, shift, b_qkv, w_hbm, kc_hbm, vc_hbm, *rest = rest
    else:
        acc, kc_hbm, vc_hbm, _, _, *rest = rest
    msg, ko_hbm, vo_hbm, kbuf, vbuf, qs, kns, vns, os, ms, ls, ksem, vsem, osem, *rest = rest
    sp = lax.axis_index('sp')
    tp = lax.axis_index('tp')
    base = sp * SLOTS

    def in_copy(hbm, buf, sem, i):
        return pltpu.make_async_copy(hbm.at[layer, pl.ds(i * G, G)], buf.at[pl.ds(i * G, G)], sem.at[i])

    def out_copy(buf, hbm, j, i):
        return pltpu.make_async_copy(buf.at[pl.ds(i * G, G)], hbm.at[layer, pl.ds(i * G, G)], osem.at[j, i])

    def fetch_cache():
        for i in range(NG):
            in_copy(kc_hbm, kbuf, ksem, i).start(priority=0)
            in_copy(vc_hbm, vbuf, vsem, i).start(priority=1)

    if layer == 0:
        w, u, acc, wsem, *places, msg_buf, small_sem = rest
        msg_hbm, msg = msg, msg_buf
        small = [pltpu.make_async_copy(src, dst, small_sem.at[i]) for i, (src, dst) in enumerate(zip((pos, x, gain, shift, b_qkv), places))]
        for copy in small:
            copy.start()
        pos, x, gain, shift, b_qkv = places

        def w_copy(i):
            return pltpu.make_async_copy(w_hbm.at[layer, pl.ds(i * KCS, KCS), :], w.at[i], wsem.at[i])

        for i in range(KCH):
            w_copy(i).start(priority=i % 2)
        fetch_cache()
        for copy in small:
            copy.wait()
        g_row = gain[layer, 0:1, :].astype(f32)
        s_row = shift[layer, 0:1, :].astype(f32)
        for i in range(NB // 16):
            rows = x[pl.ds(i * 16, 16), :].astype(f32)
            normed = norm_rows(rows, g_row, s_row).astype(bf16)
            for j in range(KCH):
                u[j, pl.ds(i * 16, 16), :] = normed[:, j * KCS:(j + 1) * KCS]
        acc[...] = jnp.broadcast_to(b_qkv[layer:layer + 1, :].astype(f32), (NB, QW))
    else:
        fetch_cache()
    qs[...] = jnp.zeros_like(qs)
    cos_t, sin_t = rope_tables(pos)
    if layer == 0:
        def qkv_step(i, carry):
            w_copy(i).wait()
            acc[...] += jnp.dot(u[i], w[i], preferred_element_type=f32)
            return carry

        lax.fori_loop(0, KCH, qkv_step, 0)

    for c in range(KVL):
        for j in range(GRP + 2):
            if layer == 0:
                col = (c * (GRP + 2) + j) * HD
                tile = acc[:, col:col + HD]
            else:
                tile = acc[c, :, j * HD:(j + 1) * HD]
            if j <= GRP:
                tile = tile * cos_t + pltpu.roll(tile, HD // 2, 1) * sin_t
            for i in range(NB // 8):
                part = tile[i * 8:(i + 1) * 8]
                if j < GRP:
                    qs[pl.ds(i * 8 * QROWS + c * GRP + j, 8, stride=QROWS), :] = part
                else:
                    dst = kns if j == GRP else vns
                    dst[pl.ds(i * 64 + c, 8, stride=8), :] = part
                    dst[pl.ds(i * 64 + c + 4, 8, stride=8), :] = part

    row_h = lax.broadcasted_iota(jnp.int32, (QROWS, SLOTS * KVL), 0)
    col_i = lax.broadcasted_iota(jnp.int32, (QROWS, SLOTS * KVL), 1)
    slot_of = jnp.where(row_h // GRP == col_i % KVL, col_i // KVL, 1 << 20)
    head_id = tp * KVL * GRP + row_h
    vertical = (sp + head_id + 1) % VERT_STRIDE == 0
    sub_row = lax.broadcasted_iota(jnp.int32, (16, HD), 0) // KVL

    def patch(buf, new, b):
        at = pos[b] - base
        atc = jnp.clip(at, 0, SLOTS - 1)
        hit = jnp.logical_and(at >= 0, at < SLOTS)
        put = sub_row == jnp.where(hit, atc % KVL, -1)
        r0 = pl.multiple_of((atc // KVL) * 16, 16)
        new8 = new[b * 8:b * 8 + 8, :]
        new16 = jnp.concatenate([new8, new8], axis=0)
        old = buf[b, pl.ds(r0, 16), :].astype(f32)
        buf[b, pl.ds(r0, 16), :] = jnp.where(put, new16, old).astype(bf16)

    def score(step):
        seqs = range(step * GS, (step + 1) * GS)
        for b in seqs:
            patch(kbuf, kns, b)
        return [lax.dot_general(qs[b * QROWS:(b + 1) * QROWS, :].astype(bf16), kbuf[b], (((1,), (1,)), ((), ())),
                                preferred_element_type=f32) for b in seqs]

    def keep_of(b):
        at = pos[b] - base
        if layer == 0:
            near = pos[b] // BLOCK_SIZE - sp < LOCAL_BLOCKS
            return slot_of <= jnp.where(vertical, at, jnp.where(near, at, -1))
        return slot_of <= at

    def mix(step, scores):
        seqs = range(step * GS, (step + 1) * GS)
        for b in seqs:
            patch(vbuf, vns, b)
        keeps = [keep_of(b) for b in seqs]
        scores = [jnp.where(keep, s * (1.0 / HD), MASKED) for keep, s in zip(keeps, scores)]
        peaks = [jnp.max(s, axis=1, keepdims=True) for s in scores]
        weights = [jnp.where(keep, jnp.exp(s - peak), 0.0) for keep, s, peak in zip(keeps, scores, peaks)]
        outs = [jnp.dot(wt.astype(bf16), vbuf[b], preferred_element_type=f32) for b, wt in zip(seqs, weights)]
        sums = [jnp.sum(wt, axis=1, keepdims=True) for wt in weights]
        for j, b in enumerate(seqs):
            rows = slice(b * QROWS, (b + 1) * QROWS)
            ms[rows, :] = jnp.broadcast_to(peaks[j], (QROWS, HD))
            ls[rows, :] = jnp.broadcast_to(sums[j], (QROWS, HD))
            os[rows, :] = outs[j]

    per = GS // G
    steps = NB // GS
    for j in range(per):
        in_copy(kc_hbm, kbuf, ksem, j).wait()
    scores = score(0)
    for step in range(steps):
        for j in range(step * per, (step + 1) * per):
            in_copy(vc_hbm, vbuf, vsem, j).wait()
            if step + 1 < steps:
                in_copy(kc_hbm, kbuf, ksem, j + per).wait()
        later = score(step + 1) if step + 1 < steps else None
        mix(step, scores)
        scores = later
        for j in range(step * per, (step + 1) * per):
            out_copy(kbuf, ko_hbm, 0, j).start()
            out_copy(vbuf, vo_hbm, 1, j).start(priority=1)

    lane = lax.broadcasted_iota(jnp.int32, (8, HD), 1)
    for half in range(2):
        for c in range(2):
            stat = jnp.zeros((8, HD), f32)
            for g in range(HPC):
                for i in range(HALF // 8):
                    rows = pl.ds((half * HALF + i * 8) * QROWS + c * HPC + g, 8, stride=QROWS)
                    at = 2 * (g * (HALF // 8) + i)
                    msg[half * 2 + c, pl.ds(g * HALF + i * 8, 8), :] = os[rows, :]
                    stat = jnp.where(lane == at, ms[rows, :], stat)
                    stat = jnp.where(lane == at + 1, ls[rows, :], stat)
            msg[half * 2 + c, pl.ds(HPC * HALF, 8), :] = stat
    if layer == 0:
        send = pltpu.make_async_copy(msg, msg_hbm.at[pl.ds(0, KVL)], small_sem.at[5])
        send.start()
    for i in range(NG):
        out_copy(kbuf, ko_hbm, 0, i).wait()
        out_copy(vbuf, vo_hbm, 1, i).wait()
    if layer == 0:
        send.wait()


def attn_call(layer, pos, operands, k_cache, v_cache, prev):
    vm = pl.BlockSpec(memory_space=pltpu.VMEM)
    hbm = pl.BlockSpec(memory_space=pltpu.HBM)
    args = [pos, *operands, k_cache, v_cache]
    if layer == 0:
        specs = [hbm] * 8
        alias = {}
        extra = [
            pltpu.VMEM((KCH, KCS, QW), bf16),
            pltpu.VMEM((KCH, NB, KCS), bf16),
            pltpu.VMEM((NB, QW), f32),
            pltpu.SemaphoreType.DMA((KCH,)),
            pltpu.SMEM(pos.shape, jnp.int32),
            *[pltpu.VMEM(arr.shape, bf16) for arr in operands[:4]],
            pltpu.VMEM((KVL, MSG, HD), f32),
            pltpu.SemaphoreType.DMA((6,)),
        ]
        limit = 60 * 1024 * 1024
    else:
        args += list(prev)
        specs = [pl.BlockSpec(memory_space=pltpu.SMEM), vm] + [hbm] * 4
        alias = {4: 1, 5: 2}
        extra = []
        limit = VMEM_BYTES
    cache = jax.ShapeDtypeStruct(k_cache.shape, bf16)
    return pl.pallas_call(
        functools.partial(attn_kernel, layer),
        out_shape=(jax.ShapeDtypeStruct((MSG_ROOM if layer == 0 else KVL, MSG, HD), f32), cache, cache),
        in_specs=specs,
        out_specs=(hbm if layer == 0 else vm, hbm, hbm),
        scratch_shapes=[
            pltpu.VMEM((NB, SLOTS * KVL, HD), bf16),
            pltpu.VMEM((NB, SLOTS * KVL, HD), bf16),
            pltpu.VMEM((NB * QROWS, HD), f32),
            pltpu.VMEM((NB * 8, HD), f32),
            pltpu.VMEM((NB * 8, HD), f32),
            pltpu.VMEM((NB * QROWS, HD), f32),
            pltpu.VMEM((NB * QROWS, HD), f32),
            pltpu.VMEM((NB * QROWS, HD), f32),
            pltpu.SemaphoreType.DMA((NG,)),
            pltpu.SemaphoreType.DMA((NG,)),
            pltpu.SemaphoreType.DMA((2, NG)),
            *extra,
        ],
        input_output_aliases=alias,
        compiler_params=pltpu.CompilerParams(vmem_limit_bytes=limit),
        name=f'attn{layer}',
    )(*args)


def rest_kernel(layer, msg, x, gain, shift, b_dense, b_up, b_down, wd_hbm, wu_hbm, wn_hbm, *rest):
    if layer == 0:
        b_qkv, wq_hbm, x_out, out, *rest = rest
        msg_hbm, (*rest, msg) = msg, rest
    else:
        out, *rest = rest
    (wd, wu, wn, got, sent, o_buf, part, pair, sums, other, ag, full, xrow, up, mbuf,
     wsem, a_sem, d_sem, y_sem, g_sem, x_sem) = rest
    dp = lax.axis_index('dp')
    tp = lax.axis_index('tp')
    sp = lax.axis_index('sp')
    core = sp % 2
    cx = sp // 2
    ox = 1 - cx
    mate = (dp, tp, cx * 2 + 1 - core)
    x_dev = (dp, tp, ox * 2 + core)
    y_dev = (dp, 1 - tp, sp)

    def load(src, dst, i):
        return pltpu.make_async_copy(src, dst, wsem.at[i])

    wd_copy = load(wd_hbm.at[layer, pl.ds(pl.multiple_of(core * DR, DR), DR), :], wd, 0)

    def wu_copy(i):
        return load(wu_hbm.at[layer, pl.ds(i * CW, CW), pl.ds(pl.multiple_of(core * F_LOC, F_LOC), F_LOC)], wu.at[i], 1 + i)

    wn_copy = load(wn_hbm.at[layer, pl.ds(pl.multiple_of(core * M_LOC, M_LOC), M_LOC), :], wn, 1 + NCH)

    def wq_copy(i):
        return load(wq_hbm.at[1, pl.ds(i * CW, CW), :], wu.at[i, :, pl.ds(0, QW)], 2 + NCH + i)

    barrier = pltpu.get_barrier_semaphore()
    for peer in (mate, x_dev, y_dev):
        pl.semaphore_signal(barrier, inc=1, device_id=peer, device_id_type=MESH)
    if layer == 0:
        msg_copy = load(msg_hbm.at[pl.ds(0, KVL)], msg, 2 + 2 * NCH)
        msg_copy.start()
    wd_copy.start()
    for i in range(NCH):
        wu_copy(i).start()
    wn_copy.start()
    pl.semaphore_wait(barrier, 3)
    if layer == 0:
        msg_copy.wait()

    def remote(src, dst, sems, idx, peer):
        return pltpu.make_async_remote_copy(
            src_ref=src, dst_ref=dst, send_sem=sems.at[(0,) + idx], recv_sem=sems.at[(1,) + idx],
            device_id=peer, device_id_type=MESH)

    near = cx * 2 + core
    far = ox * 2 + core
    swap = [remote(msg.at[ox * 2 + 1 - core], got.at[0], a_sem, (0,), mate),
            remote(msg.at[cx * 2 + 1 - core], got.at[1], a_sem, (1,), mate)]
    for copy in swap:
        copy.start()

    gain1 = gain[layer, 1:2, :].astype(f32)
    shift1 = shift[layer, 1:2, :].astype(f32)
    own = pl.ds(pl.multiple_of(core * ROWS, ROWS), ROWS)
    theirs = pl.ds(pl.multiple_of((1 - core) * ROWS, ROWS), ROWS)

    def all_rows(x_, c_):
        return pl.ds(pl.multiple_of(x_ * HALF + c_ * ROWS, ROWS), ROWS)

    xrow[...] = x[all_rows(cx, core), :].astype(f32) if layer == 0 else x[...]
    lane = lax.broadcasted_iota(jnp.int32, (8, HD), 1)

    def merge(one, two, put, stat_out=None):
        stats = [ref[pl.ds(HPC * HALF, 8), :] for ref in (one, two)]
        new_stat = jnp.zeros((8, HD), f32)
        for g in range(HPC):
            for i in range(HALF // 8):
                at = 2 * (g * (HALF // 8) + i)
                peaks = [jnp.broadcast_to(st[:, at:at + 1], (8, HD)) for st in stats]
                tots = [jnp.broadcast_to(st[:, at + 1:at + 2], (8, HD)) for st in stats]
                top = jnp.maximum(peaks[0], peaks[1])
                scale = [jnp.exp(p - top) for p in peaks]
                rows = pl.ds(g * HALF + i * 8, 8)
                num = one[rows, :] * scale[0] + two[rows, :] * scale[1]
                den = tots[0] * scale[0] + tots[1] * scale[1]
                put(g, i, num, den)
                if stat_out is not None:
                    new_stat = jnp.where(lane == at, top, new_stat)
                    new_stat = jnp.where(lane == at + 1, den, new_stat)
        if stat_out is not None:
            stat_out[pl.ds(HPC * HALF, 8), :] = new_stat

    def put_part(ref):
        def put(g, i, num, den):
            ref[pl.ds(g * HALF + i * 8, 8), :] = num
        return put

    def put_out(g, i, num, den):
        o_buf[pl.ds(i * 8, 8), g * HD:(g + 1) * HD] = num / den

    swap[0].wait_recv()
    merge(msg.at[far], got.at[0], put_part(sent.at[0]), sent.at[0])
    cross = remote(sent.at[0], got.at[2], a_sem, (2,), x_dev)
    cross.start()
    swap[1].wait_recv()
    merge(msg.at[near], got.at[1], put_part(sent.at[1]), sent.at[1])
    cross.wait_recv()
    merge(sent.at[1], got.at[2], put_out)
    sends = swap + [cross]

    def reduce(ph, product, finish):
        first = [remote(part.at[ph, n, theirs, :], pair.at[ph, n], d_sem, (ph, n), mate) for n in range(RCH)]
        second = [remote(sums.at[ph, n], other.at[ph, n], y_sem, (ph, n), y_dev) for n in range(RCH)]
        for step in range(RCH + LAG):
            if step < RCH:
                part[ph, step] = product(step)
                first[step].start()
            if step >= LAG:
                n = step - LAG
                first[n].wait_recv()
                sums[ph, n] = part[ph, n, own, :] + pair[ph, n]
                second[n].start()
        for n in range(RCH):
            second[n].wait_recv()
            finish(n, sums[ph, n] + other[ph, n])
        return first + second

    def residual(n, total, bias):
        cols = slice(n * RW, (n + 1) * RW)
        v = xrow[:, cols] + total + bias[layer:layer + 1, cols].astype(f32)
        xrow[:, cols] = v.astype(bf16).astype(f32)

    wd_copy.wait()
    o = o_buf[...].astype(bf16)
    sends += reduce(0, lambda n: jnp.dot(o, wd[:, n * RW:(n + 1) * RW], preferred_element_type=f32),
                   lambda n, total: residual(n, total, b_dense))

    normed = norm_rows(xrow[...], gain1, shift1).astype(bf16).astype(f32)
    swap = []
    for n in range(NCH):
        ag[n, own, :] = normed[:, n * CW:(n + 1) * CW]
        here = ag.at[n, own, :]
        swap.append(remote(here, here, g_sem, (n,), mate))
        swap[n].start()
    cols_up = pl.ds(pl.multiple_of(core * F_LOC, F_LOC), F_LOC)
    up[...] = jnp.broadcast_to(b_up[layer:layer + 1, cols_up].astype(f32), (HALF, F_LOC))
    for n in range(NCH):
        wu_copy(n).wait()
        swap[n].wait_recv()
        up[...] += jnp.dot(ag[n].astype(bf16), wu[n], preferred_element_type=f32)
        if layer == 0:
            wq_copy(n).start()

    pick = (lax.broadcasted_iota(jnp.int32, (256, 128), 0) == 2 * lax.broadcasted_iota(jnp.int32, (256, 128), 1))
    pick = jnp.where(pick, 1.0, 0.0).astype(bf16)
    for k in range(F_LOC // 256):
        a = up[:, k * 256:(k + 1) * 256]
        z = jnp.minimum(a, GELU_LIMIT)
        gate = z * jax.nn.sigmoid(1.702 * z)
        lin = jnp.clip(a, -GELU_LIMIT, GELU_LIMIT) + 1.0
        prod = (gate * pltpu.roll(lin, 255, 1)).astype(bf16)
        mbuf[:, k * 128:(k + 1) * 128] = jnp.dot(prod, pick, preferred_element_type=f32).astype(bf16)
    wn_copy.wait()
    m = mbuf[...]
    sends += swap

    def spread(n, value):
        full[n, all_rows(cx, core), :] = value
        here = full.at[n, all_rows(cx, core), :]
        for k, peer in enumerate((x_dev, mate)):
            copy = remote(here, here, x_sem, (k, n), peer)
            copy.start()
            sends.append(copy)

    def collect(chunks, use):
        for n in range(chunks):
            there = full.at[n, all_rows(ox, core), :]
            remote(there, there, x_sem, (0, n), x_dev).wait_recv()
            copy = remote(there, there, x_sem, (2, n), mate)
            copy.start()
            sends.append(copy)
        for n in range(chunks):
            for k, x_ in ((1, cx), (2, ox)):
                there = full.at[n, all_rows(x_, 1 - core), :]
                remote(there, there, x_sem, (k, n), mate).wait_recv()
            use(n)

    def take_down(n, total):
        residual(n, total, b_down)
        if layer == 1:
            spread(n, xrow[:, n * RW:(n + 1) * RW])

    sends += reduce(1, lambda n: jnp.dot(m, wn[:, n * RW:(n + 1) * RW], preferred_element_type=f32), take_down)
    if layer == 0:
        x_out[...] = xrow[...]
        u = norm_rows(xrow[...], gain[1, 0:1, :].astype(f32), shift[1, 0:1, :].astype(f32)).astype(bf16)
        for i in range(NCH):
            wq_copy(i).wait()
        for n in range(QCH):
            cols = slice(n * QC, (n + 1) * QC)
            r = jnp.broadcast_to(b_qkv[1:2, cols].astype(f32), (ROWS, QC))
            for i in range(NCH):
                r += jnp.dot(u[:, i * CW:(i + 1) * CW], wu[i, :, cols], preferred_element_type=f32)
            spread(n, r)

        def use(n):
            out[n] = full[n]
    else:
        def use(n):
            out[:, n * RW:(n + 1) * RW] = full[n].astype(bf16)

    collect(QCH if layer == 0 else RCH, use)
    for copy in sends:
        copy.wait_send()


def rest_call(layer, msg, x, gain, shift, b_dense, b_up, b_down, w_dense, w_up, w_down, *qkv):
    vm = pl.BlockSpec(memory_space=pltpu.VMEM)
    hbm = pl.BlockSpec(memory_space=pltpu.HBM)
    if layer == 0:
        in_specs = [hbm] + [vm] * 6 + [hbm] * 3 + [vm, hbm]
        out_shape = (jax.ShapeDtypeStruct((ROWS, D), f32), jax.ShapeDtypeStruct((QCH, NB, QC), f32))
        out_specs = (vm, vm)
    else:
        in_specs = [vm] * 7 + [hbm] * 3
        out_shape = jax.ShapeDtypeStruct((NB, D), bf16)
        out_specs = vm
    return pl.pallas_call(
        functools.partial(rest_kernel, layer),
        out_shape=out_shape,
        in_specs=in_specs,
        out_specs=out_specs,
        scratch_shapes=[
            pltpu.VMEM((DR, D), bf16),
            pltpu.VMEM((NCH, CW, F_LOC), bf16),
            pltpu.VMEM((M_LOC, D), bf16),
            pltpu.VMEM((3, MSG, HD), f32),
            pltpu.VMEM((2, MSG, HD), f32),
            pltpu.VMEM((HALF, DR), f32),
            pltpu.VMEM((2, RCH, HALF, RW), f32),
            pltpu.VMEM((2, RCH, ROWS, RW), f32),
            pltpu.VMEM((2, RCH, ROWS, RW), f32),
            pltpu.VMEM((2, RCH, ROWS, RW), f32),
            pltpu.VMEM((NCH, HALF, CW), f32),
            pltpu.VMEM((QCH, NB, QC) if layer == 0 else (RCH, NB, RW), f32),
            pltpu.VMEM((ROWS, D), f32),
            pltpu.VMEM((HALF, F_LOC), f32),
            pltpu.VMEM((HALF, M_LOC), bf16),
            pltpu.SemaphoreType.DMA((3 + 2 * NCH,)),
            pltpu.SemaphoreType.DMA((2, 3)),
            pltpu.SemaphoreType.DMA((2, 2, RCH)),
            pltpu.SemaphoreType.DMA((2, 2, RCH)),
            pltpu.SemaphoreType.DMA((2, NCH)),
            pltpu.SemaphoreType.DMA((2, 3, RCH)),
            *([pltpu.VMEM((KVL, MSG, HD), f32)] if layer == 0 else []),
        ],
        compiler_params=pltpu.CompilerParams(vmem_limit_bytes=VMEM_BYTES, collective_id=layer, has_side_effects=True),
        name=f'rest{layer}',
    )(msg, x, gain, shift, b_dense, b_up, b_down, w_dense, w_up, w_down, *qkv)


def solution(mesh):
    cache_spec = P(None, 'dp', 'sp', 'tp', None)
    in_specs = (P('dp', None), P('dp'), cache_spec, cache_spec, P(), P(), P(None, None, 'tp'), P(None, 'tp'), P(None, 'tp', None), P(), P(None, None, 'tp'), P(None, 'tp'), P(None, 'tp', None), P())
    out_specs = (P('dp', None), cache_spec, cache_spec)

    def device_step(hidden, positions, k_cache, v_cache, ln_gain, ln_bias, w_qkv, b_qkv, w_dense, b_dense, w_up, b_up, w_down, b_down):
        shape = k_cache.shape
        flat = (2, NB, SLOTS * KVL, HD)
        k_cache = k_cache.reshape(flat)
        v_cache = v_cache.reshape(flat)
        shared = (ln_gain, ln_bias, b_dense, b_up, b_down, w_dense, w_up, w_down)
        msg, *caches = attn_call(0, positions, (hidden, ln_gain, ln_bias, b_qkv, w_qkv), k_cache, v_cache, None)
        rows, qkv = rest_call(0, msg, hidden, *shared, b_qkv, w_qkv)
        msg, *caches = attn_call(1, positions, (qkv,), k_cache, v_cache, caches)
        hidden = rest_call(1, msg, rows, *shared)
        return hidden, caches[0].reshape(shape), caches[1].reshape(shape)

    return jax.shard_map(device_step, mesh=mesh, in_specs=in_specs, out_specs=out_specs, check_vma=False)
```

```python
import functools
import math

import jax
import jax.numpy as jnp
from jax import lax
from jax.experimental import pallas as pl
from jax.experimental.pallas import tpu as pltpu
from jax.sharding import PartitionSpec as P

BLOCK_SIZE = 64
LOCAL_BLOCKS = 16
VERT_STRIDE = 8
ROPE_THETA = 1000000.0
GELU_LIMIT = 20.0
NORM_EPS = 0.00001
MASKED = -1e30
MESH = pl.DeviceIdType.MESH

NB = 64
D = 3072
HD = 128
KVL = 4
GRP = 3
SLOTS = 64
QW = KVL * (GRP + 2) * HD
QROWS = 16
KCH = 6
KCS = D // KCH
G = 8
NG = NB // G
GS = 16
HALF = NB // 2
HPC = 6
MSG = HPC * HALF + 8
MSG_ROOM = 160
ROWS = HALF // 2
F_LOC = 4096
M_LOC = F_LOC // 2
NCH = 3
CW = D // NCH
QCH = 5
QC = QW // QCH
DR = HPC * HD
RCH = 6
RW = D // RCH
LAG = 2
VMEM_BYTES = 52 * 1024 * 1024

f32 = jnp.float32
bf16 = jnp.bfloat16


def norm_rows(rows, gain, shift):
    mean = jnp.mean(rows, axis=-1, keepdims=True)
    cent = rows - mean
    var = jnp.mean(jnp.square(cent), axis=-1, keepdims=True)
    return (cent * lax.rsqrt(var + NORM_EPS)) * gain + shift


def rope_tables(pos):
    half = HD // 2
    row = lax.broadcasted_iota(jnp.int32, (8, HD), 0)
    lane = lax.broadcasted_iota(jnp.int32, (NB, HD), 1)
    groups = []
    for i in range(NB // 8):
        at = jnp.zeros((8, HD), jnp.int32)
        for r in range(8):
            at = jnp.where(row == r, pos[i * 8 + r], at)
        groups.append(at)
    where = jnp.concatenate(groups, axis=0).astype(f32)
    power = (lane % half).astype(f32) * (2.0 / HD)
    angles = where * jnp.exp(power * -math.log(ROPE_THETA))
    sin = jnp.sin(angles)
    return jnp.cos(angles), jnp.where(lane < half, -sin, sin)


def attn_kernel(layer, pos, *rest):
    if layer == 0:
        x, gain, shift, b_qkv, w_hbm, kc_hbm, vc_hbm, *rest = rest
    else:
        acc, kc_hbm, vc_hbm, _, _, *rest = rest
    msg, ko_hbm, vo_hbm, kbuf, vbuf, qs, kns, vns, os, ms, ls, ksem, vsem, osem, *rest = rest
    sp = lax.axis_index('sp')
    tp = lax.axis_index('tp')
    base = sp * SLOTS

    def in_copy(hbm, buf, sem, i):
        return pltpu.make_async_copy(hbm.at[layer, pl.ds(i * G, G)], buf.at[pl.ds(i * G, G)], sem.at[i])

    def out_copy(buf, hbm, j, i):
        return pltpu.make_async_copy(buf.at[pl.ds(i * G, G)], hbm.at[layer, pl.ds(i * G, G)], osem.at[j, i])

    def fetch_cache():
        for i in range(NG):
            in_copy(kc_hbm, kbuf, ksem, i).start(priority=0)
            in_copy(vc_hbm, vbuf, vsem, i).start(priority=1)

    if layer == 0:
        w, u, acc, wsem, *places, msg_buf, small_sem = rest
        msg_hbm, msg = msg, msg_buf
        small = [pltpu.make_async_copy(src, dst, small_sem.at[i]) for i, (src, dst) in enumerate(zip((pos, x, gain, shift, b_qkv), places))]
        for copy in small:
            copy.start()
        pos, x, gain, shift, b_qkv = places

        def w_copy(i):
            return pltpu.make_async_copy(w_hbm.at[layer, pl.ds(i * KCS, KCS), :], w.at[i], wsem.at[i])

        for i in range(KCH):
            w_copy(i).start(priority=i % 2)
        fetch_cache()
        for copy in small:
            copy.wait()
        g_row = gain[layer, 0:1, :].astype(f32)
        s_row = shift[layer, 0:1, :].astype(f32)
        for i in range(NB // 16):
            rows = x[pl.ds(i * 16, 16), :].astype(f32)
            normed = norm_rows(rows, g_row, s_row).astype(bf16)
            for j in range(KCH):
                u[j, pl.ds(i * 16, 16), :] = normed[:, j * KCS:(j + 1) * KCS]
        acc[...] = jnp.broadcast_to(b_qkv[layer:layer + 1, :].astype(f32), (NB, QW))
    else:
        fetch_cache()
    qs[...] = jnp.zeros_like(qs)
    cos_t, sin_t = rope_tables(pos)
    if layer == 0:
        def qkv_step(i, carry):
            w_copy(i).wait()
            acc[...] += jnp.dot(u[i], w[i], preferred_element_type=f32)
            return carry

        lax.fori_loop(0, KCH, qkv_step, 0)

    for c in range(KVL):
        for j in range(GRP + 2):
            if layer == 0:
                col = (c * (GRP + 2) + j) * HD
                tile = acc[:, col:col + HD]
            else:
                head = c * (GRP + 2) + j
                tile = acc[head // (QC // HD), :, head % (QC // HD) * HD:(head % (QC // HD) + 1) * HD]
            if j <= GRP:
                tile = tile * cos_t + pltpu.roll(tile, HD // 2, 1) * sin_t
            for i in range(NB // 8):
                part = tile[i * 8:(i + 1) * 8]
                if j < GRP:
                    qs[pl.ds(i * 8 * QROWS + c * GRP + j, 8, stride=QROWS), :] = part
                else:
                    dst = kns if j == GRP else vns
                    dst[pl.ds(i * 64 + c, 8, stride=8), :] = part
                    dst[pl.ds(i * 64 + c + 4, 8, stride=8), :] = part

    row_h = lax.broadcasted_iota(jnp.int32, (QROWS, SLOTS * KVL), 0)
    col_i = lax.broadcasted_iota(jnp.int32, (QROWS, SLOTS * KVL), 1)
    slot_of = jnp.where(row_h // GRP == col_i % KVL, col_i // KVL, 1 << 20)
    head_id = tp * KVL * GRP + row_h
    vertical = (sp + head_id + 1) % VERT_STRIDE == 0
    sub_row = lax.broadcasted_iota(jnp.int32, (16, HD), 0) // KVL

    def patch(buf, new, b):
        at = pos[b] - base
        atc = jnp.clip(at, 0, SLOTS - 1)
        hit = jnp.logical_and(at >= 0, at < SLOTS)
        put = sub_row == jnp.where(hit, atc % KVL, -1)
        r0 = pl.multiple_of((atc // KVL) * 16, 16)
        new8 = new[b * 8:b * 8 + 8, :]
        new16 = jnp.concatenate([new8, new8], axis=0)
        old = buf[b, pl.ds(r0, 16), :].astype(f32)
        buf[b, pl.ds(r0, 16), :] = jnp.where(put, new16, old).astype(bf16)

    def score(step):
        seqs = range(step * GS, (step + 1) * GS)
        for b in seqs:
            patch(kbuf, kns, b)
        return [lax.dot_general(qs[b * QROWS:(b + 1) * QROWS, :].astype(bf16), kbuf[b], (((1,), (1,)), ((), ())),
                                preferred_element_type=f32) for b in seqs]

    def keep_of(b):
        at = pos[b] - base
        if layer == 0:
            near = pos[b] // BLOCK_SIZE - sp < LOCAL_BLOCKS
            return slot_of <= jnp.where(vertical, at, jnp.where(near, at, -1))
        return slot_of <= at

    def mix(step, scores):
        seqs = range(step * GS, (step + 1) * GS)
        for b in seqs:
            patch(vbuf, vns, b)
        keeps = [keep_of(b) for b in seqs]
        scores = [jnp.where(keep, s * (1.0 / HD), MASKED) for keep, s in zip(keeps, scores)]
        peaks = [jnp.max(s, axis=1, keepdims=True) for s in scores]
        weights = [jnp.where(keep, jnp.exp(s - peak), 0.0) for keep, s, peak in zip(keeps, scores, peaks)]
        outs = [jnp.dot(wt.astype(bf16), vbuf[b], preferred_element_type=f32) for b, wt in zip(seqs, weights)]
        sums = [jnp.sum(wt, axis=1, keepdims=True) for wt in weights]
        for j, b in enumerate(seqs):
            rows = slice(b * QROWS, (b + 1) * QROWS)
            ms[rows, :] = jnp.broadcast_to(peaks[j], (QROWS, HD))
            ls[rows, :] = jnp.broadcast_to(sums[j], (QROWS, HD))
            os[rows, :] = outs[j]

    per = GS // G
    steps = NB // GS
    for j in range(per):
        in_copy(kc_hbm, kbuf, ksem, j).wait()
    scores = score(0)
    for step in range(steps):
        for j in range(step * per, (step + 1) * per):
            in_copy(vc_hbm, vbuf, vsem, j).wait()
            if step + 1 < steps:
                in_copy(kc_hbm, kbuf, ksem, j + per).wait()
        later = score(step + 1) if step + 1 < steps else None
        mix(step, scores)
        scores = later
        for j in range(step * per, (step + 1) * per):
            if step == 0:
                out_copy(kbuf, ko_hbm, 0, j).start()
            if step + 1 < steps:
                out_copy(kbuf, ko_hbm, 0, j + per).start()
            out_copy(vbuf, vo_hbm, 1, j).start(priority=1)

    lane = lax.broadcasted_iota(jnp.int32, (8, HD), 1)
    for half in range(2):
        for c in range(2):
            stat = jnp.zeros((8, HD), f32)
            for g in range(HPC):
                for i in range(HALF // 8):
                    rows = pl.ds((half * HALF + i * 8) * QROWS + c * HPC + g, 8, stride=QROWS)
                    at = 2 * (g * (HALF // 8) + i)
                    msg[half * 2 + c, pl.ds(g * HALF + i * 8, 8), :] = os[rows, :]
                    stat = jnp.where(lane == at, ms[rows, :], stat)
                    stat = jnp.where(lane == at + 1, ls[rows, :], stat)
            msg[half * 2 + c, pl.ds(HPC * HALF, 8), :] = stat
    if layer == 0:
        send = pltpu.make_async_copy(msg, msg_hbm.at[pl.ds(0, KVL)], small_sem.at[5])
        send.start()
    for i in range(NG):
        out_copy(kbuf, ko_hbm, 0, i).wait()
        out_copy(vbuf, vo_hbm, 1, i).wait()
    if layer == 0:
        send.wait()


def attn_call(layer, pos, operands, k_cache, v_cache, prev):
    vm = pl.BlockSpec(memory_space=pltpu.VMEM)
    hbm = pl.BlockSpec(memory_space=pltpu.HBM)
    args = [pos, *operands, k_cache, v_cache]
    if layer == 0:
        specs = [hbm] * 8
        alias = {}
        extra = [
            pltpu.VMEM((KCH, KCS, QW), bf16),
            pltpu.VMEM((KCH, NB, KCS), bf16),
            pltpu.VMEM((NB, QW), f32),
            pltpu.SemaphoreType.DMA((KCH,)),
            pltpu.SMEM(pos.shape, jnp.int32),
            *[pltpu.VMEM(arr.shape, bf16) for arr in operands[:4]],
            pltpu.VMEM((KVL, MSG, HD), f32),
            pltpu.SemaphoreType.DMA((6,)),
        ]
        limit = 60 * 1024 * 1024
    else:
        args += list(prev)
        specs = [pl.BlockSpec(memory_space=pltpu.SMEM), vm] + [hbm] * 4
        alias = {4: 1, 5: 2}
        extra = []
        limit = VMEM_BYTES
    cache = jax.ShapeDtypeStruct(k_cache.shape, bf16)
    return pl.pallas_call(
        functools.partial(attn_kernel, layer),
        out_shape=(jax.ShapeDtypeStruct((MSG_ROOM if layer == 0 else KVL, MSG, HD), f32), cache, cache),
        in_specs=specs,
        out_specs=(hbm if layer == 0 else vm, hbm, hbm),
        scratch_shapes=[
            pltpu.VMEM((NB, SLOTS * KVL, HD), bf16),
            pltpu.VMEM((NB, SLOTS * KVL, HD), bf16),
            pltpu.VMEM((NB * QROWS, HD), f32),
            pltpu.VMEM((NB * 8, HD), f32),
            pltpu.VMEM((NB * 8, HD), f32),
            pltpu.VMEM((NB * QROWS, HD), f32),
            pltpu.VMEM((NB * QROWS, HD), f32),
            pltpu.VMEM((NB * QROWS, HD), f32),
            pltpu.SemaphoreType.DMA((NG,)),
            pltpu.SemaphoreType.DMA((NG,)),
            pltpu.SemaphoreType.DMA((2, NG)),
            *extra,
        ],
        input_output_aliases=alias,
        compiler_params=pltpu.CompilerParams(vmem_limit_bytes=limit),
        name=f'attn{layer}',
    )(*args)


def rest_kernel(layer, msg, x, gain, shift, b_dense, b_up, b_down, wd_hbm, wu_hbm, wn_hbm, *rest):
    if layer == 0:
        b_qkv, wq_hbm, x_out, out, *rest = rest
        msg_hbm, (*rest, msg) = msg, rest
    else:
        out, *rest = rest
    (wd, wu, wn, got, sent, o_buf, part, pair, sums, other, ag, full, xrow, up, mbuf,
     wsem, a_sem, d_sem, y_sem, g_sem, x_sem) = rest
    dp = lax.axis_index('dp')
    tp = lax.axis_index('tp')
    sp = lax.axis_index('sp')
    core = sp % 2
    cx = sp // 2
    ox = 1 - cx
    mate = (dp, tp, cx * 2 + 1 - core)
    x_dev = (dp, tp, ox * 2 + core)
    y_dev = (dp, 1 - tp, sp)

    def load(src, dst, i):
        return pltpu.make_async_copy(src, dst, wsem.at[i])

    wd_copy = load(wd_hbm.at[layer, pl.ds(pl.multiple_of(core * DR, DR), DR), :], wd, 0)

    def wu_copy(i):
        return load(wu_hbm.at[layer, pl.ds(i * CW, CW), pl.ds(pl.multiple_of(core * F_LOC, F_LOC), F_LOC)], wu.at[i], 1 + i)

    wn_copy = load(wn_hbm.at[layer, pl.ds(pl.multiple_of(core * M_LOC, M_LOC), M_LOC), :], wn, 1 + NCH)

    def wq_copy(i):
        return load(wq_hbm.at[1, pl.ds(i * CW, CW), :], wu.at[i, :, pl.ds(0, QW)], 2 + NCH + i)

    barrier = pltpu.get_barrier_semaphore()
    for peer in (mate, x_dev, y_dev):
        pl.semaphore_signal(barrier, inc=1, device_id=peer, device_id_type=MESH)
    if layer == 0:
        msg_copy = load(msg_hbm.at[pl.ds(0, KVL)], msg, 2 + 2 * NCH)
        msg_copy.start()
    wd_copy.start()
    for i in range(NCH):
        wu_copy(i).start()
    wn_copy.start()
    pl.semaphore_wait(barrier, 3)
    if layer == 0:
        msg_copy.wait()

    def remote(src, dst, sems, idx, peer):
        return pltpu.make_async_remote_copy(
            src_ref=src, dst_ref=dst, send_sem=sems.at[(0,) + idx], recv_sem=sems.at[(1,) + idx],
            device_id=peer, device_id_type=MESH)

    near = cx * 2 + core
    far = ox * 2 + core
    swap = [remote(msg.at[ox * 2 + 1 - core], got.at[0], a_sem, (0,), mate),
            remote(msg.at[cx * 2 + 1 - core], got.at[1], a_sem, (1,), mate)]
    for copy in swap:
        copy.start()

    gain1 = gain[layer, 1:2, :].astype(f32)
    shift1 = shift[layer, 1:2, :].astype(f32)
    own = pl.ds(pl.multiple_of(core * ROWS, ROWS), ROWS)
    theirs = pl.ds(pl.multiple_of((1 - core) * ROWS, ROWS), ROWS)

    def all_rows(x_, c_):
        return pl.ds(pl.multiple_of(x_ * HALF + c_ * ROWS, ROWS), ROWS)

    xrow[...] = x[all_rows(cx, core), :].astype(f32) if layer == 0 else x[...]
    lane = lax.broadcasted_iota(jnp.int32, (8, HD), 1)

    def merge(one, two, put, stat_out=None):
        stats = [ref[pl.ds(HPC * HALF, 8), :] for ref in (one, two)]
        new_stat = jnp.zeros((8, HD), f32)
        for g in range(HPC):
            for i in range(HALF // 8):
                at = 2 * (g * (HALF // 8) + i)
                peaks = [jnp.broadcast_to(st[:, at:at + 1], (8, HD)) for st in stats]
                tots = [jnp.broadcast_to(st[:, at + 1:at + 2], (8, HD)) for st in stats]
                top = jnp.maximum(peaks[0], peaks[1])
                scale = [jnp.exp(p - top) for p in peaks]
                rows = pl.ds(g * HALF + i * 8, 8)
                num = one[rows, :] * scale[0] + two[rows, :] * scale[1]
                den = tots[0] * scale[0] + tots[1] * scale[1]
                put(g, i, num, den)
                if stat_out is not None:
                    new_stat = jnp.where(lane == at, top, new_stat)
                    new_stat = jnp.where(lane == at + 1, den, new_stat)
        if stat_out is not None:
            stat_out[pl.ds(HPC * HALF, 8), :] = new_stat

    def put_part(ref):
        def put(g, i, num, den):
            ref[pl.ds(g * HALF + i * 8, 8), :] = num
        return put

    def put_out(g, i, num, den):
        o_buf[pl.ds(i * 8, 8), g * HD:(g + 1) * HD] = num / den

    swap[0].wait_recv()
    merge(msg.at[far], got.at[0], put_part(sent.at[0]), sent.at[0])
    cross = remote(sent.at[0], got.at[2], a_sem, (2,), x_dev)
    cross.start()
    swap[1].wait_recv()
    merge(msg.at[near], got.at[1], put_part(sent.at[1]), sent.at[1])
    cross.wait_recv()
    merge(sent.at[1], got.at[2], put_out)
    sends = swap + [cross]

    def reduce(ph, product, finish):
        first = [remote(part.at[ph, n, theirs, :], pair.at[ph, n], d_sem, (ph, n), mate) for n in range(RCH)]
        second = [remote(sums.at[ph, n], other.at[ph, n], y_sem, (ph, n), y_dev) for n in range(RCH)]
        for step in range(RCH + LAG):
            if step < RCH:
                part[ph, step] = product(step)
                first[step].start()
            if step >= LAG:
                n = step - LAG
                first[n].wait_recv()
                sums[ph, n] = part[ph, n, own, :] + pair[ph, n]
                second[n].start()
        for n in range(RCH):
            second[n].wait_recv()
            finish(n, sums[ph, n] + other[ph, n])
        return first + second

    def residual(n, total, bias):
        cols = slice(n * RW, (n + 1) * RW)
        v = xrow[:, cols] + total + bias[layer:layer + 1, cols].astype(f32)
        xrow[:, cols] = v.astype(bf16).astype(f32)

    wd_copy.wait()
    o = o_buf[...].astype(bf16)
    sends += reduce(0, lambda n: jnp.dot(o, wd[:, n * RW:(n + 1) * RW], preferred_element_type=f32),
                   lambda n, total: residual(n, total, b_dense))

    normed = norm_rows(xrow[...], gain1, shift1).astype(bf16).astype(f32)
    swap = []
    for n in range(NCH):
        ag[n, own, :] = normed[:, n * CW:(n + 1) * CW]
        here = ag.at[n, own, :]
        swap.append(remote(here, here, g_sem, (n,), mate))
        swap[n].start()
    cols_up = pl.ds(pl.multiple_of(core * F_LOC, F_LOC), F_LOC)
    up[...] = jnp.broadcast_to(b_up[layer:layer + 1, cols_up].astype(f32), (HALF, F_LOC))
    for n in range(NCH):
        wu_copy(n).wait()
        swap[n].wait_recv()
        up[...] += jnp.dot(ag[n].astype(bf16), wu[n], preferred_element_type=f32)
        if layer == 0:
            wq_copy(n).start()

    pick = (lax.broadcasted_iota(jnp.int32, (256, 128), 0) == 2 * lax.broadcasted_iota(jnp.int32, (256, 128), 1))
    pick = jnp.where(pick, 1.0, 0.0).astype(bf16)
    for k in range(F_LOC // 256):
        a = up[:, k * 256:(k + 1) * 256]
        z = jnp.minimum(a, GELU_LIMIT)
        gate = z * jax.nn.sigmoid(1.702 * z)
        lin = jnp.clip(a, -GELU_LIMIT, GELU_LIMIT) + 1.0
        prod = (gate * pltpu.roll(lin, 255, 1)).astype(bf16)
        mbuf[:, k * 128:(k + 1) * 128] = jnp.dot(prod, pick, preferred_element_type=f32).astype(bf16)
    wn_copy.wait()
    m = mbuf[...]
    sends += swap

    def spread(n, value):
        full[n, all_rows(cx, core), :] = value
        here = full.at[n, all_rows(cx, core), :]
        for k, peer in enumerate((x_dev, mate)):
            copy = remote(here, here, x_sem, (k, n), peer)
            copy.start()
            sends.append(copy)

    def collect(chunks, use):
        for n in range(chunks):
            there = full.at[n, all_rows(ox, core), :]
            remote(there, there, x_sem, (0, n), x_dev).wait_recv()
            copy = remote(there, there, x_sem, (2, n), mate)
            copy.start()
            sends.append(copy)
        for n in range(chunks):
            for k, x_ in ((1, cx), (2, ox)):
                there = full.at[n, all_rows(x_, 1 - core), :]
                remote(there, there, x_sem, (k, n), mate).wait_recv()
            use(n)

    def take_down(n, total):
        residual(n, total, b_down)
        if layer == 1:
            spread(n, xrow[:, n * RW:(n + 1) * RW])

    sends += reduce(1, lambda n: jnp.dot(m, wn[:, n * RW:(n + 1) * RW], preferred_element_type=f32), take_down)
    if layer == 0:
        x_out[...] = xrow[...]
        u = norm_rows(xrow[...], gain[1, 0:1, :].astype(f32), shift[1, 0:1, :].astype(f32)).astype(bf16)
        for i in range(NCH):
            wq_copy(i).wait()
        for n in range(QCH):
            cols = slice(n * QC, (n + 1) * QC)
            r = jnp.broadcast_to(b_qkv[1:2, cols].astype(f32), (ROWS, QC))
            for i in range(NCH):
                r += jnp.dot(u[:, i * CW:(i + 1) * CW], wu[i, :, cols], preferred_element_type=f32)
            spread(n, r)

        def use(n):
            out[n] = full[n]
    else:
        def use(n):
            out[:, n * RW:(n + 1) * RW] = full[n].astype(bf16)

    collect(QCH if layer == 0 else RCH, use)
    for copy in sends:
        copy.wait_send()


def rest_call(layer, msg, x, gain, shift, b_dense, b_up, b_down, w_dense, w_up, w_down, *qkv):
    vm = pl.BlockSpec(memory_space=pltpu.VMEM)
    hbm = pl.BlockSpec(memory_space=pltpu.HBM)
    if layer == 0:
        in_specs = [hbm] + [vm] * 6 + [hbm] * 3 + [vm, hbm]
        out_shape = (jax.ShapeDtypeStruct((ROWS, D), f32), jax.ShapeDtypeStruct((QCH, NB, QC), f32))
        out_specs = (vm, vm)
    else:
        in_specs = [vm] * 7 + [hbm] * 3
        out_shape = jax.ShapeDtypeStruct((NB, D), bf16)
        out_specs = vm
    return pl.pallas_call(
        functools.partial(rest_kernel, layer),
        out_shape=out_shape,
        in_specs=in_specs,
        out_specs=out_specs,
        scratch_shapes=[
            pltpu.VMEM((DR, D), bf16),
            pltpu.VMEM((NCH, CW, F_LOC), bf16),
            pltpu.VMEM((M_LOC, D), bf16),
            pltpu.VMEM((3, MSG, HD), f32),
            pltpu.VMEM((2, MSG, HD), f32),
            pltpu.VMEM((HALF, DR), f32),
            pltpu.VMEM((2, RCH, HALF, RW), f32),
            pltpu.VMEM((2, RCH, ROWS, RW), f32),
            pltpu.VMEM((2, RCH, ROWS, RW), f32),
            pltpu.VMEM((2, RCH, ROWS, RW), f32),
            pltpu.VMEM((NCH, HALF, CW), f32),
            pltpu.VMEM((QCH, NB, QC) if layer == 0 else (RCH, NB, RW), f32),
            pltpu.VMEM((ROWS, D), f32),
            pltpu.VMEM((HALF, F_LOC), f32),
            pltpu.VMEM((HALF, M_LOC), bf16),
            pltpu.SemaphoreType.DMA((3 + 2 * NCH,)),
            pltpu.SemaphoreType.DMA((2, 3)),
            pltpu.SemaphoreType.DMA((2, 2, RCH)),
            pltpu.SemaphoreType.DMA((2, 2, RCH)),
            pltpu.SemaphoreType.DMA((2, NCH)),
            pltpu.SemaphoreType.DMA((2, 3, RCH)),
            *([pltpu.VMEM((KVL, MSG, HD), f32)] if layer == 0 else []),
        ],
        compiler_params=pltpu.CompilerParams(vmem_limit_bytes=VMEM_BYTES, collective_id=layer, has_side_effects=True),
        name=f'rest{layer}',
    )(msg, x, gain, shift, b_dense, b_up, b_down, w_dense, w_up, w_down, *qkv)


def solution(mesh):
    cache_spec = P(None, 'dp', 'sp', 'tp', None)
    in_specs = (P('dp', None), P('dp'), cache_spec, cache_spec, P(), P(), P(None, None, 'tp'), P(None, 'tp'), P(None, 'tp', None), P(), P(None, None, 'tp'), P(None, 'tp'), P(None, 'tp', None), P())
    out_specs = (P('dp', None), cache_spec, cache_spec)

    def device_step(hidden, positions, k_cache, v_cache, ln_gain, ln_bias, w_qkv, b_qkv, w_dense, b_dense, w_up, b_up, w_down, b_down):
        shape = k_cache.shape
        flat = (2, NB, SLOTS * KVL, HD)
        k_cache = k_cache.reshape(flat)
        v_cache = v_cache.reshape(flat)
        shared = (ln_gain, ln_bias, b_dense, b_up, b_down, w_dense, w_up, w_down)
        msg, *caches = attn_call(0, positions, (hidden, ln_gain, ln_bias, b_qkv, w_qkv), k_cache, v_cache, None)
        rows, qkv = rest_call(0, msg, hidden, *shared, b_qkv, w_qkv)
        msg, *caches = attn_call(1, positions, (qkv,), k_cache, v_cache, caches)
        hidden = rest_call(1, msg, rows, *shared)
        return hidden, caches[0].reshape(shape), caches[1].reshape(shape)

    return jax.shard_map(device_step, mesh=mesh, in_specs=in_specs, out_specs=out_specs, check_vma=False)
```

```python
import functools
import math

import jax
import jax.numpy as jnp
from jax import lax
from jax.experimental import pallas as pl
from jax.experimental.pallas import tpu as pltpu
from jax.sharding import PartitionSpec as P

BLOCK_SIZE = 64
LOCAL_BLOCKS = 16
VERT_STRIDE = 8
ROPE_THETA = 1000000.0
GELU_LIMIT = 20.0
NORM_EPS = 0.00001
MASKED = -1e30
MESH = pl.DeviceIdType.MESH

NB = 64
D = 3072
HD = 128
KVL = 4
GRP = 3
SLOTS = 64
QW = KVL * (GRP + 2) * HD
QROWS = 16
KCH = 6
KCS = D // KCH
G = 8
NG = NB // G
GS = 16
HALF = NB // 2
HPC = 6
PART = HPC // 2 * HALF + 8
MSG = 2 * PART
MSG_ROOM = 160
ROWS = HALF // 2
F_LOC = 4096
M_LOC = F_LOC // 2
NCH = 3
CW = D // NCH
QCH = 5
QC = QW // QCH
DR = HPC * HD
RCH = 6
RW = D // RCH
LAG = 2
VMEM_BYTES = 52 * 1024 * 1024

f32 = jnp.float32
bf16 = jnp.bfloat16


def norm_rows(rows, gain, shift):
    mean = jnp.mean(rows, axis=-1, keepdims=True)
    cent = rows - mean
    var = jnp.mean(jnp.square(cent), axis=-1, keepdims=True)
    return (cent * lax.rsqrt(var + NORM_EPS)) * gain + shift


def rope_tables(pos):
    half = HD // 2
    row = lax.broadcasted_iota(jnp.int32, (8, HD), 0)
    lane = lax.broadcasted_iota(jnp.int32, (NB, HD), 1)
    groups = []
    for i in range(NB // 8):
        at = jnp.zeros((8, HD), jnp.int32)
        for r in range(8):
            at = jnp.where(row == r, pos[i * 8 + r], at)
        groups.append(at)
    where = jnp.concatenate(groups, axis=0).astype(f32)
    power = (lane % half).astype(f32) * (2.0 / HD)
    angles = where * jnp.exp(power * -math.log(ROPE_THETA))
    sin = jnp.sin(angles)
    return jnp.cos(angles), jnp.where(lane < half, -sin, sin)


def attn_kernel(layer, pos, *rest):
    if layer == 0:
        x, gain, shift, b_qkv, w_hbm, kc_hbm, vc_hbm, *rest = rest
    else:
        acc, kc_hbm, vc_hbm, _, _, *rest = rest
    msg, ko_hbm, vo_hbm, kbuf, vbuf, qs, kns, vns, os, ms, ls, ksem, vsem, osem, *rest = rest
    sp = lax.axis_index('sp')
    tp = lax.axis_index('tp')
    base = sp * SLOTS

    def in_copy(hbm, buf, sem, i):
        return pltpu.make_async_copy(hbm.at[layer, pl.ds(i * G, G)], buf.at[pl.ds(i * G, G)], sem.at[i])

    def out_copy(buf, hbm, j, i):
        return pltpu.make_async_copy(buf.at[pl.ds(i * G, G)], hbm.at[layer, pl.ds(i * G, G)], osem.at[j, i])

    def fetch_cache():
        for i in range(NG):
            in_copy(kc_hbm, kbuf, ksem, i).start(priority=0)
            in_copy(vc_hbm, vbuf, vsem, i).start(priority=1)

    if layer == 0:
        w, u, acc, wsem, *places, msg_buf, small_sem = rest
        msg_hbm, msg = msg, msg_buf
        small = [pltpu.make_async_copy(src, dst, small_sem.at[i]) for i, (src, dst) in enumerate(zip((pos, x, gain, shift, b_qkv), places))]
        for copy in small:
            copy.start()
        pos, x, gain, shift, b_qkv = places

        def w_copy(i):
            return pltpu.make_async_copy(w_hbm.at[layer, pl.ds(i * KCS, KCS), :], w.at[i], wsem.at[i])

        for i in range(KCH):
            w_copy(i).start(priority=i % 2)
        fetch_cache()
        for copy in small:
            copy.wait()
        g_row = gain[layer, 0:1, :].astype(f32)
        s_row = shift[layer, 0:1, :].astype(f32)
        for i in range(NB // 16):
            rows = x[pl.ds(i * 16, 16), :].astype(f32)
            normed = norm_rows(rows, g_row, s_row).astype(bf16)
            for j in range(KCH):
                u[j, pl.ds(i * 16, 16), :] = normed[:, j * KCS:(j + 1) * KCS]
        acc[...] = jnp.broadcast_to(b_qkv[layer:layer + 1, :].astype(f32), (NB, QW))
    else:
        fetch_cache()
    qs[...] = jnp.zeros_like(qs)
    cos_t, sin_t = rope_tables(pos)
    if layer == 0:
        def qkv_step(i, carry):
            w_copy(i).wait()
            acc[...] += jnp.dot(u[i], w[i], preferred_element_type=f32)
            return carry

        lax.fori_loop(0, KCH, qkv_step, 0)

    for c in range(KVL):
        for j in range(GRP + 2):
            if layer == 0:
                col = (c * (GRP + 2) + j) * HD
                tile = acc[:, col:col + HD]
            else:
                head = c * (GRP + 2) + j
                tile = acc[head // (QC // HD), :, head % (QC // HD) * HD:(head % (QC // HD) + 1) * HD]
            if j <= GRP:
                tile = tile * cos_t + pltpu.roll(tile, HD // 2, 1) * sin_t
            for i in range(NB // 8):
                part = tile[i * 8:(i + 1) * 8]
                if j < GRP:
                    qs[pl.ds(i * 8 * QROWS + c * GRP + j, 8, stride=QROWS), :] = part
                else:
                    dst = kns if j == GRP else vns
                    dst[pl.ds(i * 64 + c, 8, stride=8), :] = part
                    dst[pl.ds(i * 64 + c + 4, 8, stride=8), :] = part

    row_h = lax.broadcasted_iota(jnp.int32, (QROWS, SLOTS * KVL), 0)
    col_i = lax.broadcasted_iota(jnp.int32, (QROWS, SLOTS * KVL), 1)
    slot_of = jnp.where(row_h // GRP == col_i % KVL, col_i // KVL, 1 << 20)
    head_id = tp * KVL * GRP + row_h
    vertical = (sp + head_id + 1) % VERT_STRIDE == 0
    sub_row = lax.broadcasted_iota(jnp.int32, (16, HD), 0) // KVL

    def patch(buf, new, b):
        at = pos[b] - base
        atc = jnp.clip(at, 0, SLOTS - 1)
        hit = jnp.logical_and(at >= 0, at < SLOTS)
        put = sub_row == jnp.where(hit, atc % KVL, -1)
        r0 = pl.multiple_of((atc // KVL) * 16, 16)
        new8 = new[b * 8:b * 8 + 8, :]
        new16 = jnp.concatenate([new8, new8], axis=0)
        old = buf[b, pl.ds(r0, 16), :].astype(f32)
        buf[b, pl.ds(r0, 16), :] = jnp.where(put, new16, old).astype(bf16)

    def score(step):
        seqs = range(step * GS, (step + 1) * GS)
        for b in seqs:
            patch(kbuf, kns, b)
        return [lax.dot_general(qs[b * QROWS:(b + 1) * QROWS, :].astype(bf16), kbuf[b], (((1,), (1,)), ((), ())),
                                preferred_element_type=f32) for b in seqs]

    def keep_of(b):
        at = pos[b] - base
        if layer == 0:
            near = pos[b] // BLOCK_SIZE - sp < LOCAL_BLOCKS
            return slot_of <= jnp.where(vertical, at, jnp.where(near, at, -1))
        return slot_of <= at

    def mix(step, scores):
        seqs = range(step * GS, (step + 1) * GS)
        for b in seqs:
            patch(vbuf, vns, b)
        keeps = [keep_of(b) for b in seqs]
        scores = [jnp.where(keep, s * (1.0 / HD), MASKED) for keep, s in zip(keeps, scores)]
        peaks = [jnp.max(s, axis=1, keepdims=True) for s in scores]
        weights = [jnp.where(keep, jnp.exp(s - peak), 0.0) for keep, s, peak in zip(keeps, scores, peaks)]
        outs = [jnp.dot(wt.astype(bf16), vbuf[b], preferred_element_type=f32) for b, wt in zip(seqs, weights)]
        sums = [jnp.sum(wt, axis=1, keepdims=True) for wt in weights]
        for j, b in enumerate(seqs):
            rows = slice(b * QROWS, (b + 1) * QROWS)
            ms[rows, :] = jnp.broadcast_to(peaks[j], (QROWS, HD))
            ls[rows, :] = jnp.broadcast_to(sums[j], (QROWS, HD))
            os[rows, :] = outs[j]

    per = GS // G
    steps = NB // GS
    for j in range(per):
        in_copy(kc_hbm, kbuf, ksem, j).wait()
    scores = score(0)
    for step in range(steps):
        for j in range(step * per, (step + 1) * per):
            in_copy(vc_hbm, vbuf, vsem, j).wait()
            if step + 1 < steps:
                in_copy(kc_hbm, kbuf, ksem, j + per).wait()
        later = score(step + 1) if step + 1 < steps else None
        mix(step, scores)
        scores = later
        for j in range(step * per, (step + 1) * per):
            if step == 0:
                out_copy(kbuf, ko_hbm, 0, j).start()
            if step + 1 < steps:
                out_copy(kbuf, ko_hbm, 0, j + per).start()
            out_copy(vbuf, vo_hbm, 1, j).start(priority=1)

    lane = lax.broadcasted_iota(jnp.int32, (8, HD), 1)
    for half in range(2):
        for c in range(2):
            for part in range(2):
                stat = jnp.zeros((8, HD), f32)
                for g in range(HPC // 2):
                    for i in range(HALF // 8):
                        head = c * HPC + part * (HPC // 2) + g
                        rows = pl.ds((half * HALF + i * 8) * QROWS + head, 8, stride=QROWS)
                        at = 2 * (g * (HALF // 8) + i)
                        msg[half * 2 + c, pl.ds(part * PART + g * HALF + i * 8, 8), :] = os[rows, :]
                        stat = jnp.where(lane == at, ms[rows, :], stat)
                        stat = jnp.where(lane == at + 1, ls[rows, :], stat)
                msg[half * 2 + c, pl.ds(part * PART + PART - 8, 8), :] = stat
    if layer == 0:
        send = pltpu.make_async_copy(msg, msg_hbm.at[pl.ds(0, KVL)], small_sem.at[5])
        send.start()
    for i in range(NG):
        out_copy(kbuf, ko_hbm, 0, i).wait()
        out_copy(vbuf, vo_hbm, 1, i).wait()
    if layer == 0:
        send.wait()


def attn_call(layer, pos, operands, k_cache, v_cache, prev):
    vm = pl.BlockSpec(memory_space=pltpu.VMEM)
    hbm = pl.BlockSpec(memory_space=pltpu.HBM)
    args = [pos, *operands, k_cache, v_cache]
    if layer == 0:
        specs = [hbm] * 8
        alias = {}
        extra = [
            pltpu.VMEM((KCH, KCS, QW), bf16),
            pltpu.VMEM((KCH, NB, KCS), bf16),
            pltpu.VMEM((NB, QW), f32),
            pltpu.SemaphoreType.DMA((KCH,)),
            pltpu.SMEM(pos.shape, jnp.int32),
            *[pltpu.VMEM(arr.shape, bf16) for arr in operands[:4]],
            pltpu.VMEM((KVL, MSG, HD), f32),
            pltpu.SemaphoreType.DMA((6,)),
        ]
        limit = 60 * 1024 * 1024
    else:
        args += list(prev)
        specs = [pl.BlockSpec(memory_space=pltpu.SMEM), vm] + [hbm] * 4
        alias = {4: 1, 5: 2}
        extra = []
        limit = VMEM_BYTES
    cache = jax.ShapeDtypeStruct(k_cache.shape, bf16)
    return pl.pallas_call(
        functools.partial(attn_kernel, layer),
        out_shape=(jax.ShapeDtypeStruct((MSG_ROOM if layer == 0 else KVL, MSG, HD), f32), cache, cache),
        in_specs=specs,
        out_specs=(hbm if layer == 0 else vm, hbm, hbm),
        scratch_shapes=[
            pltpu.VMEM((NB, SLOTS * KVL, HD), bf16),
            pltpu.VMEM((NB, SLOTS * KVL, HD), bf16),
            pltpu.VMEM((NB * QROWS, HD), f32),
            pltpu.VMEM((NB * 8, HD), f32),
            pltpu.VMEM((NB * 8, HD), f32),
            pltpu.VMEM((NB * QROWS, HD), f32),
            pltpu.VMEM((NB * QROWS, HD), f32),
            pltpu.VMEM((NB * QROWS, HD), f32),
            pltpu.SemaphoreType.DMA((NG,)),
            pltpu.SemaphoreType.DMA((NG,)),
            pltpu.SemaphoreType.DMA((2, NG)),
            *extra,
        ],
        input_output_aliases=alias,
        compiler_params=pltpu.CompilerParams(vmem_limit_bytes=limit),
        name=f'attn{layer}',
    )(*args)


def rest_kernel(layer, msg, x, gain, shift, b_dense, b_up, b_down, wd_hbm, wu_hbm, wn_hbm, *rest):
    if layer == 0:
        b_qkv, wq_hbm, x_out, out, *rest = rest
        msg_hbm, (*rest, msg) = msg, rest
    else:
        out, *rest = rest
    (wd, wu, wn, got, sent, o_buf, part, pair, sums, other, ag, full, xrow, up, mbuf,
     wsem, a_sem, d_sem, y_sem, g_sem, x_sem) = rest
    dp = lax.axis_index('dp')
    tp = lax.axis_index('tp')
    sp = lax.axis_index('sp')
    core = sp % 2
    cx = sp // 2
    ox = 1 - cx
    mate = (dp, tp, cx * 2 + 1 - core)
    x_dev = (dp, tp, ox * 2 + core)
    y_dev = (dp, 1 - tp, sp)

    def load(src, dst, i):
        return pltpu.make_async_copy(src, dst, wsem.at[i])

    wd_copy = load(wd_hbm.at[layer, pl.ds(pl.multiple_of(core * DR, DR), DR), :], wd, 0)

    def wu_copy(i):
        return load(wu_hbm.at[layer, pl.ds(i * CW, CW), pl.ds(pl.multiple_of(core * F_LOC, F_LOC), F_LOC)], wu.at[i], 1 + i)

    wn_copy = load(wn_hbm.at[layer, pl.ds(pl.multiple_of(core * M_LOC, M_LOC), M_LOC), :], wn, 1 + NCH)

    def wq_copy(i):
        return load(wq_hbm.at[1, pl.ds(i * CW, CW), :], wu.at[i, :, pl.ds(0, QW)], 2 + NCH + i)

    barrier = pltpu.get_barrier_semaphore()
    for peer in (mate, x_dev, y_dev):
        pl.semaphore_signal(barrier, inc=1, device_id=peer, device_id_type=MESH)
    if layer == 0:
        msg_copy = load(msg_hbm.at[pl.ds(0, KVL)], msg, 2 + 2 * NCH)
        msg_copy.start()
    wd_copy.start()
    for i in range(NCH):
        wu_copy(i).start()
    wn_copy.start()
    pl.semaphore_wait(barrier, 3)
    if layer == 0:
        msg_copy.wait()

    def remote(src, dst, sems, idx, peer):
        return pltpu.make_async_remote_copy(
            src_ref=src, dst_ref=dst, send_sem=sems.at[(0,) + idx], recv_sem=sems.at[(1,) + idx],
            device_id=peer, device_id_type=MESH)

    near = cx * 2 + core
    far = ox * 2 + core
    parts = [pl.ds(k * PART, PART) for k in range(2)]
    swap = [[remote(msg.at[home, parts[k], :], got.at[j, parts[k], :], a_sem, (2 * j + k,), mate) for k in range(2)]
            for j, home in enumerate((ox * 2 + 1 - core, cx * 2 + 1 - core))]
    cross = [remote(sent.at[0, parts[k], :], got.at[2, parts[k], :], a_sem, (4 + k,), x_dev) for k in range(2)]
    for copy in swap[0] + swap[1]:
        copy.start()

    gain1 = gain[layer, 1:2, :].astype(f32)
    shift1 = shift[layer, 1:2, :].astype(f32)
    own = pl.ds(pl.multiple_of(core * ROWS, ROWS), ROWS)
    theirs = pl.ds(pl.multiple_of((1 - core) * ROWS, ROWS), ROWS)

    def all_rows(x_, c_):
        return pl.ds(pl.multiple_of(x_ * HALF + c_ * ROWS, ROWS), ROWS)

    xrow[...] = x[all_rows(cx, core), :].astype(f32) if layer == 0 else x[...]
    lane = lax.broadcasted_iota(jnp.int32, (8, HD), 1)

    def merge(one, two, k, put, stat_out=None):
        stats = [ref[pl.ds(k * PART + PART - 8, 8), :] for ref in (one, two)]
        new_stat = jnp.zeros((8, HD), f32)
        for g in range(HPC // 2):
            for i in range(HALF // 8):
                at = 2 * (g * (HALF // 8) + i)
                peaks = [jnp.broadcast_to(st[:, at:at + 1], (8, HD)) for st in stats]
                tots = [jnp.broadcast_to(st[:, at + 1:at + 2], (8, HD)) for st in stats]
                top = jnp.maximum(peaks[0], peaks[1])
                scale = [jnp.exp(p - top) for p in peaks]
                rows = pl.ds(k * PART + g * HALF + i * 8, 8)
                num = one[rows, :] * scale[0] + two[rows, :] * scale[1]
                den = tots[0] * scale[0] + tots[1] * scale[1]
                put(k, g, i, num, den)
                if stat_out is not None:
                    new_stat = jnp.where(lane == at, top, new_stat)
                    new_stat = jnp.where(lane == at + 1, den, new_stat)
        if stat_out is not None:
            stat_out[pl.ds(k * PART + PART - 8, 8), :] = new_stat

    def put_part(ref):
        def put(k, g, i, num, den):
            ref[pl.ds(k * PART + g * HALF + i * 8, 8), :] = num
        return put

    def put_out(k, g, i, num, den):
        head = k * (HPC // 2) + g
        o_buf[pl.ds(i * 8, 8), head * HD:(head + 1) * HD] = num / den

    for k in range(2):
        swap[0][k].wait_recv()
        merge(msg.at[far], got.at[0], k, put_part(sent.at[0]), sent.at[0])
        cross[k].start()
    for k in range(2):
        swap[1][k].wait_recv()
        merge(msg.at[near], got.at[1], k, put_part(sent.at[1]), sent.at[1])
    for k in range(2):
        cross[k].wait_recv()
        merge(sent.at[1], got.at[2], k, put_out)
    sends = swap[0] + swap[1] + cross

    def reduce(ph, product, finish):
        first = [remote(part.at[ph, n, theirs, :], pair.at[ph, n], d_sem, (ph, n), mate) for n in range(RCH)]
        second = [remote(sums.at[ph, n], other.at[ph, n], y_sem, (ph, n), y_dev) for n in range(RCH)]
        for step in range(RCH + LAG):
            if step < RCH:
                part[ph, step] = product(step)
                first[step].start()
            if step >= LAG:
                n = step - LAG
                first[n].wait_recv()
                sums[ph, n] = part[ph, n, own, :] + pair[ph, n]
                second[n].start()
        for n in range(RCH):
            second[n].wait_recv()
            finish(n, sums[ph, n] + other[ph, n])
        return first + second

    def residual(n, total, bias):
        cols = slice(n * RW, (n + 1) * RW)
        v = xrow[:, cols] + total + bias[layer:layer + 1, cols].astype(f32)
        xrow[:, cols] = v.astype(bf16).astype(f32)

    wd_copy.wait()
    o = o_buf[...].astype(bf16)
    sends += reduce(0, lambda n: jnp.dot(o, wd[:, n * RW:(n + 1) * RW], preferred_element_type=f32),
                   lambda n, total: residual(n, total, b_dense))

    normed = norm_rows(xrow[...], gain1, shift1).astype(bf16).astype(f32)
    swap = []
    for n in range(NCH):
        ag[n, own, :] = normed[:, n * CW:(n + 1) * CW]
        here = ag.at[n, own, :]
        swap.append(remote(here, here, g_sem, (n,), mate))
        swap[n].start()
    cols_up = pl.ds(pl.multiple_of(core * F_LOC, F_LOC), F_LOC)
    up[...] = jnp.broadcast_to(b_up[layer:layer + 1, cols_up].astype(f32), (HALF, F_LOC))
    for n in range(NCH):
        wu_copy(n).wait()
        swap[n].wait_recv()
        up[...] += jnp.dot(ag[n].astype(bf16), wu[n], preferred_element_type=f32)
        if layer == 0:
            wq_copy(n).start()

    pick = (lax.broadcasted_iota(jnp.int32, (256, 128), 0) == 2 * lax.broadcasted_iota(jnp.int32, (256, 128), 1))
    pick = jnp.where(pick, 1.0, 0.0).astype(bf16)
    for k in range(F_LOC // 256):
        a = up[:, k * 256:(k + 1) * 256]
        z = jnp.minimum(a, GELU_LIMIT)
        gate = z * jax.nn.sigmoid(1.702 * z)
        lin = jnp.clip(a, -GELU_LIMIT, GELU_LIMIT) + 1.0
        prod = (gate * pltpu.roll(lin, 255, 1)).astype(bf16)
        mbuf[:, k * 128:(k + 1) * 128] = jnp.dot(prod, pick, preferred_element_type=f32).astype(bf16)
    wn_copy.wait()
    m = mbuf[...]
    sends += swap

    def spread(n, value):
        full[n, all_rows(cx, core), :] = value
        here = full.at[n, all_rows(cx, core), :]
        for k, peer in enumerate((x_dev, mate)):
            copy = remote(here, here, x_sem, (k, n), peer)
            copy.start()
            sends.append(copy)

    def collect(chunks, use):
        for n in range(chunks):
            there = full.at[n, all_rows(ox, core), :]
            remote(there, there, x_sem, (0, n), x_dev).wait_recv()
            copy = remote(there, there, x_sem, (2, n), mate)
            copy.start()
            sends.append(copy)
        for n in range(chunks):
            for k, x_ in ((1, cx), (2, ox)):
                there = full.at[n, all_rows(x_, 1 - core), :]
                remote(there, there, x_sem, (k, n), mate).wait_recv()
            use(n)

    def take_down(n, total):
        residual(n, total, b_down)
        if layer == 1:
            spread(n, xrow[:, n * RW:(n + 1) * RW])

    sends += reduce(1, lambda n: jnp.dot(m, wn[:, n * RW:(n + 1) * RW], preferred_element_type=f32), take_down)
    if layer == 0:
        x_out[...] = xrow[...]
        u = norm_rows(xrow[...], gain[1, 0:1, :].astype(f32), shift[1, 0:1, :].astype(f32)).astype(bf16)
        for i in range(NCH):
            wq_copy(i).wait()
        for n in range(QCH):
            cols = slice(n * QC, (n + 1) * QC)
            r = jnp.broadcast_to(b_qkv[1:2, cols].astype(f32), (ROWS, QC))
            for i in range(NCH):
                r += jnp.dot(u[:, i * CW:(i + 1) * CW], wu[i, :, cols], preferred_element_type=f32)
            spread(n, r)

        def use(n):
            out[n] = full[n]
    else:
        def use(n):
            out[:, n * RW:(n + 1) * RW] = full[n].astype(bf16)

    collect(QCH if layer == 0 else RCH, use)
    for copy in sends:
        copy.wait_send()


def rest_call(layer, msg, x, gain, shift, b_dense, b_up, b_down, w_dense, w_up, w_down, *qkv):
    vm = pl.BlockSpec(memory_space=pltpu.VMEM)
    hbm = pl.BlockSpec(memory_space=pltpu.HBM)
    if layer == 0:
        in_specs = [hbm] + [vm] * 6 + [hbm] * 3 + [vm, hbm]
        out_shape = (jax.ShapeDtypeStruct((ROWS, D), f32), jax.ShapeDtypeStruct((QCH, NB, QC), f32))
        out_specs = (vm, vm)
    else:
        in_specs = [vm] * 7 + [hbm] * 3
        out_shape = jax.ShapeDtypeStruct((NB, D), bf16)
        out_specs = vm
    return pl.pallas_call(
        functools.partial(rest_kernel, layer),
        out_shape=out_shape,
        in_specs=in_specs,
        out_specs=out_specs,
        scratch_shapes=[
            pltpu.VMEM((DR, D), bf16),
            pltpu.VMEM((NCH, CW, F_LOC), bf16),
            pltpu.VMEM((M_LOC, D), bf16),
            pltpu.VMEM((3, MSG, HD), f32),
            pltpu.VMEM((2, MSG, HD), f32),
            pltpu.VMEM((HALF, DR), f32),
            pltpu.VMEM((2, RCH, HALF, RW), f32),
            pltpu.VMEM((2, RCH, ROWS, RW), f32),
            pltpu.VMEM((2, RCH, ROWS, RW), f32),
            pltpu.VMEM((2, RCH, ROWS, RW), f32),
            pltpu.VMEM((NCH, HALF, CW), f32),
            pltpu.VMEM((QCH, NB, QC) if layer == 0 else (RCH, NB, RW), f32),
            pltpu.VMEM((ROWS, D), f32),
            pltpu.VMEM((HALF, F_LOC), f32),
            pltpu.VMEM((HALF, M_LOC), bf16),
            pltpu.SemaphoreType.DMA((3 + 2 * NCH,)),
            pltpu.SemaphoreType.DMA((2, 6)),
            pltpu.SemaphoreType.DMA((2, 2, RCH)),
            pltpu.SemaphoreType.DMA((2, 2, RCH)),
            pltpu.SemaphoreType.DMA((2, NCH)),
            pltpu.SemaphoreType.DMA((2, 3, RCH)),
            *([pltpu.VMEM((KVL, MSG, HD), f32)] if layer == 0 else []),
        ],
        compiler_params=pltpu.CompilerParams(vmem_limit_bytes=VMEM_BYTES, collective_id=layer, has_side_effects=True),
        name=f'rest{layer}',
    )(msg, x, gain, shift, b_dense, b_up, b_down, w_dense, w_up, w_down, *qkv)


def solution(mesh):
    cache_spec = P(None, 'dp', 'sp', 'tp', None)
    in_specs = (P('dp', None), P('dp'), cache_spec, cache_spec, P(), P(), P(None, None, 'tp'), P(None, 'tp'), P(None, 'tp', None), P(), P(None, None, 'tp'), P(None, 'tp'), P(None, 'tp', None), P())
    out_specs = (P('dp', None), cache_spec, cache_spec)

    def device_step(hidden, positions, k_cache, v_cache, ln_gain, ln_bias, w_qkv, b_qkv, w_dense, b_dense, w_up, b_up, w_down, b_down):
        shape = k_cache.shape
        flat = (2, NB, SLOTS * KVL, HD)
        k_cache = k_cache.reshape(flat)
        v_cache = v_cache.reshape(flat)
        shared = (ln_gain, ln_bias, b_dense, b_up, b_down, w_dense, w_up, w_down)
        msg, *caches = attn_call(0, positions, (hidden, ln_gain, ln_bias, b_qkv, w_qkv), k_cache, v_cache, None)
        rows, qkv = rest_call(0, msg, hidden, *shared, b_qkv, w_qkv)
        msg, *caches = attn_call(1, positions, (qkv,), k_cache, v_cache, caches)
        hidden = rest_call(1, msg, rows, *shared)
        return hidden, caches[0].reshape(shape), caches[1].reshape(shape)

    return jax.shard_map(device_step, mesh=mesh, in_specs=in_specs, out_specs=out_specs, check_vma=False)
```

```python
import functools
import math

import jax
import jax.numpy as jnp
from jax import lax
from jax.experimental import pallas as pl
from jax.experimental.pallas import tpu as pltpu
from jax.sharding import PartitionSpec as P

BLOCK_SIZE = 64
LOCAL_BLOCKS = 16
VERT_STRIDE = 8
ROPE_THETA = 1000000.0
GELU_LIMIT = 20.0
NORM_EPS = 0.00001
MASKED = -1e30
MESH = pl.DeviceIdType.MESH

NB = 64
D = 3072
HD = 128
KVL = 4
GRP = 3
SLOTS = 64
QW = KVL * (GRP + 2) * HD
QROWS = 16
KCH = 6
KCS = D // KCH
G = 8
NG = NB // G
GS = 16
HALF = NB // 2
HPC = 6
PART = HPC // 2 * HALF + 8
MSG = 2 * PART
MSG_ROOM = 160
ROWS = HALF // 2
F_LOC = 4096
M_LOC = F_LOC // 2
NCH = 2
CW = D // NCH
QCH = 5
QC = QW // QCH
DR = HPC * HD
RCH = 6
RW = D // RCH
LAG = 2
VMEM_BYTES = 52 * 1024 * 1024

f32 = jnp.float32
bf16 = jnp.bfloat16


def norm_rows(rows, gain, shift):
    mean = jnp.mean(rows, axis=-1, keepdims=True)
    cent = rows - mean
    var = jnp.mean(jnp.square(cent), axis=-1, keepdims=True)
    return (cent * lax.rsqrt(var + NORM_EPS)) * gain + shift


def rope_tables(pos):
    half = HD // 2
    row = lax.broadcasted_iota(jnp.int32, (8, HD), 0)
    lane = lax.broadcasted_iota(jnp.int32, (NB, HD), 1)
    groups = []
    for i in range(NB // 8):
        at = jnp.zeros((8, HD), jnp.int32)
        for r in range(8):
            at = jnp.where(row == r, pos[i * 8 + r], at)
        groups.append(at)
    where = jnp.concatenate(groups, axis=0).astype(f32)
    power = (lane % half).astype(f32) * (2.0 / HD)
    angles = where * jnp.exp(power * -math.log(ROPE_THETA))
    sin = jnp.sin(angles)
    return jnp.cos(angles), jnp.where(lane < half, -sin, sin)


def attn_kernel(layer, pos, *rest):
    if layer == 0:
        x, gain, shift, b_qkv, w_hbm, kc_hbm, vc_hbm, *rest = rest
    else:
        acc, kc_hbm, vc_hbm, _, _, *rest = rest
    msg, ko_hbm, vo_hbm, kbuf, vbuf, qs, kns, vns, os, ms, ls, ksem, vsem, osem, *rest = rest
    sp = lax.axis_index('sp')
    tp = lax.axis_index('tp')
    base = sp * SLOTS

    def in_copy(hbm, buf, sem, i):
        return pltpu.make_async_copy(hbm.at[layer, pl.ds(i * G, G)], buf.at[pl.ds(i * G, G)], sem.at[i])

    def out_copy(buf, hbm, j, i):
        return pltpu.make_async_copy(buf.at[pl.ds(i * G, G)], hbm.at[layer, pl.ds(i * G, G)], osem.at[j, i])

    def fetch_cache():
        for i in range(NG):
            in_copy(kc_hbm, kbuf, ksem, i).start(priority=0)
            in_copy(vc_hbm, vbuf, vsem, i).start(priority=1)

    if layer == 0:
        w, u, acc, wsem, *places, msg_buf, small_sem = rest
        msg_hbm, msg = msg, msg_buf
        small = [pltpu.make_async_copy(src, dst, small_sem.at[i]) for i, (src, dst) in enumerate(zip((pos, x, gain, shift, b_qkv), places))]
        for copy in small:
            copy.start()
        pos, x, gain, shift, b_qkv = places

        def w_copy(i):
            return pltpu.make_async_copy(w_hbm.at[layer, pl.ds(i * KCS, KCS), :], w.at[i], wsem.at[i])

        for i in range(KCH):
            w_copy(i).start(priority=i % 2)
        fetch_cache()
        for copy in small:
            copy.wait()
        g_row = gain[layer, 0:1, :].astype(f32)
        s_row = shift[layer, 0:1, :].astype(f32)
        for i in range(NB // 16):
            rows = x[pl.ds(i * 16, 16), :].astype(f32)
            normed = norm_rows(rows, g_row, s_row).astype(bf16)
            for j in range(KCH):
                u[j, pl.ds(i * 16, 16), :] = normed[:, j * KCS:(j + 1) * KCS]
        acc[...] = jnp.broadcast_to(b_qkv[layer:layer + 1, :].astype(f32), (NB, QW))
    else:
        fetch_cache()
    qs[...] = jnp.zeros_like(qs)
    cos_t, sin_t = rope_tables(pos)
    if layer == 0:
        def qkv_step(i, carry):
            w_copy(i).wait()
            acc[...] += jnp.dot(u[i], w[i], preferred_element_type=f32)
            return carry

        lax.fori_loop(0, KCH, qkv_step, 0)

    for c in range(KVL):
        for j in range(GRP + 2):
            if layer == 0:
                col = (c * (GRP + 2) + j) * HD
                tile = acc[:, col:col + HD]
            else:
                head = c * (GRP + 2) + j
                tile = acc[head // (QC // HD), :, head % (QC // HD) * HD:(head % (QC // HD) + 1) * HD]
            if j <= GRP:
                tile = tile * cos_t + pltpu.roll(tile, HD // 2, 1) * sin_t
            for i in range(NB // 8):
                part = tile[i * 8:(i + 1) * 8]
                if j < GRP:
                    qs[pl.ds(i * 8 * QROWS + c * GRP + j, 8, stride=QROWS), :] = part
                else:
                    dst = kns if j == GRP else vns
                    dst[pl.ds(i * 64 + c, 8, stride=8), :] = part
                    dst[pl.ds(i * 64 + c + 4, 8, stride=8), :] = part

    row_h = lax.broadcasted_iota(jnp.int32, (QROWS, SLOTS * KVL), 0)
    col_i = lax.broadcasted_iota(jnp.int32, (QROWS, SLOTS * KVL), 1)
    slot_of = jnp.where(row_h // GRP == col_i % KVL, col_i // KVL, 1 << 20)
    head_id = tp * KVL * GRP + row_h
    vertical = (sp + head_id + 1) % VERT_STRIDE == 0
    sub_row = lax.broadcasted_iota(jnp.int32, (16, HD), 0) // KVL

    def patch(buf, new, b):
        at = pos[b] - base
        atc = jnp.clip(at, 0, SLOTS - 1)
        hit = jnp.logical_and(at >= 0, at < SLOTS)
        put = sub_row == jnp.where(hit, atc % KVL, -1)
        r0 = pl.multiple_of((atc // KVL) * 16, 16)
        new8 = new[b * 8:b * 8 + 8, :]
        new16 = jnp.concatenate([new8, new8], axis=0)
        old = buf[b, pl.ds(r0, 16), :].astype(f32)
        buf[b, pl.ds(r0, 16), :] = jnp.where(put, new16, old).astype(bf16)

    def score(step):
        seqs = range(step * GS, (step + 1) * GS)
        for b in seqs:
            patch(kbuf, kns, b)
        return [lax.dot_general(qs[b * QROWS:(b + 1) * QROWS, :].astype(bf16), kbuf[b], (((1,), (1,)), ((), ())),
                                preferred_element_type=f32) for b in seqs]

    def keep_of(b):
        at = pos[b] - base
        if layer == 0:
            near = pos[b] // BLOCK_SIZE - sp < LOCAL_BLOCKS
            return slot_of <= jnp.where(vertical, at, jnp.where(near, at, -1))
        return slot_of <= at

    def mix(step, scores):
        seqs = range(step * GS, (step + 1) * GS)
        for b in seqs:
            patch(vbuf, vns, b)
        keeps = [keep_of(b) for b in seqs]
        scores = [jnp.where(keep, s * (1.0 / HD), MASKED) for keep, s in zip(keeps, scores)]
        peaks = [jnp.max(s, axis=1, keepdims=True) for s in scores]
        weights = [jnp.where(keep, jnp.exp(s - peak), 0.0) for keep, s, peak in zip(keeps, scores, peaks)]
        outs = [jnp.dot(wt.astype(bf16), vbuf[b], preferred_element_type=f32) for b, wt in zip(seqs, weights)]
        sums = [jnp.sum(wt, axis=1, keepdims=True) for wt in weights]
        for j, b in enumerate(seqs):
            rows = slice(b * QROWS, (b + 1) * QROWS)
            ms[rows, :] = jnp.broadcast_to(peaks[j], (QROWS, HD))
            ls[rows, :] = jnp.broadcast_to(sums[j], (QROWS, HD))
            os[rows, :] = outs[j]

    per = GS // G
    steps = NB // GS
    for j in range(per):
        in_copy(kc_hbm, kbuf, ksem, j).wait()
    scores = score(0)
    for step in range(steps):
        for j in range(step * per, (step + 1) * per):
            in_copy(vc_hbm, vbuf, vsem, j).wait()
            if step + 1 < steps:
                in_copy(kc_hbm, kbuf, ksem, j + per).wait()
        later = score(step + 1) if step + 1 < steps else None
        mix(step, scores)
        scores = later
        for j in range(step * per, (step + 1) * per):
            if step == 0:
                out_copy(kbuf, ko_hbm, 0, j).start()
            if step + 1 < steps:
                out_copy(kbuf, ko_hbm, 0, j + per).start()
            out_copy(vbuf, vo_hbm, 1, j).start(priority=1)

    lane = lax.broadcasted_iota(jnp.int32, (8, HD), 1)
    for half in range(2):
        for c in range(2):
            for part in range(2):
                stat = jnp.zeros((8, HD), f32)
                for g in range(HPC // 2):
                    for i in range(HALF // 8):
                        head = c * HPC + part * (HPC // 2) + g
                        rows = pl.ds((half * HALF + i * 8) * QROWS + head, 8, stride=QROWS)
                        at = 2 * (g * (HALF // 8) + i)
                        msg[half * 2 + c, pl.ds(part * PART + g * HALF + i * 8, 8), :] = os[rows, :]
                        stat = jnp.where(lane == at, ms[rows, :], stat)
                        stat = jnp.where(lane == at + 1, ls[rows, :], stat)
                msg[half * 2 + c, pl.ds(part * PART + PART - 8, 8), :] = stat
    if layer == 0:
        send = pltpu.make_async_copy(msg, msg_hbm.at[pl.ds(0, KVL)], small_sem.at[5])
        send.start()
    for i in range(NG):
        out_copy(kbuf, ko_hbm, 0, i).wait()
        out_copy(vbuf, vo_hbm, 1, i).wait()
    if layer == 0:
        send.wait()


def attn_call(layer, pos, operands, k_cache, v_cache, prev):
    vm = pl.BlockSpec(memory_space=pltpu.VMEM)
    hbm = pl.BlockSpec(memory_space=pltpu.HBM)
    args = [pos, *operands, k_cache, v_cache]
    if layer == 0:
        specs = [hbm] * 8
        alias = {}
        extra = [
            pltpu.VMEM((KCH, KCS, QW), bf16),
            pltpu.VMEM((KCH, NB, KCS), bf16),
            pltpu.VMEM((NB, QW), f32),
            pltpu.SemaphoreType.DMA((KCH,)),
            pltpu.SMEM(pos.shape, jnp.int32),
            *[pltpu.VMEM(arr.shape, bf16) for arr in operands[:4]],
            pltpu.VMEM((KVL, MSG, HD), f32),
            pltpu.SemaphoreType.DMA((6,)),
        ]
        limit = 60 * 1024 * 1024
    else:
        args += list(prev)
        specs = [pl.BlockSpec(memory_space=pltpu.SMEM), vm] + [hbm] * 4
        alias = {4: 1, 5: 2}
        extra = []
        limit = VMEM_BYTES
    cache = jax.ShapeDtypeStruct(k_cache.shape, bf16)
    return pl.pallas_call(
        functools.partial(attn_kernel, layer),
        out_shape=(jax.ShapeDtypeStruct((MSG_ROOM if layer == 0 else KVL, MSG, HD), f32), cache, cache),
        in_specs=specs,
        out_specs=(hbm if layer == 0 else vm, hbm, hbm),
        scratch_shapes=[
            pltpu.VMEM((NB, SLOTS * KVL, HD), bf16),
            pltpu.VMEM((NB, SLOTS * KVL, HD), bf16),
            pltpu.VMEM((NB * QROWS, HD), f32),
            pltpu.VMEM((NB * 8, HD), f32),
            pltpu.VMEM((NB * 8, HD), f32),
            pltpu.VMEM((NB * QROWS, HD), f32),
            pltpu.VMEM((NB * QROWS, HD), f32),
            pltpu.VMEM((NB * QROWS, HD), f32),
            pltpu.SemaphoreType.DMA((NG,)),
            pltpu.SemaphoreType.DMA((NG,)),
            pltpu.SemaphoreType.DMA((2, NG)),
            *extra,
        ],
        input_output_aliases=alias,
        compiler_params=pltpu.CompilerParams(vmem_limit_bytes=limit),
        name=f'attn{layer}',
    )(*args)


def rest_kernel(layer, msg, x, gain, shift, b_dense, b_up, b_down, wd_hbm, wu_hbm, wn_hbm, *rest):
    if layer == 0:
        b_qkv, wq_hbm, x_out, out, *rest = rest
        msg_hbm, (*rest, msg) = msg, rest
    else:
        out, *rest = rest
    (wd, wu, wn, got, sent, o_buf, part, pair, sums, other, ag, full, xrow, up, mbuf,
     wsem, a_sem, d_sem, y_sem, g_sem, x_sem) = rest
    dp = lax.axis_index('dp')
    tp = lax.axis_index('tp')
    sp = lax.axis_index('sp')
    core = sp % 2
    cx = sp // 2
    ox = 1 - cx
    mate = (dp, tp, cx * 2 + 1 - core)
    x_dev = (dp, tp, ox * 2 + core)
    y_dev = (dp, 1 - tp, sp)

    def load(src, dst, i):
        return pltpu.make_async_copy(src, dst, wsem.at[i])

    wd_copy = load(wd_hbm.at[layer, pl.ds(pl.multiple_of(core * DR, DR), DR), :], wd, 0)

    def wu_copy(i):
        return load(wu_hbm.at[layer, pl.ds(i * CW, CW), pl.ds(pl.multiple_of(core * F_LOC, F_LOC), F_LOC)], wu.at[i], 1 + i)

    wn_copy = load(wn_hbm.at[layer, pl.ds(pl.multiple_of(core * M_LOC, M_LOC), M_LOC), :], wn, 1 + NCH)

    def wq_copy(i):
        return load(wq_hbm.at[1, pl.ds(i * CW, CW), :], wu.at[i, :, pl.ds(0, QW)], 2 + NCH + i)

    barrier = pltpu.get_barrier_semaphore()
    for peer in (mate, x_dev, y_dev):
        pl.semaphore_signal(barrier, inc=1, device_id=peer, device_id_type=MESH)
    if layer == 0:
        msg_copy = load(msg_hbm.at[pl.ds(0, KVL)], msg, 2 + 2 * NCH)
        msg_copy.start()
    wd_copy.start()
    for i in range(NCH):
        wu_copy(i).start()
    wn_copy.start()
    pl.semaphore_wait(barrier, 3)
    if layer == 0:
        msg_copy.wait()

    def remote(src, dst, sems, idx, peer):
        return pltpu.make_async_remote_copy(
            src_ref=src, dst_ref=dst, send_sem=sems.at[(0,) + idx], recv_sem=sems.at[(1,) + idx],
            device_id=peer, device_id_type=MESH)

    near = cx * 2 + core
    far = ox * 2 + core
    parts = [pl.ds(k * PART, PART) for k in range(2)]
    swap = [[remote(msg.at[home, parts[k], :], got.at[j, parts[k], :], a_sem, (2 * j + k,), mate) for k in range(2)]
            for j, home in enumerate((ox * 2 + 1 - core, cx * 2 + 1 - core))]
    cross = [remote(sent.at[0, parts[k], :], got.at[2, parts[k], :], a_sem, (4 + k,), x_dev) for k in range(2)]
    for copy in swap[0] + swap[1]:
        copy.start()

    gain1 = gain[layer, 1:2, :].astype(f32)
    shift1 = shift[layer, 1:2, :].astype(f32)
    own = pl.ds(pl.multiple_of(core * ROWS, ROWS), ROWS)
    theirs = pl.ds(pl.multiple_of((1 - core) * ROWS, ROWS), ROWS)

    def all_rows(x_, c_):
        return pl.ds(pl.multiple_of(x_ * HALF + c_ * ROWS, ROWS), ROWS)

    xrow[...] = x[all_rows(cx, core), :].astype(f32) if layer == 0 else x[...]
    lane = lax.broadcasted_iota(jnp.int32, (8, HD), 1)

    def merge(one, two, k, put, stat_out=None):
        stats = [ref[pl.ds(k * PART + PART - 8, 8), :] for ref in (one, two)]
        new_stat = jnp.zeros((8, HD), f32)
        for g in range(HPC // 2):
            for i in range(HALF // 8):
                at = 2 * (g * (HALF // 8) + i)
                peaks = [jnp.broadcast_to(st[:, at:at + 1], (8, HD)) for st in stats]
                tots = [jnp.broadcast_to(st[:, at + 1:at + 2], (8, HD)) for st in stats]
                top = jnp.maximum(peaks[0], peaks[1])
                scale = [jnp.exp(p - top) for p in peaks]
                rows = pl.ds(k * PART + g * HALF + i * 8, 8)
                num = one[rows, :] * scale[0] + two[rows, :] * scale[1]
                den = tots[0] * scale[0] + tots[1] * scale[1]
                put(k, g, i, num, den)
                if stat_out is not None:
                    new_stat = jnp.where(lane == at, top, new_stat)
                    new_stat = jnp.where(lane == at + 1, den, new_stat)
        if stat_out is not None:
            stat_out[pl.ds(k * PART + PART - 8, 8), :] = new_stat

    def put_part(ref):
        def put(k, g, i, num, den):
            ref[pl.ds(k * PART + g * HALF + i * 8, 8), :] = num
        return put

    def put_out(k, g, i, num, den):
        head = k * (HPC // 2) + g
        o_buf[pl.ds(i * 8, 8), head * HD:(head + 1) * HD] = num / den

    for k in range(2):
        swap[0][k].wait_recv()
        merge(msg.at[far], got.at[0], k, put_part(sent.at[0]), sent.at[0])
        cross[k].start()
    for k in range(2):
        swap[1][k].wait_recv()
        merge(msg.at[near], got.at[1], k, put_part(sent.at[1]), sent.at[1])
    for k in range(2):
        cross[k].wait_recv()
        merge(sent.at[1], got.at[2], k, put_out)
    sends = swap[0] + swap[1] + cross

    def reduce(ph, product, finish):
        first = [remote(part.at[ph, n, theirs, :], pair.at[ph, n], d_sem, (ph, n), mate) for n in range(RCH)]
        second = [remote(sums.at[ph, n], other.at[ph, n], y_sem, (ph, n), y_dev) for n in range(RCH)]
        for step in range(RCH + LAG):
            if step < RCH:
                part[ph, step] = product(step)
                first[step].start()
            if step >= LAG:
                n = step - LAG
                first[n].wait_recv()
                sums[ph, n] = part[ph, n, own, :] + pair[ph, n]
                second[n].start()
        for n in range(RCH):
            second[n].wait_recv()
            finish(n, sums[ph, n] + other[ph, n])
        return first + second

    def residual(n, total, bias):
        cols = slice(n * RW, (n + 1) * RW)
        v = xrow[:, cols] + total + bias[layer:layer + 1, cols].astype(f32)
        xrow[:, cols] = v.astype(bf16).astype(f32)

    wd_copy.wait()
    o = o_buf[...].astype(bf16)
    sends += reduce(0, lambda n: jnp.dot(o, wd[:, n * RW:(n + 1) * RW], preferred_element_type=f32),
                   lambda n, total: residual(n, total, b_dense))

    normed = norm_rows(xrow[...], gain1, shift1).astype(bf16).astype(f32)
    swap = []
    for n in range(NCH):
        ag[n, own, :] = normed[:, n * CW:(n + 1) * CW]
        here = ag.at[n, own, :]
        swap.append(remote(here, here, g_sem, (n,), mate))
        swap[n].start()
    cols_up = pl.ds(pl.multiple_of(core * F_LOC, F_LOC), F_LOC)
    up[...] = jnp.broadcast_to(b_up[layer:layer + 1, cols_up].astype(f32), (HALF, F_LOC))
    for n in range(NCH):
        wu_copy(n).wait()
        swap[n].wait_recv()
        up[...] += jnp.dot(ag[n].astype(bf16), wu[n], preferred_element_type=f32)
        if layer == 0:
            wq_copy(n).start()

    pick = (lax.broadcasted_iota(jnp.int32, (256, 128), 0) == 2 * lax.broadcasted_iota(jnp.int32, (256, 128), 1))
    pick = jnp.where(pick, 1.0, 0.0).astype(bf16)
    for k in range(F_LOC // 256):
        a = up[:, k * 256:(k + 1) * 256]
        z = jnp.minimum(a, GELU_LIMIT)
        gate = z * jax.nn.sigmoid(1.702 * z)
        lin = jnp.clip(a, -GELU_LIMIT, GELU_LIMIT) + 1.0
        prod = (gate * pltpu.roll(lin, 255, 1)).astype(bf16)
        mbuf[:, k * 128:(k + 1) * 128] = jnp.dot(prod, pick, preferred_element_type=f32).astype(bf16)
    wn_copy.wait()
    m = mbuf[...]
    sends += swap

    def spread(n, value):
        full[n, all_rows(cx, core), :] = value
        here = full.at[n, all_rows(cx, core), :]
        for k, peer in enumerate((x_dev, mate)):
            copy = remote(here, here, x_sem, (k, n), peer)
            copy.start()
            sends.append(copy)

    def collect(chunks, use):
        for n in range(chunks):
            there = full.at[n, all_rows(ox, core), :]
            remote(there, there, x_sem, (0, n), x_dev).wait_recv()
            copy = remote(there, there, x_sem, (2, n), mate)
            copy.start()
            sends.append(copy)
        for n in range(chunks):
            for k, x_ in ((1, cx), (2, ox)):
                there = full.at[n, all_rows(x_, 1 - core), :]
                remote(there, there, x_sem, (k, n), mate).wait_recv()
            use(n)

    def take_down(n, total):
        residual(n, total, b_down)
        if layer == 1:
            spread(n, xrow[:, n * RW:(n + 1) * RW])

    sends += reduce(1, lambda n: jnp.dot(m, wn[:, n * RW:(n + 1) * RW], preferred_element_type=f32), take_down)
    if layer == 0:
        x_out[...] = xrow[...]
        u = norm_rows(xrow[...], gain[1, 0:1, :].astype(f32), shift[1, 0:1, :].astype(f32)).astype(bf16)
        for i in range(NCH):
            wq_copy(i).wait()
        for n in range(QCH):
            cols = slice(n * QC, (n + 1) * QC)
            r = jnp.broadcast_to(b_qkv[1:2, cols].astype(f32), (ROWS, QC))
            for i in range(NCH):
                r += jnp.dot(u[:, i * CW:(i + 1) * CW], wu[i, :, cols], preferred_element_type=f32)
            spread(n, r)

        def use(n):
            out[n] = full[n]
    else:
        def use(n):
            out[:, n * RW:(n + 1) * RW] = full[n].astype(bf16)

    collect(QCH if layer == 0 else RCH, use)
    for copy in sends:
        copy.wait_send()


def rest_call(layer, msg, x, gain, shift, b_dense, b_up, b_down, w_dense, w_up, w_down, *qkv):
    vm = pl.BlockSpec(memory_space=pltpu.VMEM)
    hbm = pl.BlockSpec(memory_space=pltpu.HBM)
    if layer == 0:
        in_specs = [hbm] + [vm] * 6 + [hbm] * 3 + [vm, hbm]
        out_shape = (jax.ShapeDtypeStruct((ROWS, D), f32), jax.ShapeDtypeStruct((QCH, NB, QC), f32))
        out_specs = (vm, vm)
    else:
        in_specs = [vm] * 7 + [hbm] * 3
        out_shape = jax.ShapeDtypeStruct((NB, D), bf16)
        out_specs = vm
    return pl.pallas_call(
        functools.partial(rest_kernel, layer),
        out_shape=out_shape,
        in_specs=in_specs,
        out_specs=out_specs,
        scratch_shapes=[
            pltpu.VMEM((DR, D), bf16),
            pltpu.VMEM((NCH, CW, F_LOC), bf16),
            pltpu.VMEM((M_LOC, D), bf16),
            pltpu.VMEM((3, MSG, HD), f32),
            pltpu.VMEM((2, MSG, HD), f32),
            pltpu.VMEM((HALF, DR), f32),
            pltpu.VMEM((2, RCH, HALF, RW), f32),
            pltpu.VMEM((2, RCH, ROWS, RW), f32),
            pltpu.VMEM((2, RCH, ROWS, RW), f32),
            pltpu.VMEM((2, RCH, ROWS, RW), f32),
            pltpu.VMEM((NCH, HALF, CW), f32),
            pltpu.VMEM((QCH, NB, QC) if layer == 0 else (RCH, NB, RW), f32),
            pltpu.VMEM((ROWS, D), f32),
            pltpu.VMEM((HALF, F_LOC), f32),
            pltpu.VMEM((HALF, M_LOC), bf16),
            pltpu.SemaphoreType.DMA((3 + 2 * NCH,)),
            pltpu.SemaphoreType.DMA((2, 6)),
            pltpu.SemaphoreType.DMA((2, 2, RCH)),
            pltpu.SemaphoreType.DMA((2, 2, RCH)),
            pltpu.SemaphoreType.DMA((2, NCH)),
            pltpu.SemaphoreType.DMA((2, 3, RCH)),
            *([pltpu.VMEM((KVL, MSG, HD), f32)] if layer == 0 else []),
        ],
        compiler_params=pltpu.CompilerParams(vmem_limit_bytes=VMEM_BYTES, collective_id=layer, has_side_effects=True),
        name=f'rest{layer}',
    )(msg, x, gain, shift, b_dense, b_up, b_down, w_dense, w_up, w_down, *qkv)


def solution(mesh):
    cache_spec = P(None, 'dp', 'sp', 'tp', None)
    in_specs = (P('dp', None), P('dp'), cache_spec, cache_spec, P(), P(), P(None, None, 'tp'), P(None, 'tp'), P(None, 'tp', None), P(), P(None, None, 'tp'), P(None, 'tp'), P(None, 'tp', None), P())
    out_specs = (P('dp', None), cache_spec, cache_spec)

    def device_step(hidden, positions, k_cache, v_cache, ln_gain, ln_bias, w_qkv, b_qkv, w_dense, b_dense, w_up, b_up, w_down, b_down):
        shape = k_cache.shape
        flat = (2, NB, SLOTS * KVL, HD)
        k_cache = k_cache.reshape(flat)
        v_cache = v_cache.reshape(flat)
        shared = (ln_gain, ln_bias, b_dense, b_up, b_down, w_dense, w_up, w_down)
        msg, *caches = attn_call(0, positions, (hidden, ln_gain, ln_bias, b_qkv, w_qkv), k_cache, v_cache, None)
        rows, qkv = rest_call(0, msg, hidden, *shared, b_qkv, w_qkv)
        msg, *caches = attn_call(1, positions, (qkv,), k_cache, v_cache, caches)
        hidden = rest_call(1, msg, rows, *shared)
        return hidden, caches[0].reshape(shape), caches[1].reshape(shape)

    return jax.shard_map(device_step, mesh=mesh, in_specs=in_specs, out_specs=out_specs, check_vma=False)
```
